32 devices in a mesh: dp: 8 (over z, y), mp: 4 (over x, core).
Axes of the slice: x: 2, y: 2, z: 4, core: 2. Of those that a mesh axis runs over, the one named last changes fastest.
Arguments:
- inputs: bfloat16 [8192, 768], P(('dp', 'mp')), may hold values from -6 to 6
- memory: bfloat16 [32768, 768], P(('dp', 'mp')), may hold values from -6 to 6
- target_len: int32 [64], P('dp'), may hold values from 8 to 114, as said below
- memory_len: int32 [64], P('dp'), may hold values from 32 to 512, as said below
- bucket_map: int32 [128], replicated, may hold values from 0 to 31, as said below
- self_gain: float32 [768], replicated, may hold values from 0.5 to 1.5
- self_query: bfloat16 [768, 768], P(None, 'mp'), may hold values from -0.02734375 to 0.02734375
- self_key: bfloat16 [768, 768], P(None, 'mp'), may hold values from -0.21875 to 0.21875
- self_value: bfloat16 [768, 768], P(None, 'mp'), may hold values from -0.21875 to 0.21875
- self_out: bfloat16 [768, 768], P('mp'), may hold values from -1.25 to 1.25
- bias_table: float32 [32, 12], P(None, 'mp'), may hold values from -4 to 4
- cross_gain: float32 [768], replicated, may hold values from 0.5 to 1.5
- cross_query: bfloat16 [768, 768], P(None, 'mp'), may hold values from -0.02734375 to 0.02734375
- cross_key: bfloat16 [768, 768], P(None, 'mp'), may hold values from -0.21875 to 0.21875
- cross_value: bfloat16 [768, 768], P(None, 'mp'), may hold values from -0.21875 to 0.21875
- cross_out: bfloat16 [768, 768], P('mp'), may hold values from -2.5 to 2.5
- feed_gain: float32 [768], replicated, may hold values from 0.5 to 1.5
- feed_input: bfloat16 [768, 3072], P(None, 'mp'), may hold values from -0.21875 to 0.21875
- feed_output: bfloat16 [3072, 768], P('mp'), may hold values from -0.15625 to 0.15625
- cotangent: bfloat16 [8192, 768], P(('dp', 'mp')), may hold values from -6 to 6
Outputs:
- layer_out: bfloat16 [8192, 768], P(('dp', 'mp'))
- inputs_grad: float32 [8192, 768], P(('dp', 'mp'))
- memory_grad: float32 [32768, 768], P(('dp', 'mp'))
- self_gain_grad: float32 [768], replicated
- self_query_grad: float32 [768, 768], P(None, 'mp')
- self_key_grad: float32 [768, 768], P(None, 'mp')
- self_value_grad: float32 [768, 768], P(None, 'mp')
- self_out_grad: float32 [768, 768], P('mp')
- bias_table_grad: float32 [32, 12], P(None, 'mp')
- cross_gain_grad: float32 [768], replicated
- cross_query_grad: float32 [768, 768], P(None, 'mp')
- cross_key_grad: float32 [768, 768], P(None, 'mp')
- cross_value_grad: float32 [768, 768], P(None, 'mp')
- cross_out_grad: float32 [768, 768], P('mp')
- feed_gain_grad: float32 [768], replicated
- feed_input_grad: float32 [768, 3072], P(None, 'mp')
- feed_output_grad: float32 [3072, 768], P('mp')
The draws below stay inside these ranges and needn't reach their ends.
Inputs may be any that keep to these rules, and one draw needn't show every extreme that they name: bucket_map[d] is the bucket of a key d positions before its query: it equals d below 16, never falls as d grows, and reaches 31. An example's target rows at positions from target_len on are padding. An example's memory rows at positions from memory_len on are padding.
All inputs are finite; a program needn't handle non-finite values.
Results may differ from the reference program's by a relative error of at most 0.023.
Values may be sent and summed in bfloat16 or wider, within the bound.
No kernel may reach another device: no remote copies, remote signals or barrier semaphores. Data moves between devices by JAX's collectives and lax.ppermute only.
A program may use at most 128 MiB of HBM per device.

```python
import jax
import jax.numpy as jnp
from jax import lax

D = 768
HEADS = 12
HEAD_DIM = 64
FF = 3072
BUCKETS = 32
TGT_LEN = 128
MEM_LEN = 512
EX_DEV = 8
EXAMPLES = 64
TOKENS = 8192
MEM_TOKENS = 32768


def draw_target_len(key, part):
    key_lengths, key_longest, key_offset = jax.random.split(key, 3)
    lengths = jax.random.randint(key_lengths, (EXAMPLES,), 8, 115)
    longest = jax.random.randint(key_longest, (), 0, EXAMPLES)
    offset = jax.random.randint(key_offset, (), 1, EXAMPLES)
    shortest = (longest + offset) % EXAMPLES
    slots = jnp.arange(EXAMPLES)
    lengths = jnp.where(slots == longest, 114, lengths)
    lengths = jnp.where(slots == shortest, 8, lengths)
    return lengths.astype(jnp.int32)


def draw_memory_len(key, part):
    key_first, key_second, key_longest, key_offset = jax.random.split(key, 4)
    spread = MEM_LEN - 32
    factor_one = jax.random.randint(key_first, (EXAMPLES,), 0, spread + 1)
    factor_two = jax.random.randint(key_second, (EXAMPLES,), 0, spread + 1)
    lengths = MEM_LEN - factor_one * factor_two // spread
    longest = jax.random.randint(key_longest, (), 0, EXAMPLES)
    offset = jax.random.randint(key_offset, (), 1, EXAMPLES)
    shortest = (longest + offset) % EXAMPLES
    slots = jnp.arange(EXAMPLES)
    lengths = jnp.where(slots == longest, MEM_LEN, lengths)
    lengths = jnp.where(slots == shortest, 32, lengths)
    return lengths.astype(jnp.int32)


def draw_bucket_map(key, part):
    exact = BUCKETS // 2
    cuts = jax.random.permutation(key, TGT_LEN - exact - 1)[:exact - 1] + 1
    distance = jnp.arange(TGT_LEN)
    beyond = distance - exact
    counted = jnp.sum((cuts[None, :] <= beyond[:, None]).astype(jnp.int32), -1)
    return jnp.where(distance < exact, distance, exact + counted).astype(jnp.int32)


def block_levels(stream_key, dims, cuts, low, top_value):
    factor_of = 1.0
    for position, blocks in cuts:
        draws = jax.random.uniform(jax.random.fold_in(jax.random.fold_in(stream_key, 6), position), (blocks,), jnp.float32, low / len(cuts), top_value / len(cuts))
        factor_of = factor_of * jnp.repeat(jnp.exp(draws), dims[position] // blocks).reshape((-1,) + (1,) * (len(dims) - 1 - position))
    return factor_of


def bell_draw(rng, extent, scale, reach, cuts=(), kind=jnp.bfloat16):
    level = block_levels(rng, extent, cuts, -0.22, 0.18) if cuts else 1.0
    array = jax.random.normal(rng, extent, jnp.float32) * scale * level
    return jnp.minimum(jnp.maximum(array, -reach), reach).astype(kind)


def setup_inputs(seed: int = 0) -> dict:
    keys = jax.random.split(jax.random.key(seed), 21)
    inputs = bell_draw(keys[0], (TOKENS, D), 1.0, 6.0, ((0, 32),))
    memory = bell_draw(keys[1], (MEM_TOKENS, D), 1.0, 6.0, ((0, 32),))
    target_len = draw_target_len(jax.random.fold_in(keys[20], 71), 0)
    memory_len = draw_memory_len(jax.random.fold_in(keys[20], 71), 0)
    bucket_map = draw_bucket_map(jax.random.fold_in(keys[20], 71), 0)
    self_gain = jnp.clip(1.0 + 0.1 * jax.random.normal(keys[5], (D,), jnp.float32), 0.5, 1.5)
    self_query = bell_draw(keys[6], (D, HEADS * HEAD_DIM), (D * HEAD_DIM) ** -0.5, 0.02734375, ((1, 4),))
    self_key = bell_draw(keys[7], (D, HEADS * HEAD_DIM), D ** -0.5, 0.21875, ((1, 4),))
    self_value = bell_draw(keys[8], (D, HEADS * HEAD_DIM), D ** -0.5, 0.21875, ((1, 4),))
    self_out = bell_draw(keys[9], (HEADS * HEAD_DIM, D), (max(HEADS * HEAD_DIM // 32, 1)) ** -0.5, 1.25, ((0, 4),))
    bias_table = bell_draw(keys[10], (BUCKETS, HEADS), 1.0, 4.0, ((1, 4),), jnp.float32)
    cross_gain = jnp.clip(1.0 + 0.1 * jax.random.normal(keys[11], (D,), jnp.float32), 0.5, 1.5)
    cross_query = bell_draw(keys[12], (D, HEADS * HEAD_DIM), (D * HEAD_DIM) ** -0.5, 0.02734375, ((1, 4),))
    cross_key = bell_draw(keys[13], (D, HEADS * HEAD_DIM), D ** -0.5, 0.21875, ((1, 4),))
    cross_value = bell_draw(keys[14], (D, HEADS * HEAD_DIM), D ** -0.5, 0.21875, ((1, 4),))
    cross_out = bell_draw(keys[15], (HEADS * HEAD_DIM, D), (max(HEADS * HEAD_DIM // 128, 1)) ** -0.5, 2.5, ((0, 4),))
    feed_gain = jnp.clip(1.0 + 0.1 * jax.random.normal(keys[16], (D,), jnp.float32), 0.5, 1.5)
    feed_input = bell_draw(keys[17], (D, FF), D ** -0.5, 0.21875, ((1, 4),))
    feed_output = bell_draw(keys[18], (FF, D), (FF // 2) ** -0.5, 0.15625, ((0, 4),))
    cotangent = bell_draw(keys[19], (TOKENS, D), 1.0, 6.0, ((0, 32),))
    return {"inputs": inputs, "memory": memory, "target_len": target_len, "memory_len": memory_len, "bucket_map": bucket_map, "self_gain": self_gain, "self_query": self_query, "self_key": self_key, "self_value": self_value, "self_out": self_out, "bias_table": bias_table, "cross_gain": cross_gain, "cross_query": cross_query, "cross_key": cross_key, "cross_value": cross_value, "cross_out": cross_out, "feed_gain": feed_gain, "feed_input": feed_input, "feed_output": feed_output, "cotangent": cotangent}


@jax.custom_vjp
def low(v):
    return lax.optimization_barrier(v.astype(jnp.bfloat16)).astype(jnp.float32)

@jax.custom_vjp
def low_back(v):
    return v

def low_keep(v):
    return (low(v), None)

def low_pass(kept, grad):
    return (grad,)

def back_keep(v):
    return (v, None)

def back_low(kept, grad):
    return (low(grad),)
low.defvjp(low_keep, low_pass)
low_back.defvjp(back_keep, back_low)
masked_fill = -1000000000.0
epsilon = 1e-06
highest = lax.Precision.HIGHEST
tanh_scale = 0.7978845608
cubic_term = 0.044715

def gelu_tanh(value):
    return 0.5 * value * (1.0 + jnp.tanh(tanh_scale * (value + cubic_term * value * value * value)))

def matmul(left, right):
    return jnp.dot(left, right, precision=highest)

def norm_rows(hidden, gain):
    return hidden * lax.rsqrt(lax.optimization_barrier(jnp.mean(hidden * hidden, -1, keepdims=True)) + epsilon) * gain

def project(normed, weight):
    return low(low_back(matmul(normed, weight)))

def attention(queries, key_blocks, value_blocks, extra, valid):
    scores = low_back(jnp.einsum('eqhd,ekhd->ehqk', queries, key_blocks, precision=highest)) + extra
    filler = jnp.full_like(scores, masked_fill)
    scores = jnp.where(valid, scores, filler)
    probs = low(jax.nn.softmax(scores, axis=-1))
    mixed = jnp.einsum('ehqk,ekhd->eqhd', probs, value_blocks, precision=highest)
    return low(low_back(mixed))

def layer(inputs, memory, target_len, memory_len, bucket_map, weights):
    self_gain, self_query, self_key, self_value, self_out, bias_table, cross_gain, cross_query, cross_key, cross_value, cross_out, feed_gain, feed_input, feed_output = weights
    groups = target_len.shape[0]
    target_len = target_len.astype(jnp.int32)
    memory_len = memory_len.astype(jnp.int32)
    bucket_map = bucket_map.astype(jnp.int32)

    def heads_of(rows, length):
        return rows.reshape(groups, length, HEADS, HEAD_DIM)

    def merged(mixed):
        return mixed.reshape(groups * TGT_LEN, HEADS * HEAD_DIM)
    positions = jnp.arange(TGT_LEN, dtype=jnp.int32)
    distance = jnp.maximum(positions[:, None] - positions[None, :], 0).astype(jnp.int32)
    bucket_index = jnp.take(bucket_map, distance.reshape(-1), axis=0).astype(jnp.int32)
    bias_rows = jnp.take(bias_table, bucket_index, axis=0).reshape(TGT_LEN, TGT_LEN, -1)
    bias_term = jnp.transpose(bias_rows, (2, 0, 1))[None]
    causal = positions[None, :] <= positions[:, None]
    self_valid = causal[None, None] & (positions[None, None, None, :] < target_len[:, None, None, None])
    memory_pos = jnp.arange(MEM_LEN, dtype=jnp.int32)
    cross_valid = (memory_pos[None, :] < memory_len[:, None])[:, None, None, :]
    normed = low(norm_rows(inputs, self_gain))
    mixed = attention(heads_of(project(normed, self_query), TGT_LEN), heads_of(project(normed, self_key), TGT_LEN), heads_of(project(normed, self_value), TGT_LEN), bias_term, self_valid)
    stream = inputs + low_back(matmul(merged(mixed), self_out))
    normed = low(norm_rows(stream, cross_gain))
    mixed = attention(heads_of(project(normed, cross_query), TGT_LEN), heads_of(project(memory, cross_key), MEM_LEN), heads_of(project(memory, cross_value), MEM_LEN), jnp.zeros((), stream.dtype), cross_valid)
    stream = stream + low_back(matmul(merged(mixed), cross_out))
    normed = low(norm_rows(stream, feed_gain))
    hidden = low(gelu_tanh(low_back(matmul(normed, feed_input))))
    return stream + low_back(matmul(hidden, feed_output))

def reference(inputs, memory, target_len, memory_len, bucket_map, self_gain, self_query, self_key, self_value, self_out, bias_table, cross_gain, cross_query, cross_key, cross_value, cross_out, feed_gain, feed_input, feed_output, cotangent):
    weights = tuple((weight.astype(jnp.float32) for weight in (self_gain, self_query, self_key, self_value, self_out, bias_table, cross_gain, cross_query, cross_key, cross_value, cross_out, feed_gain, feed_input, feed_output)))
    groups = target_len.shape[0] // EX_DEV
    input_rows = inputs.astype(jnp.float32).reshape(groups, EX_DEV * TGT_LEN, D)
    memory_rows = memory.astype(jnp.float32).reshape(groups, EX_DEV * MEM_LEN, D)
    upstream_rows = cotangent.astype(jnp.float32).reshape(groups, EX_DEV * TGT_LEN, D)
    target_rows = target_len.astype(jnp.int32).reshape(groups, EX_DEV)
    length_rows = memory_len.astype(jnp.int32).reshape(groups, EX_DEV)
    bucket_ids = bucket_map.astype(jnp.int32)

    def accumulate(totals, pieces):
        input_piece, memory_piece, target_piece, length_piece, upstream_piece = pieces

        def forward(input_value, memory_value, *weight_values):
            return layer(input_value, memory_value, target_piece, length_piece, bucket_ids, weight_values)
        output, pullback = jax.vjp(forward, input_piece, memory_piece, *weights)
        grads = pullback(upstream_piece)
        totals = tuple((total + grad.astype(total.dtype) for total, grad in zip(totals, grads[2:])))
        return (totals, (output.astype(jnp.bfloat16), grads[0], grads[1]))
    zeros = tuple((jnp.zeros(weight.shape, weight.dtype) for weight in weights))
    totals, stacked = lax.scan(accumulate, zeros, (input_rows, memory_rows, target_rows, length_rows, upstream_rows))
    outputs, input_grads, memory_grads = stacked
    gain_one, query_one, key_one, value_one, out_one, table_grad, gain_two, query_two, key_two, value_two, out_two, gain_three, input_three, output_three = totals
    return (outputs.reshape(-1, D), input_grads.reshape(-1, D), memory_grads.reshape(-1, D), gain_one, query_one, key_one, value_one, out_one, table_grad, gain_two, query_two, key_two, value_two, out_two, gain_three, input_three, output_three)
```

```python
import jax
import jax.numpy as jnp
from jax import lax
from jax.sharding import PartitionSpec as P

HEAD_DIM = 64
BUCKETS = 32
TGT_LEN = 128
MEM_LEN = 512

masked_fill = -1000000000.0
epsilon = 1e-06
highest = lax.Precision.HIGHEST
tanh_scale = 0.7978845608
cubic_term = 0.044715
bf16 = jnp.bfloat16
f32 = jnp.float32


def gelu_tanh(value):
    return 0.5 * value * (1.0 + jnp.tanh(tanh_scale * (value + cubic_term * value * value * value)))


def norm_forward(hidden, gain):
    scale = lax.rsqrt(jnp.mean(hidden * hidden, -1, keepdims=True) + epsilon)
    return (hidden * scale * gain, scale)


def norm_backward(hidden, scale, gain, upstream):
    weighted = gain * upstream
    return scale * weighted - hidden * scale**3 * jnp.mean(hidden * weighted, -1, keepdims=True)


def swap_core(a):
    return lax.ppermute(a, "mp", [(0, 1), (1, 0), (2, 3), (3, 2)])


def swap_chip(a):
    return lax.ppermute(a, "mp", [(0, 2), (2, 0), (1, 3), (3, 1)])


def gather_blocks(a):
    far = swap_chip(a)
    return (a, swap_core(a), far, swap_core(far))


def scatter_sum(own, core, chip, both):
    got = swap_core(jnp.stack([core.astype(bf16), both.astype(bf16)]))
    mine = own + got[0].astype(f32)
    far = (chip + got[1].astype(f32)).astype(bf16)
    return mine + swap_chip(far).astype(f32)


def reduce_dp(rows):
    size = lax.axis_size("dp")
    me = lax.axis_index("dp")
    value = rows
    bits = size.bit_length() - 1
    for bit in range(bits):
        half = value.shape[0] // 2
        mine = (me >> bit) & 1
        pairs = [(i, i ^ (1 << bit)) for i in range(size)]
        send = lax.dynamic_slice_in_dim(value, (1 - mine) * half, half, 0).astype(bf16)
        keep = lax.dynamic_slice_in_dim(value, mine * half, half, 0)
        value = keep.astype(f32) + lax.ppermute(send, "dp", pairs).astype(f32)
    value = value.astype(bf16)
    for bit in reversed(range(bits)):
        mine = (me >> bit) & 1
        pairs = [(i, i ^ (1 << bit)) for i in range(size)]
        other = lax.ppermute(value, "dp", pairs)
        first = jnp.where(mine == 0, value, other)
        second = jnp.where(mine == 0, other, value)
        value = jnp.concatenate([first, second], 0)
    return value.astype(f32)


def dot(a, b, dims):
    return lax.dot_general(a, b, ((dims[0:1], dims[1:2]), ((), ())), preferred_element_type=f32)


def split_heads(rows, groups, length):
    return rows.reshape(groups, length, rows.shape[1] // HEAD_DIM, HEAD_DIM)


def probabilities(queries, key_blocks, extra, valid):
    scores = jnp.einsum("eqhd,ekhd->ehqk", queries, key_blocks, preferred_element_type=f32) + extra
    scores = jnp.where(valid, scores, masked_fill)
    weights = jnp.exp(scores - jnp.max(scores, -1, keepdims=True))
    return weights / jnp.sum(weights, -1, keepdims=True)


def attend(query_rows, key_rows, value_rows, extra, valid, key_len):
    groups = valid.shape[0]
    probs = probabilities(
        split_heads(query_rows, groups, TGT_LEN), split_heads(key_rows, groups, key_len), extra, valid
    )
    mixed = jnp.einsum(
        "ehqk,ekhd->eqhd", probs.astype(bf16), split_heads(value_rows, groups, key_len), preferred_element_type=f32
    )
    return mixed.astype(bf16).reshape(query_rows.shape)


def attend_back(query_rows, key_rows, value_rows, extra, valid, key_len, mixed_grad):
    groups = valid.shape[0]
    queries = split_heads(query_rows, groups, TGT_LEN)
    key_blocks = split_heads(key_rows, groups, key_len)
    value_blocks = split_heads(value_rows, groups, key_len)
    grad_blocks = split_heads(mixed_grad, groups, TGT_LEN)
    probs = probabilities(queries, key_blocks, extra, valid)
    value_grad = jnp.einsum("ehqk,eqhd->ekhd", probs.astype(bf16), grad_blocks, preferred_element_type=f32)
    prob_grad = jnp.einsum("eqhd,ekhd->ehqk", grad_blocks, value_blocks, preferred_element_type=f32)
    score_grad = probs * (prob_grad - jnp.sum(probs * prob_grad, -1, keepdims=True))
    score_low = score_grad.astype(bf16)
    query_grad = jnp.einsum("ehqk,ekhd->eqhd", score_low, key_blocks, preferred_element_type=f32)
    key_grad = jnp.einsum("ehqk,eqhd->ekhd", score_low, queries, preferred_element_type=f32)
    return (
        query_grad.astype(bf16).reshape(query_rows.shape),
        key_grad.astype(bf16).reshape(key_rows.shape),
        value_grad.astype(bf16).reshape(value_rows.shape),
        score_grad,
    )


def matrices(blocks, count):
    width = blocks[0].shape[0] // count
    return [jnp.concatenate([b[m * width : (m + 1) * width] for b in blocks], 0) for m in range(count)]


def mp_sum(grads):
    width = grads[0].shape[0] // 4
    parts = [jnp.concatenate([g[j * width : (j + 1) * width] for g in grads], 0) for j in range(4)]
    return scatter_sum(*parts)


def body(
    inputs,
    memory,
    target_len,
    memory_len,
    bucket_map,
    self_gain,
    self_query,
    self_key,
    self_value,
    self_out,
    bias_table,
    cross_gain,
    cross_query,
    cross_key,
    cross_value,
    cross_out,
    feed_gain,
    feed_input,
    feed_output,
    cotangent,
):
    rank = lax.axis_index("mp")
    examples = inputs.shape[0] // TGT_LEN
    target_len = lax.dynamic_slice_in_dim(target_len, rank * examples, examples, 0)
    memory_len = lax.dynamic_slice_in_dim(memory_len, rank * examples, examples, 0)
    width = self_query.shape[1]

    self_stack = jnp.concatenate([self_query.T, self_key.T, self_value.T, self_out], 0)
    cross_stack = jnp.concatenate([cross_query.T, cross_key.T, cross_value.T, cross_out], 0)
    table = jnp.concatenate(gather_blocks(bias_table), 1)
    sq, sk, sv, so = matrices(gather_blocks(self_stack), 4)
    cq, ck, cv, co = matrices(gather_blocks(cross_stack), 4)
    feed_up = jnp.concatenate(gather_blocks(cotangent), 0)

    positions = jnp.arange(TGT_LEN, dtype=jnp.int32)
    distance = jnp.maximum(positions[:, None] - positions[None, :], 0)
    lookup = distance[:, :, None] == positions[None, None, :]
    bucket_index = jnp.sum(jnp.where(lookup, bucket_map[None, None, :], 0), -1)
    causal = positions[None, :] <= positions[:, None]
    bucket_ids = jnp.arange(BUCKETS, dtype=jnp.int32)
    bucket_hot = (
        (bucket_index[:, :, None] == bucket_ids[None, None, :]) & causal[:, :, None]
    ).astype(jnp.float32)
    self_bias = jnp.einsum("qkb,bh->hqk", bucket_hot, table, precision=highest)[None]
    self_valid = causal[None, None] & (positions[None, None, None, :] < target_len[:, None, None, None])
    memory_pos = jnp.arange(MEM_LEN, dtype=jnp.int32)
    cross_valid = (memory_pos[None, :] < memory_len[:, None])[:, None, None, :]

    stream = inputs.astype(f32)
    normed, scale_one = norm_forward(stream, self_gain)
    normed_one = normed.astype(bf16)
    self_q = dot(normed_one, sq, (1, 1)).astype(bf16)
    self_k = dot(normed_one, sk, (1, 1)).astype(bf16)
    self_v = dot(normed_one, sv, (1, 1)).astype(bf16)
    self_mixed = attend(self_q, self_k, self_v, self_bias, self_valid, TGT_LEN)
    after_self = stream + dot(self_mixed, so, (1, 0))
    normed, scale_two = norm_forward(after_self, cross_gain)
    normed_two = normed.astype(bf16)
    cross_q = dot(normed_two, cq, (1, 1)).astype(bf16)
    cross_k = dot(memory, ck, (1, 1)).astype(bf16)
    cross_v = dot(memory, cv, (1, 1)).astype(bf16)
    cross_mixed = attend(cross_q, cross_k, cross_v, 0.0, cross_valid, MEM_LEN)
    after_cross = after_self + dot(cross_mixed, co, (1, 0))
    normed, scale_three = norm_forward(after_cross, feed_gain)
    gathered = jnp.concatenate(gather_blocks(normed.astype(bf16)), 0)

    rows = inputs.shape[0]

    def blocks_of(a):
        return [a[j * rows : (j + 1) * rows] for j in range(4)]

    pre_act = dot(gathered, feed_input, (1, 0))
    act_value, act_pullback = jax.vjp(gelu_tanh, pre_act)
    activated = act_value.astype(bf16)
    hidden_grad = dot(feed_up, feed_output, (1, 1))
    pre_grad = act_pullback(hidden_grad)[0].astype(bf16)
    normed_three_grad = scatter_sum(*blocks_of(dot(pre_grad, feed_input, (1, 1))))
    layer_out = (after_cross + scatter_sum(*blocks_of(dot(activated, feed_output, (1, 0))))).astype(bf16)
    feed_part = jnp.concatenate([dot(gathered, pre_grad, (0, 0)), dot(activated, feed_up, (0, 0))], 0)
    feed_sum = reduce_dp(feed_part)

    upstream = cotangent.astype(f32)
    feed_gain_part = jnp.sum(normed_three_grad * after_cross * scale_three, 0)
    grad_two = upstream + norm_backward(after_cross, scale_three, feed_gain, normed_three_grad)
    up_two = grad_two.astype(bf16)
    mixed_two = dot(up_two, co, (1, 1)).astype(bf16)
    cq_grad, ck_grad, cv_grad, _ = attend_back(cross_q, cross_k, cross_v, 0.0, cross_valid, MEM_LEN, mixed_two)
    normed_two_grad = dot(cq_grad, cq, (1, 0))
    memory_grad = dot(ck_grad, ck, (1, 0)) + dot(cv_grad, cv, (1, 0))
    cross_part = mp_sum(
        [
            dot(cq_grad, normed_two, (0, 0)),
            dot(ck_grad, memory, (0, 0)),
            dot(cv_grad, memory, (0, 0)),
            dot(cross_mixed, up_two, (0, 0)),
        ]
    )
    cross_sum = reduce_dp(cross_part)
    cross_gain_part = jnp.sum(normed_two_grad * after_self * scale_two, 0)
    grad_one = grad_two + norm_backward(after_self, scale_two, cross_gain, normed_two_grad)
    up_one = grad_one.astype(bf16)
    mixed_one = dot(up_one, so, (1, 1)).astype(bf16)
    sq_grad, sk_grad, sv_grad, score_grad = attend_back(
        self_q, self_k, self_v, self_bias, self_valid, TGT_LEN, mixed_one
    )
    bias_part = jnp.einsum("ehqk,qkb->hb", score_grad, bucket_hot, precision=highest)
    self_part = mp_sum(
        [
            dot(sq_grad, normed_one, (0, 0)),
            dot(sk_grad, normed_one, (0, 0)),
            dot(sv_grad, normed_one, (0, 0)),
            dot(self_mixed, up_one, (0, 0)),
        ]
    )
    self_sum = reduce_dp(self_part)
    normed_one_grad = dot(sq_grad, sq, (1, 0)) + dot(sk_grad, sk, (1, 0)) + dot(sv_grad, sv, (1, 0))
    self_gain_part = jnp.sum(normed_one_grad * stream * scale_one, 0)
    inputs_grad = grad_one + norm_backward(stream, scale_one, self_gain, normed_one_grad)

    heads = bias_table.shape[1]
    bias_blocks = jnp.take(bias_part.reshape(4, heads * BUCKETS), jnp.arange(4) ^ rank, axis=0)
    small = lax.psum(
        jnp.concatenate([self_gain_part, cross_gain_part, feed_gain_part, bias_blocks.reshape(-1)]), ("dp", "mp")
    )
    d = inputs.shape[1]
    bias_all = small[3 * d :].reshape(4, heads, BUCKETS)
    bias_sum = lax.dynamic_slice_in_dim(bias_all, rank, 1, 0)[0].T

    def own(total, m):
        return total[m * width : (m + 1) * width]

    return (
        layer_out,
        inputs_grad,
        memory_grad,
        small[:d],
        own(self_sum, 0).T,
        own(self_sum, 1).T,
        own(self_sum, 2).T,
        own(self_sum, 3),
        bias_sum,
        small[d : 2 * d],
        own(cross_sum, 0).T,
        own(cross_sum, 1).T,
        own(cross_sum, 2).T,
        own(cross_sum, 3),
        small[2 * d : 3 * d],
        feed_sum[:d],
        feed_sum[d:],
    )


def solution(mesh):
    in_specs = (
        P(("dp", "mp"), None),
        P(("dp", "mp"), None),
        P("dp"),
        P("dp"),
        P(),
        P(),
        P(None, "mp"),
        P(None, "mp"),
        P(None, "mp"),
        P("mp", None),
        P(None, "mp"),
        P(),
        P(None, "mp"),
        P(None, "mp"),
        P(None, "mp"),
        P("mp", None),
        P(),
        P(None, "mp"),
        P("mp", None),
        P(("dp", "mp"), None),
    )
    out_specs = (
        P(("dp", "mp"), None),
        P(("dp", "mp"), None),
        P(("dp", "mp"), None),
        P(),
        P(None, "mp"),
        P(None, "mp"),
        P(None, "mp"),
        P("mp", None),
        P(None, "mp"),
        P(),
        P(None, "mp"),
        P(None, "mp"),
        P(None, "mp"),
        P("mp", None),
        P(),
        P(None, "mp"),
        P("mp", None),
    )
    return jax.shard_map(body, mesh=mesh, in_specs=in_specs, out_specs=out_specs, check_vma=False)
```

```python
import functools

import jax
import jax.numpy as jnp
from jax import lax
from jax.experimental import pallas as pl
from jax.experimental.pallas import tpu as pltpu
from jax.sharding import PartitionSpec as P

HEAD_DIM = 64
PAIR = 2 * HEAD_DIM
BUCKETS = 32
TGT_LEN = 128
MEM_LEN = 512

masked_fill = -1000000000.0
epsilon = 1e-06
highest = lax.Precision.HIGHEST
tanh_scale = 0.7978845608
cubic_term = 0.044715
bf16 = jnp.bfloat16
f32 = jnp.float32


def dot_nn(a, b):
    return lax.dot_general(a, b, (((1,), (0,)), ((), ())), preferred_element_type=f32)


def dot_nt(a, b):
    return lax.dot_general(a, b, (((1,), (1,)), ((), ())), preferred_element_type=f32)


def dot_tn(a, b):
    return lax.dot_general(a, b, (((0,), (0,)), ((), ())), preferred_element_type=f32)


def row_scale(hidden):
    return lax.rsqrt(jnp.mean(hidden * hidden, -1, keepdims=True) + epsilon)


def norm_backward(hidden, scale, gain, upstream):
    weighted = gain * upstream
    return scale * weighted - hidden * (scale * scale * scale) * jnp.mean(hidden * weighted, -1, keepdims=True)


def matrix(blocks, index, width):
    return jnp.concatenate([b[index * width : (index + 1) * width, :] for b in blocks], 0)


def store_rows(ref, lead, index, grad, turn):
    blocks = ref.shape[len(lead)]
    size = grad.shape[0] // blocks
    for a in range(blocks):
        ref[(*lead, a ^ turn, index)] = grad[a * size : (a + 1) * size].astype(bf16)


def store_grad(keep_ref, send_ref, index, grad, turn):
    width = grad.shape[0] // 4
    for j in range(4):
        store_rows((keep_ref, send_ref)[j % 2], (j // 2,), index, grad[j * width : (j + 1) * width], turn)


def pair_masks():
    lane = lax.broadcasted_iota(jnp.int32, (1, PAIR), 1)
    return (lane < HEAD_DIM).astype(bf16), (lane >= HEAD_DIM).astype(bf16)


def stack_pair(rows, masks):
    return jnp.concatenate([rows * masks[0], rows * masks[1]], 0)


def unstack_pair(both):
    lane = lax.broadcasted_iota(jnp.int32, (TGT_LEN, PAIR), 1)
    return jnp.where(lane < HEAD_DIM, both[:TGT_LEN], both[TGT_LEN:])


def softmax_rows(scores):
    weights = jnp.exp(scores - jnp.max(scores, -1, keepdims=True))
    return weights * (1.0 / jnp.sum(weights, -1, keepdims=True))


def locate(step, pairs, keys):
    example = lax.div(step, pairs)
    pair = lax.rem(step, pairs)
    rows = pl.ds(pl.multiple_of(example * TGT_LEN, TGT_LEN), TGT_LEN)
    key_rows = pl.ds(pl.multiple_of(example * keys, keys), keys)
    cols = pl.ds(pl.multiple_of(pair * PAIR, PAIR), PAIR)
    return example, pair, rows, key_rows, cols


def cross_probs(queries, key_rows, length):
    scores = dot_nt(queries, key_rows)
    key = lax.broadcasted_iota(jnp.int32, scores.shape, 1)
    return softmax_rows(jnp.where(key < length, scores, masked_fill))


def attend(q_ref, k_ref, v_ref, mixed_ref, keys, probs_of):
    masks = pair_masks()
    pairs = q_ref.shape[1] // PAIR
    examples = q_ref.shape[0] // TGT_LEN

    def step(i, carry):
        example, pair, rows, key_rows, cols = locate(i, pairs, keys)
        probs = probs_of(stack_pair(q_ref[rows, cols], masks), k_ref[key_rows, cols], example, pair)
        mixed = dot_nn(probs.astype(bf16), v_ref[key_rows, cols])
        mixed_ref[rows, cols] = unstack_pair(mixed).astype(bf16)
        return carry

    lax.fori_loop(0, examples * pairs, step, 0, unroll=2)


def attend_back(q_ref, k_ref, v_ref, m_ref, dq_ref, dk_ref, dv_ref, keys, probs_of):
    masks = pair_masks()
    pairs = q_ref.shape[1] // PAIR
    examples = q_ref.shape[0] // TGT_LEN

    def step(i, carry):
        example, pair, rows, key_rows, cols = locate(i, pairs, keys)
        queries = stack_pair(q_ref[rows, cols], masks)
        grads = stack_pair(m_ref[rows, cols], masks)
        key_block = k_ref[key_rows, cols]
        probs = probs_of(queries, key_block, example, pair)
        dv_ref[key_rows, cols] = dot_tn(probs.astype(bf16), grads).astype(bf16)
        prob_grad = dot_nt(grads, v_ref[key_rows, cols])
        score_grad = probs * (prob_grad - jnp.sum(probs * prob_grad, -1, keepdims=True))
        low = score_grad.astype(bf16)
        dq_ref[rows, cols] = unstack_pair(dot_nn(low, key_block)).astype(bf16)
        dk_ref[key_rows, cols] = dot_tn(low, queries).astype(bf16)
        return carry

    lax.fori_loop(0, examples * pairs, step, 0, unroll=UNROLL_BACK)


UNROLL_BACK = 2


def fill_bias(table_ref, bias_ref):
    for head in range(bias_ref.shape[0] // TGT_LEN):
        row = jnp.broadcast_to(table_ref[head : head + 1, :], (TGT_LEN, TGT_LEN))
        bias_ref[head * TGT_LEN : (head + 1) * TGT_LEN, :] = pltpu.roll(row, 0, axis=1, stride=1, stride_axis=0)


def stack_heads(rows):
    lane = lax.broadcasted_iota(jnp.int32, (1, rows.shape[1]), 1)
    heads = rows.shape[1] // HEAD_DIM
    return jnp.concatenate([rows * (lax.div(lane, HEAD_DIM) == h).astype(bf16) for h in range(heads)], 0)


def unstack_heads(stacked):
    length = TGT_LEN
    lane = lax.broadcasted_iota(jnp.int32, (length, stacked.shape[1]), 1)
    out = stacked[:length]
    for h in range(1, stacked.shape[1] // HEAD_DIM):
        out = jnp.where(lane >= h * HEAD_DIM, stacked[h * length : (h + 1) * length], out)
    return out


def self_probs(queries, key_rows, bias, length):
    scores = dot_nt(queries, key_rows) + bias
    key = lax.broadcasted_iota(jnp.int32, scores.shape, 1)
    query = lax.rem(lax.broadcasted_iota(jnp.int32, scores.shape, 0), TGT_LEN)
    return softmax_rows(jnp.where((key <= query) & (key < length), scores, masked_fill))


def diagonal_sums(grad):
    query = lax.broadcasted_iota(jnp.int32, grad.shape, 0)
    for bit in range(TGT_LEN.bit_length() - 1):
        moved = pltpu.roll(grad, TGT_LEN - (1 << bit), axis=1)
        grad = jnp.where((query >> bit) & 1 == 1, moved, grad)
    return jnp.sum(grad, 0, keepdims=True)


def first_norm(x_ref, gain_ref, n_ref):
    hidden = x_ref[...].astype(f32)
    n_ref[...] = (hidden * row_scale(hidden) * gain_ref[...]).astype(bf16)


def store_parts(own_ref, chip_ref, send_ref, parts):
    for j, part in enumerate(parts):
        if j == 0:
            own_ref[...] = part
        elif j == 2:
            chip_ref[...] = part
        else:
            send_ref[j // 2] = part.astype(bf16)


def self_forward(
    n0, n1, n2, n3, wq_ref, wk_ref, wv_ref, wo_ref, table_ref, rank_ref, len_ref,
    q_ref, k_ref, v_ref, mixed_ref, own_ref, chip_ref, send_ref, bias_ref,
):
    fill_bias(table_ref, bias_ref)
    size = n0.shape[0]
    for j, n in enumerate((n0, n1, n2, n3)):
        rows = slice(j * size, (j + 1) * size)
        for ref, w in ((q_ref, wq_ref), (k_ref, wk_ref), (v_ref, wv_ref)):
            ref[rows, :] = dot_nn(n[...], w[...]).astype(bf16)

    def step(i, carry):
        rows = pl.ds(pl.multiple_of(i * TGT_LEN, TGT_LEN), TGT_LEN)
        length = len_ref[(rank_ref[0] * (size // TGT_LEN)) ^ i]
        probs = self_probs(stack_heads(q_ref[rows, :]), k_ref[rows, :], bias_ref[...], length)
        mixed_ref[rows, :] = unstack_heads(dot_nn(probs.astype(bf16), v_ref[rows, :])).astype(bf16)
        return carry

    lax.fori_loop(0, 4 * size // TGT_LEN, step, 0, unroll=2)
    store_parts(
        own_ref, chip_ref, send_ref,
        (dot_nn(mixed_ref[j * size : (j + 1) * size, :], wo_ref[...]) for j in range(4)),
    )


def memory_forward(mem_ref, w0, w1, w2, w3, k_ref, v_ref):
    width = k_ref.shape[1] // 4
    blocks = (w0, w1, w2, w3)
    k_ref[...] = dot_nt(mem_ref[...], matrix(blocks, 0, width)).astype(bf16)
    v_ref[...] = dot_nt(mem_ref[...], matrix(blocks, 1, width)).astype(bf16)


def cross_forward(
    x_ref, near_ref, far_ref, k_ref, v_ref, gain_two_ref, gain_three_ref, w0, w1, w2, w3, len_ref,
    after_self_ref, n2_ref, q_ref, mixed_ref, after_ref, n3_ref,
):
    blocks = (w0, w1, w2, w3)
    width = q_ref.shape[1] // 4
    after_self = x_ref[...].astype(f32) + near_ref[...] + far_ref[...].astype(f32)
    after_self_ref[...] = after_self
    normed = (after_self * row_scale(after_self) * gain_two_ref[...]).astype(bf16)
    n2_ref[...] = normed
    q_ref[...] = dot_nt(normed, matrix(blocks, 0, width)).astype(bf16)

    def probs(queries, key_rows, example, pair):
        return cross_probs(queries, key_rows, len_ref[example])

    attend(q_ref, k_ref, v_ref, mixed_ref, MEM_LEN, probs)
    after = after_self_ref[...] + dot_nn(mixed_ref[...], matrix(blocks, 1, width))
    after_ref[...] = after
    n3_ref[...] = (after * row_scale(after) * gain_three_ref[...]).astype(bf16)


def feed_main(
    g0, g1, g2, g3, c0, c1, c2, c3, in_ref, out_ref, own_ref, chip_ref, send_ref, act_ref, pre_grad_ref
):
    for j, (g, c) in enumerate(zip((g0, g1, g2, g3), (c0, c1, c2, c3))):
        rows = slice(j * g.shape[0], (j + 1) * g.shape[0])
        pre = dot_nn(g[...], in_ref[...])
        hidden_grad = dot_nt(c[...], out_ref[...])
        square = pre * pre
        tanh = jnp.tanh(tanh_scale * (pre + cubic_term * square * pre))
        act_ref[rows, :] = (0.5 * pre * (1.0 + tanh)).astype(bf16)
        slope = 0.5 * (1.0 + tanh) + 0.5 * pre * (1.0 - tanh * tanh) * (
            tanh_scale * (1.0 + 3.0 * cubic_term * square)
        )
        low = (hidden_grad * slope).astype(bf16)
        pre_grad_ref[rows, :] = low
        grad = dot_nt(low, in_ref[...])
        if j == 0:
            own_ref[...] = grad
        elif j == 2:
            chip_ref[...] = grad
        else:
            send_ref[j // 2] = grad.astype(bf16)


def feed_rest(
    g0, g1, g2, g3, c0, c1, c2, c3, act_ref, pre_grad_ref, out_ref, turn_ref, own_ref, chip_ref, send_ref, grads_ref
):
    gathered = jnp.concatenate([g[...] for g in (g0, g1, g2, g3)], 0)
    store_rows(grads_ref, (), 0, dot_tn(gathered, pre_grad_ref[...]), turn_ref[0])
    upstream = jnp.concatenate([c[...] for c in (c0, c1, c2, c3)], 0)
    store_rows(grads_ref, (), 1, dot_tn(act_ref[...], upstream), turn_ref[0])
    for j in range(4):
        rows = slice(j * g0.shape[0], (j + 1) * g0.shape[0])
        part = dot_nn(act_ref[rows, :], out_ref[...])
        if j == 0:
            own_ref[...] = part
        elif j == 2:
            chip_ref[...] = part
        else:
            send_ref[j // 2] = part.astype(bf16)


def cross_backward(
    near_ref, far_ref, cot_ref, after_ref, after_self_ref, gain_two_ref, gain_three_ref,
    n2_ref, q_ref, k_ref, v_ref, mixed_ref, w0, w1, w2, w3, len_ref, turn_ref,
    grad_one_ref, up_ref, dk_ref, dv_ref, gains_ref, keep_ref, send_ref, m_ref, dq_ref,
):
    blocks = (w0, w1, w2, w3)
    width = q_ref.shape[1] // 4
    after = after_ref[...]
    scale = row_scale(after)
    upstream = near_ref[...] + far_ref[...].astype(f32)
    gains_ref[1:2, :] = jnp.sum(upstream * after * scale, 0, keepdims=True)
    grad_two = cot_ref[...].astype(f32) + norm_backward(after, scale, gain_three_ref[...], upstream)
    grad_one_ref[...] = grad_two
    up_two = grad_two.astype(bf16)
    m_ref[...] = dot_nt(up_two, matrix(blocks, 1, width)).astype(bf16)
    store_grad(keep_ref, send_ref, 1, dot_tn(mixed_ref[...], up_two), turn_ref[0])

    def probs(queries, key_rows, example, pair):
        return cross_probs(queries, key_rows, len_ref[example])

    attend_back(q_ref, k_ref, v_ref, m_ref, dq_ref, dk_ref, dv_ref, MEM_LEN, probs)
    store_grad(keep_ref, send_ref, 0, dot_tn(dq_ref[...], n2_ref[...]), turn_ref[0])
    upstream = dot_nn(dq_ref[...], matrix(blocks, 0, width))
    hidden = after_self_ref[...]
    scale = row_scale(hidden)
    gains_ref[0:1, :] = jnp.sum(upstream * hidden * scale, 0, keepdims=True)
    grad_one = grad_one_ref[...] + norm_backward(hidden, scale, gain_two_ref[...], upstream)
    grad_one_ref[...] = grad_one
    up_ref[...] = grad_one.astype(bf16)


def memory_weights(dk_ref, dv_ref, mem_ref, keep_in, send_in, turn_ref, keep_ref, send_ref):
    count = keep_in.shape[2]
    for j in range(2):
        for a in range(keep_in.shape[1]):
            keep_ref[j, a, :count] = keep_in[j, a]
            send_ref[j, a, :count] = send_in[j, a]
    store_grad(keep_ref, send_ref, count, dot_tn(dk_ref[...], mem_ref[...]), turn_ref[0])
    store_grad(keep_ref, send_ref, count + 1, dot_tn(dv_ref[...], mem_ref[...]), turn_ref[0])


def self_backward(
    u0, u1, u2, u3, n0, n1, n2, n3, q_ref, k_ref, v_ref, mixed_ref, wq_ref, wk_ref, wv_ref, wo_ref,
    table_ref, rank_ref, len_ref, turn_ref,
    grads_ref, sums_ref, own_ref, chip_ref, send_ref, bias_ref, score_ref, m_ref, dq_ref, dk_ref, dv_ref,
):
    fill_bias(table_ref, bias_ref)
    score_ref[...] = jnp.zeros_like(score_ref)
    size = n0.shape[0]
    width = q_ref.shape[1]
    for j, u in enumerate((u0, u1, u2, u3)):
        m_ref[j * size : (j + 1) * size, :] = dot_nt(u[...], wo_ref[...]).astype(bf16)

    def step(i, carry):
        rows = pl.ds(pl.multiple_of(i * TGT_LEN, TGT_LEN), TGT_LEN)
        length = len_ref[(rank_ref[0] * (size // TGT_LEN)) ^ i]
        queries = stack_heads(q_ref[rows, :])
        grads = stack_heads(m_ref[rows, :])
        key_block = k_ref[rows, :]
        probs = self_probs(queries, key_block, bias_ref[...], length)
        dv_ref[rows, :] = dot_tn(probs.astype(bf16), grads).astype(bf16)
        prob_grad = dot_nt(grads, v_ref[rows, :])
        score_grad = probs * (prob_grad - jnp.sum(probs * prob_grad, -1, keepdims=True))
        score_ref[...] += score_grad
        low = score_grad.astype(bf16)
        dq_ref[rows, :] = unstack_heads(dot_nn(low, key_block)).astype(bf16)
        dk_ref[rows, :] = dot_tn(low, queries).astype(bf16)
        return carry

    lax.fori_loop(0, 4 * size // TGT_LEN, step, 0, unroll=UNROLL_BACK)
    normed = jnp.concatenate([n[...] for n in (n0, n1, n2, n3)], 0)
    upstream = jnp.concatenate([u[...] for u in (u0, u1, u2, u3)], 0)
    for index, (left, right) in enumerate(
        ((dq_ref[...], normed), (dk_ref[...], normed), (dv_ref[...], normed), (mixed_ref[...], upstream))
    ):
        store_rows(grads_ref, (), index, dot_tn(left, right), turn_ref[0])
    heads = width // HEAD_DIM
    sums = [diagonal_sums(score_ref[h * TGT_LEN : (h + 1) * TGT_LEN, :]) for h in range(heads)]
    sums_ref[:heads, :] = jnp.concatenate(sums, 0)
    sums_ref[heads:, :] = jnp.zeros((sums_ref.shape[0] - heads, TGT_LEN), f32)

    def part(j):
        rows = slice(j * size, (j + 1) * size)
        out = dot_nt(dq_ref[rows, :], wq_ref[...])
        return out + dot_nt(dk_ref[rows, :], wk_ref[...]) + dot_nt(dv_ref[rows, :], wv_ref[...])

    store_parts(own_ref, chip_ref, send_ref, (part(j) for j in range(4)))


def last_norm(grad_one_ref, near_ref, far_ref, x_ref, gain_ref, late_ref, sums_ref, rank_ref, grad_ref, small_ref):
    upstream = near_ref[...] + far_ref[...].astype(f32)
    hidden = x_ref[...].astype(f32)
    scale = row_scale(hidden)
    small_ref[...] = jnp.zeros_like(small_ref)
    small_ref[0:1, :] = jnp.sum(upstream * hidden * scale, 0, keepdims=True)
    small_ref[1:3, :] = late_ref[...]
    for j in range(4):
        here = (rank_ref[0] == j).astype(f32)
        small_ref[8 * (j + 1) : 8 * (j + 2), :TGT_LEN] = sums_ref[...] * here
    grad_ref[...] = grad_one_ref[...] + norm_backward(hidden, scale, gain_ref[...], upstream)


def gather_rows(ref, index, turn):
    return jnp.concatenate([ref[a ^ turn, index].astype(f32) for a in range(ref.shape[0])], 0)


def finish_feed(total_ref, turn_ref, in_ref, out_ref):
    in_ref[...] = gather_rows(total_ref, 0, turn_ref[0])
    out_ref[...] = gather_rows(total_ref, 1, turn_ref[0])


def finish_heads(total_ref, turn_ref, *outs):
    for index, ref in enumerate(outs):
        rows = gather_rows(total_ref, index, turn_ref[0])
        ref[...] = rows if ref.shape == rows.shape else rows.T


def memory_backward(dk_ref, dv_ref, w0, w1, w2, w3, grad_ref):
    blocks = (w0, w1, w2, w3)
    width = dk_ref.shape[1] // 4
    grad_ref[...] = dot_nn(dk_ref[...], matrix(blocks, 0, width)) + dot_nn(dv_ref[...], matrix(blocks, 1, width))


def call(kernel, operands, outs, scratch=(), flops=0, smem=()):
    moved = sum(a.size * a.dtype.itemsize for a in operands)
    moved += sum(functools.reduce(lambda x, y: x * y, s) * jnp.dtype(t).itemsize for s, t in outs)
    return pl.pallas_call(
        kernel,
        out_shape=[jax.ShapeDtypeStruct(s, t) for s, t in outs],
        in_specs=[
            pl.BlockSpec(memory_space=pltpu.SMEM if i in smem else pltpu.VMEM) for i in range(len(operands))
        ],
        out_specs=[pl.BlockSpec(memory_space=pltpu.VMEM) for _ in outs],
        scratch_shapes=[pltpu.VMEM(s, t) for s, t in scratch],
        compiler_params=pltpu.CompilerParams(vmem_limit_bytes=VMEM_LIMIT),
        cost_estimate=pl.CostEstimate(flops=flops, bytes_accessed=moved, transcendentals=0),
    )(*operands)


VMEM_LIMIT = 56 * 1024 * 1024


def after(value, *others):
    return lax.optimization_barrier((value, *others))[0]


def swap_core(a):
    return lax.ppermute(a, "mp", [(0, 1), (1, 0), (2, 3), (3, 2)])


def swap_chip(a):
    return lax.ppermute(a, "mp", [(0, 2), (2, 0), (1, 3), (3, 1)])


def gather_blocks(a):
    far = swap_chip(a)
    return (a, swap_core(a), far, swap_core(far))


def core_sum(own, chip, send):
    got = swap_core(send)
    return own.astype(f32) + got[0].astype(f32), (chip.astype(f32) + got[1].astype(f32)).astype(bf16)


def dp_chain(value):
    size = lax.axis_size("dp")
    bits = range(size.bit_length() - 1)
    keep, send = value[: size // 2], value[size // 2 :]
    for bit in bits:
        pairs = [(i, i ^ (1 << bit)) for i in range(size)]
        got = lax.ppermute(send, "dp", pairs)
        token = yield send
        got = after(got, token)
        half = keep.shape[0] // 2
        if half:
            send = (keep[half:].astype(f32) + got[half:].astype(f32)).astype(bf16)
            keep = (keep[:half].astype(f32) + got[:half].astype(f32)).astype(bf16)
        else:
            value = (keep.astype(f32) + got.astype(f32)).astype(bf16)
    for bit in reversed(bits):
        pairs = [(i, i ^ (1 << bit)) for i in range(size)]
        other = lax.ppermute(value, "dp", pairs)
        token = yield value
        value = jnp.concatenate([value, after(other, token)], 0)
    yield value


def sum_all(value):
    steps = [("mp", 1), ("mp", 2)] + [("dp", 1 << bit) for bit in range(lax.axis_size("dp").bit_length() - 1)]
    for axis, flip in steps:
        pairs = [(i, i ^ flip) for i in range(lax.axis_size(axis))]
        got = lax.ppermute(value, axis, pairs)
        token = yield value
        value = value + after(got, token)
    yield value


def next_step(chain, token, first=False):
    try:
        return next(chain) if first else chain.send(token)
    except StopIteration:
        return None


def body(
    inputs,
    memory,
    target_len,
    memory_len,
    bucket_map,
    self_gain,
    self_query,
    self_key,
    self_value,
    self_out,
    bias_table,
    cross_gain,
    cross_query,
    cross_key,
    cross_value,
    cross_out,
    feed_gain,
    feed_input,
    feed_output,
    cotangent,
):
    rank = lax.axis_index("mp")
    rows, d = inputs.shape
    key_rows = memory.shape[0]
    width = self_query.shape[1]
    wide = 4 * width
    heads = bias_table.shape[1]
    units = feed_input.shape[1]
    examples = rows // TGT_LEN
    rank_value = rank.astype(jnp.int32).reshape(1)
    blocks = lax.axis_size("dp")
    place = lax.axis_index("dp").astype(jnp.int32)
    turn = jnp.zeros((1,), jnp.int32)
    for bit in range(blocks.bit_length() - 1):
        turn = 2 * turn + ((place >> bit) & 1)
    memory_len = lax.dynamic_slice_in_dim(memory_len, rank * examples, examples, 0)
    gain_one, gain_two, gain_three = self_gain[None], cross_gain[None], feed_gain[None]

    distance = (TGT_LEN - jnp.arange(TGT_LEN, dtype=jnp.int32)) % TGT_LEN
    lookup = distance[:, None] == jnp.arange(TGT_LEN, dtype=jnp.int32)[None, :]
    bucket = jnp.sum(jnp.where(lookup, bucket_map[None, :], 0), -1)
    hot = (bucket[:, None] == jnp.arange(BUCKETS, dtype=jnp.int32)[None, :]).astype(f32)
    by_distance = lax.dot_general(bias_table, hot, (((0,), (1,)), ((), ())), precision=highest)
    big = (rows, d)
    head_rows = (rows, wide)
    key_heads = (key_rows, wide)
    square = ((heads * TGT_LEN, TGT_LEN), f32)
    group_heads = (4 * rows, width)
    pack = ((2, rows, d), bf16)
    product = 2 * rows * d * wide

    def grad_rows(count, size, lead=()):
        return ((*lead, blocks, count, size // blocks, d), bf16)

    second_own = jnp.concatenate([cross_key.T, cross_value.T], 0)
    third_own = jnp.concatenate([cross_query.T, cross_out], 0)
    normed_one = call(first_norm, (inputs, gain_one), [(big, bf16)])[0]
    ones = gather_blocks(normed_one)
    second_far = swap_chip(after(second_own, ones[2]))
    self_q, self_k, self_v, self_mixed, near, chip, send = call(
        self_forward,
        (*ones, self_query, self_key, self_value, self_out, by_distance, rank_value, target_len),
        [(group_heads, bf16)] * 4 + [(big, f32), (big, f32), pack],
        [square],
        flops=4 * product,
        smem=(9, 10),
    )
    second_far = after(second_far, self_mixed)
    third_far = swap_chip(after(third_own, second_far))
    near, far_send = core_sum(near, chip, send)
    far = swap_chip(far_send)
    second = (second_own, swap_core(second_own), second_far, swap_core(second_far))
    cross_k, cross_v = call(
        memory_forward, (after(memory, far_send), *second), [(key_heads, bf16)] * 2, flops=8 * product
    )
    third_far = after(third_far, cross_v)
    third = (third_own, swap_core(third_own), third_far, swap_core(third_far))
    far = after(far, third_far)
    ups_far = swap_chip(after(cotangent, far))
    after_self, normed_two, cross_q, cross_mixed, after_cross, normed_three = call(
        cross_forward,
        (inputs, near, far, cross_k, cross_v, gain_two, gain_three, *third, memory_len),
        [(big, f32), (big, bf16), (head_rows, bf16), (head_rows, bf16), (big, f32), (big, bf16)],
        flops=6 * product,
        smem=(11,),
    )
    ups_far = after(ups_far, normed_three)
    ups = (cotangent, swap_core(cotangent), ups_far, swap_core(ups_far))
    gathered = gather_blocks(normed_three)
    many = 4 * rows
    near, chip, send, activated, pre_grad = call(
        feed_main,
        (*gathered, *ups, feed_input, feed_output),
        [(big, f32), (big, f32), pack, ((many, units), bf16), ((many, units), bf16)],
        flops=12 * product,
    )
    near, far_send = core_sum(near, chip, send)
    far = swap_chip(far_send)
    out_near, out_chip, out_send, feed_part = call(
        feed_rest,
        (*gathered, *ups, after(activated, far_send), pre_grad, feed_output, turn),
        [(big, f32), (big, f32), pack, grad_rows(2, d)],
        flops=12 * product,
        smem=(11,),
    )
    zero = dp_chain(feed_part)
    token = next(zero)
    far = after(far, token)
    grad_one, up_one, key_grad, value_grad, late_gains, keep, send = call(
        cross_backward,
        (near, far, cotangent, after_cross, after_self, gain_two, gain_three)
        + (normed_two, cross_q, cross_k, cross_v, cross_mixed, *third, memory_len, turn),
        [(big, f32), (big, bf16), (key_heads, bf16), (key_heads, bf16), ((2, d), f32)] + [grad_rows(2, width, (2,))] * 2,
        [(head_rows, bf16), (head_rows, bf16)],
        flops=16 * product,
        smem=(16, 17),
    )
    up_far = swap_chip(up_one)
    keep, send = call(
        memory_weights,
        (key_grad, value_grad, memory, keep, send, turn),
        [grad_rows(4, width, (2,))] * 2,
        flops=8 * product,
        smem=(5,),
    )
    up_far = after(up_far, keep)
    token = zero.send(up_far)
    one_near, one_send = core_sum(keep[0], keep[1], after(send, token))
    one_far = swap_chip(one_send)
    self_ups = (up_one, swap_core(up_one), after(up_far, one_send), swap_core(up_far))
    grads, sums, near, chip, send = call(
        self_backward,
        (*self_ups, *ones, self_q, self_k, self_v, self_mixed)
        + (self_query, self_key, self_value, self_out, by_distance, rank_value, target_len, turn),
        [grad_rows(4, width), ((8, TGT_LEN), f32), (big, f32), (big, f32), pack],
        [square, square] + [(group_heads, bf16)] * 4,
        flops=10 * product,
        smem=(17, 18, 19),
    )
    token = zero.send(sums)
    two = dp_chain(after(grads, token))
    two_token = next(two)
    near, far_send = core_sum(near, chip, after(send, two_token))
    far = swap_chip(far_send)
    memory_grad = call(
        memory_backward,
        (after(key_grad, far_send), value_grad, *second),
        [((key_rows, d), f32)],
        flops=8 * product,
    )[0]
    token = zero.send(memory_grad)
    one = dp_chain((one_near + after(one_far, token).astype(f32)).astype(bf16))
    token = next(one)
    token = two.send(token)
    inputs_grad, small = call(
        last_norm,
        (grad_one, near, after(far, token), inputs, gain_one, late_gains, sums, rank_value),
        [(big, f32), ((40, d), f32)],
        smem=(7,),
    )
    small = sum_all(small)
    token = next_step(small, inputs_grad, True)
    out_near, out_send = core_sum(out_near, out_chip, after(out_send, token))
    out_far = swap_chip(out_send)
    total = {}
    waiting = [(zero, "zero"), (one, "one"), (two, "two"), (small, "small")]
    while waiting:
        still = []
        for chain, name in waiting:
            step = next_step(chain, token)
            if step is None:
                continue
            token = total[name] = step
            still.append((chain, name))
        waiting = still
    layer_out = (after_cross + out_near + out_far.astype(f32)).astype(bf16)
    feed_in_grad, feed_out_grad = call(
        finish_feed, (total["zero"], turn), [((d, units), f32), ((units, d), f32)], smem=(1,)
    )
    column, row = ((d, width), f32), ((width, d), f32)
    cross_grads = call(finish_heads, (total["one"], turn), [column, row, column, column], smem=(1,))
    self_grads = call(finish_heads, (total["two"], turn), [column, column, column, row], smem=(1,))
    gains = total["small"][:3]
    own_sums = lax.dynamic_slice(total["small"], (8 * (rank + 1), 0), (heads, TGT_LEN))
    bias_grad = lax.dot_general(hot, own_sums, (((0,), (1,)), ((), ())), precision=highest)

    return (
        layer_out,
        inputs_grad,
        memory_grad,
        gains[0],
        self_grads[0],
        self_grads[1],
        self_grads[2],
        self_grads[3],
        bias_grad,
        gains[1],
        cross_grads[0],
        cross_grads[2],
        cross_grads[3],
        cross_grads[1],
        gains[2],
        feed_in_grad,
        feed_out_grad,
    )


def solution(mesh):
    in_specs = (
        P(("dp", "mp"), None),
        P(("dp", "mp"), None),
        P("dp"),
        P("dp"),
        P(),
        P(),
        P(None, "mp"),
        P(None, "mp"),
        P(None, "mp"),
        P("mp", None),
        P(None, "mp"),
        P(),
        P(None, "mp"),
        P(None, "mp"),
        P(None, "mp"),
        P("mp", None),
        P(),
        P(None, "mp"),
        P("mp", None),
        P(("dp", "mp"), None),
    )
    out_specs = (
        P(("dp", "mp"), None),
        P(("dp", "mp"), None),
        P(("dp", "mp"), None),
        P(),
        P(None, "mp"),
        P(None, "mp"),
        P(None, "mp"),
        P("mp", None),
        P(None, "mp"),
        P(),
        P(None, "mp"),
        P(None, "mp"),
        P(None, "mp"),
        P("mp", None),
        P(),
        P(None, "mp"),
        P("mp", None),
    )
    return jax.shard_map(body, mesh=mesh, in_specs=in_specs, out_specs=out_specs, check_vma=False)
```

```python
import functools

import jax
import jax.numpy as jnp
from jax import lax
from jax.experimental import pallas as pl
from jax.experimental.pallas import tpu as pltpu
from jax.sharding import PartitionSpec as P

HEAD_DIM = 64
PAIR = 2 * HEAD_DIM
BUCKETS = 32
TGT_LEN = 128
MEM_LEN = 512

masked_fill = -1000000000.0
epsilon = 1e-06
highest = lax.Precision.HIGHEST
tanh_scale = 0.7978845608
cubic_term = 0.044715
bf16 = jnp.bfloat16
f32 = jnp.float32


def dot_nn(a, b):
    return lax.dot_general(a, b, (((1,), (0,)), ((), ())), preferred_element_type=f32)


def dot_nt(a, b):
    return lax.dot_general(a, b, (((1,), (1,)), ((), ())), preferred_element_type=f32)


def dot_tn(a, b):
    return lax.dot_general(a, b, (((0,), (0,)), ((), ())), preferred_element_type=f32)


def row_scale(hidden):
    return lax.rsqrt(jnp.mean(hidden * hidden, -1, keepdims=True) + epsilon)


def norm_backward(hidden, scale, gain, upstream):
    weighted = gain * upstream
    return scale * weighted - hidden * (scale * scale * scale) * jnp.mean(hidden * weighted, -1, keepdims=True)


def matrix(blocks, index, width):
    return jnp.concatenate([b[index * width : (index + 1) * width, :] for b in blocks], 0)


def store_rows(ref, lead, index, grad, turn):
    blocks = ref.shape[len(lead)]
    size = grad.shape[0] // blocks
    for a in range(blocks):
        ref[(*lead, a ^ turn, index)] = grad[a * size : (a + 1) * size].astype(bf16)


def store_halves(low_ref, high_ref, ref):
    half = ref.shape[0] // 2
    low_ref[...] = ref[:half]
    high_ref[...] = ref[half:]


def store_grad(keep_ref, send_ref, index, grad, turn):
    width = grad.shape[0] // 4
    for j in range(4):
        store_rows((keep_ref, send_ref)[j % 2], (j // 2,), index, grad[j * width : (j + 1) * width], turn)


def pair_masks():
    lane = lax.broadcasted_iota(jnp.int32, (1, PAIR), 1)
    return (lane < HEAD_DIM).astype(bf16), (lane >= HEAD_DIM).astype(bf16)


def stack_pair(rows, masks):
    return jnp.concatenate([rows * masks[0], rows * masks[1]], 0)


def unstack_pair(both):
    lane = lax.broadcasted_iota(jnp.int32, (TGT_LEN, PAIR), 1)
    return jnp.where(lane < HEAD_DIM, both[:TGT_LEN], both[TGT_LEN:])


def softmax_rows(scores):
    weights = jnp.exp(scores - jnp.max(scores, -1, keepdims=True))
    return weights * (1.0 / jnp.sum(weights, -1, keepdims=True))


def locate(step, pairs, keys):
    example = lax.div(step, pairs)
    pair = lax.rem(step, pairs)
    rows = pl.ds(pl.multiple_of(example * TGT_LEN, TGT_LEN), TGT_LEN)
    key_rows = pl.ds(pl.multiple_of(example * keys, keys), keys)
    cols = pl.ds(pl.multiple_of(pair * PAIR, PAIR), PAIR)
    return example, pair, rows, key_rows, cols


def cross_probs(queries, key_rows, length):
    scores = dot_nt(queries, key_rows)
    key = lax.broadcasted_iota(jnp.int32, scores.shape, 1)
    return softmax_rows(jnp.where(key < length, scores, masked_fill))


def attend(q_ref, k_ref, v_ref, mixed_ref, keys, probs_of):
    masks = pair_masks()
    pairs = q_ref.shape[1] // PAIR
    examples = q_ref.shape[0] // TGT_LEN

    def step(i, carry):
        example, pair, rows, key_rows, cols = locate(i, pairs, keys)
        probs = probs_of(stack_pair(q_ref[rows, cols], masks), k_ref[key_rows, cols], example, pair)
        mixed = dot_nn(probs.astype(bf16), v_ref[key_rows, cols])
        mixed_ref[rows, cols] = unstack_pair(mixed).astype(bf16)
        return carry

    lax.fori_loop(0, examples * pairs, step, 0, unroll=2)


def attend_back(q_ref, k_ref, v_ref, m_ref, dq_ref, dk_ref, dv_ref, keys, probs_of):
    masks = pair_masks()
    pairs = q_ref.shape[1] // PAIR
    examples = q_ref.shape[0] // TGT_LEN

    def step(i, carry):
        example, pair, rows, key_rows, cols = locate(i, pairs, keys)
        queries = stack_pair(q_ref[rows, cols], masks)
        grads = stack_pair(m_ref[rows, cols], masks)
        key_block = k_ref[key_rows, cols]
        probs = probs_of(queries, key_block, example, pair)
        dv_ref[cols, key_rows] = dot_tn(grads, probs.astype(bf16)).astype(bf16)
        prob_grad = dot_nt(grads, v_ref[key_rows, cols])
        score_grad = probs * (prob_grad - jnp.sum(probs * prob_grad, -1, keepdims=True))
        low = score_grad.astype(bf16)
        dq_ref[rows, cols] = unstack_pair(dot_nn(low, key_block)).astype(bf16)
        dk_ref[cols, key_rows] = dot_tn(queries, low).astype(bf16)
        return carry

    lax.fori_loop(0, examples * pairs, step, 0, unroll=UNROLL_BACK)


UNROLL_BACK = 2


def fill_bias(table_ref, bias_ref):
    for head in range(bias_ref.shape[0] // TGT_LEN):
        row = jnp.broadcast_to(table_ref[head : head + 1, :], (TGT_LEN, TGT_LEN))
        bias_ref[head * TGT_LEN : (head + 1) * TGT_LEN, :] = pltpu.roll(row, 0, axis=1, stride=1, stride_axis=0)


def stack_heads(rows):
    lane = lax.broadcasted_iota(jnp.int32, (1, rows.shape[1]), 1)
    heads = rows.shape[1] // HEAD_DIM
    return jnp.concatenate([rows * (lax.div(lane, HEAD_DIM) == h).astype(bf16) for h in range(heads)], 0)


def unstack_heads(stacked):
    length = TGT_LEN
    lane = lax.broadcasted_iota(jnp.int32, (length, stacked.shape[1]), 1)
    out = stacked[:length]
    for h in range(1, stacked.shape[1] // HEAD_DIM):
        out = jnp.where(lane >= h * HEAD_DIM, stacked[h * length : (h + 1) * length], out)
    return out


def self_probs(queries, key_rows, bias, length):
    scores = dot_nt(queries, key_rows) + bias
    key = lax.broadcasted_iota(jnp.int32, scores.shape, 1)
    query = lax.rem(lax.broadcasted_iota(jnp.int32, scores.shape, 0), TGT_LEN)
    return softmax_rows(jnp.where((key <= query) & (key < length), scores, masked_fill))


def diagonal_sums(grad):
    query = lax.broadcasted_iota(jnp.int32, grad.shape, 0)
    for bit in range(TGT_LEN.bit_length() - 1):
        moved = pltpu.roll(grad, TGT_LEN - (1 << bit), axis=1)
        grad = jnp.where((query >> bit) & 1 == 1, moved, grad)
    return jnp.sum(grad, 0, keepdims=True)


def first_norm(x_ref, gain_ref, n_ref):
    hidden = x_ref[...].astype(f32)
    n_ref[...] = (hidden * row_scale(hidden) * gain_ref[...].reshape(1, -1)).astype(bf16)


def store_parts(own_ref, chip_ref, send_ref, parts):
    for j, part in enumerate(parts):
        if j == 0:
            own_ref[...] = part
        elif j == 2:
            chip_ref[...] = part
        else:
            send_ref[j // 2] = part.astype(bf16)


def self_forward(
    n0, n1, n2, n3, wq_ref, wk_ref, wv_ref, wo_ref, table_ref, rank_ref, len_ref,
    q_ref, k_ref, v_ref, mixed_ref, own_ref, chip_ref, send_ref, bias_ref,
):
    fill_bias(table_ref, bias_ref)
    size = n0.shape[0]
    for j, n in enumerate((n0, n1, n2, n3)):
        rows = slice(j * size, (j + 1) * size)
        for ref, w in ((q_ref, wq_ref), (k_ref, wk_ref), (v_ref, wv_ref)):
            ref[rows, :] = dot_nt(n[...], w[...]).astype(bf16)

    def step(i, carry):
        rows = pl.ds(pl.multiple_of(i * TGT_LEN, TGT_LEN), TGT_LEN)
        length = len_ref[(rank_ref[0] * (size // TGT_LEN)) ^ i]
        probs = self_probs(stack_heads(q_ref[rows, :]), k_ref[rows, :], bias_ref[...], length)
        mixed_ref[rows, :] = unstack_heads(dot_nn(probs.astype(bf16), v_ref[rows, :])).astype(bf16)
        return carry

    lax.fori_loop(0, 4 * size // TGT_LEN, step, 0, unroll=2)
    store_parts(
        own_ref, chip_ref, send_ref,
        (dot_nn(mixed_ref[j * size : (j + 1) * size, :], wo_ref[...]) for j in range(4)),
    )


def memory_forward(mem_ref, w0, w1, w2, w3, k_ref, v_ref):
    width = k_ref.shape[1] // 4
    blocks = (w0, w1, w2, w3)
    k_ref[...] = dot_nt(mem_ref[...], matrix(blocks, 2, width)).astype(bf16)
    v_ref[...] = dot_nt(mem_ref[...], matrix(blocks, 3, width)).astype(bf16)


def cross_forward(
    x_ref, own_ref, near_ref, far_ref, k_ref, v_ref, gain_two_ref, gain_three_ref, w0, w1, w2, w3, rank_ref, len_ref,
    after_self_ref, n2_ref, q_ref, mixed_ref, after_ref, n3_ref,
):
    blocks = (w0, w1, w2, w3)
    width = q_ref.shape[1] // 4
    after_self = x_ref[...].astype(f32) + own_ref[...] + near_ref[0].astype(f32) + far_ref[...].astype(f32)
    after_self_ref[...] = after_self
    normed = (after_self * row_scale(after_self) * gain_two_ref[...].reshape(1, -1)).astype(bf16)
    n2_ref[...] = normed
    q_ref[...] = dot_nt(normed, matrix(blocks, 0, width)).astype(bf16)

    def probs(queries, key_rows, example, pair):
        return cross_probs(queries, key_rows, len_ref[rank_ref[0] * (q_ref.shape[0] // TGT_LEN) + example])

    attend(q_ref, k_ref, v_ref, mixed_ref, MEM_LEN, probs)
    after = after_self_ref[...] + dot_nn(mixed_ref[...], matrix(blocks, 1, width))
    after_ref[...] = after
    n3_ref[...] = (after * row_scale(after) * gain_three_ref[...].reshape(1, -1)).astype(bf16)


def feed_hidden(c0, c1, c2, c3, out_ref, hidden_ref):
    for j, c in enumerate((c0, c1, c2, c3)):
        hidden_ref[j * c.shape[0] : (j + 1) * c.shape[0], :] = dot_nt(c[...], out_ref[...])


def feed_main(g0, g1, g2, g3, hidden_ref, in_ref, own_ref, chip_ref, send_ref, act_ref, pre_grad_ref):
    def part(j, g):
        rows = slice(j * g.shape[0], (j + 1) * g.shape[0])
        pre = dot_nn(g[...], in_ref[...])
        square = pre * pre
        tanh = jnp.tanh(tanh_scale * (pre + cubic_term * square * pre))
        act_ref[rows, :] = (0.5 * pre * (1.0 + tanh)).astype(bf16)
        slope = 0.5 * (1.0 + tanh) + 0.5 * pre * (1.0 - tanh * tanh) * (
            tanh_scale * (1.0 + 3.0 * cubic_term * square)
        )
        low = (hidden_ref[rows, :] * slope).astype(bf16)
        pre_grad_ref[rows, :] = low
        return dot_nt(low, in_ref[...])

    store_parts(own_ref, chip_ref, send_ref, (part(j, g) for j, g in enumerate((g0, g1, g2, g3))))


def feed_rest(
    g0, g1, g2, g3, c0, c1, c2, c3, act_ref, pre_grad_ref, out_ref, turn_ref, own_ref, chip_ref, send_ref, low_ref, high_ref, grads_ref
):
    gathered = jnp.concatenate([g[...] for g in (g0, g1, g2, g3)], 0)
    store_rows(grads_ref, (), 0, dot_tn(gathered, pre_grad_ref[...]), turn_ref[0])
    upstream = jnp.concatenate([c[...] for c in (c0, c1, c2, c3)], 0)
    store_rows(grads_ref, (), 1, dot_tn(act_ref[...], upstream), turn_ref[0])
    store_halves(low_ref, high_ref, grads_ref)
    for j in range(4):
        rows = slice(j * g0.shape[0], (j + 1) * g0.shape[0])
        part = dot_nn(act_ref[rows, :], out_ref[...])
        if j == 0:
            own_ref[...] = part
        elif j == 2:
            chip_ref[...] = part
        else:
            send_ref[j // 2] = part.astype(bf16)


def cross_backward(
    own_ref, near_ref, far_ref, cot_ref, after_ref, after_self_ref, gain_two_ref, gain_three_ref,
    n2_ref, q_ref, k_ref, v_ref, mixed_ref, w0, w1, w2, w3, rank_ref, len_ref, turn_ref,
    grad_one_ref, up_ref, dk_ref, dv_ref, gains_ref, keep_ref, send_ref, m_ref, dq_ref,
):
    blocks = (w0, w1, w2, w3)
    width = q_ref.shape[1] // 4
    after = after_ref[...]
    scale = row_scale(after)
    upstream = own_ref[...] + near_ref[0].astype(f32) + far_ref[...].astype(f32)
    gains_ref[1:2, :] = jnp.sum(upstream * after * scale, 0, keepdims=True)
    grad_two = cot_ref[...].astype(f32) + norm_backward(after, scale, gain_three_ref[...].reshape(1, -1), upstream)
    grad_one_ref[...] = grad_two
    up_two = grad_two.astype(bf16)
    m_ref[...] = dot_nt(up_two, matrix(blocks, 1, width)).astype(bf16)
    store_grad(keep_ref, send_ref, 1, dot_tn(mixed_ref[...], up_two), turn_ref[0])

    def probs(queries, key_rows, example, pair):
        return cross_probs(queries, key_rows, len_ref[rank_ref[0] * (q_ref.shape[0] // TGT_LEN) + example])

    attend_back(q_ref, k_ref, v_ref, m_ref, dq_ref, dk_ref, dv_ref, MEM_LEN, probs)
    store_grad(keep_ref, send_ref, 0, dot_tn(dq_ref[...], n2_ref[...]), turn_ref[0])
    upstream = dot_nn(dq_ref[...], matrix(blocks, 0, width))
    hidden = after_self_ref[...]
    scale = row_scale(hidden)
    gains_ref[0:1, :] = jnp.sum(upstream * hidden * scale, 0, keepdims=True)
    grad_one = grad_one_ref[...] + norm_backward(hidden, scale, gain_two_ref[...].reshape(1, -1), upstream)
    grad_one_ref[...] = grad_one
    up_ref[...] = grad_one.astype(bf16)


def memory_weights(dk_ref, dv_ref, mem_ref, keep_in, send_in, turn_ref, keep_ref, send_ref):
    count = keep_in.shape[2]
    for j in range(2):
        for a in range(keep_in.shape[1]):
            keep_ref[j, a, :count] = keep_in[j, a]
            send_ref[j, a, :count] = send_in[j, a]
    store_grad(keep_ref, send_ref, count, dot_nn(dk_ref[...], mem_ref[...]), turn_ref[0])
    store_grad(keep_ref, send_ref, count + 1, dot_nn(dv_ref[...], mem_ref[...]), turn_ref[0])


def self_backward(
    u0, u1, u2, u3, n0, n1, n2, n3, q_ref, k_ref, v_ref, mixed_ref, wq_ref, wk_ref, wv_ref, wo_ref,
    table_ref, rank_ref, len_ref, turn_ref,
    low_ref, high_ref, sums_ref, own_ref, chip_ref, send_ref,
    bias_ref, score_ref, m_ref, dq_ref, dk_ref, dv_ref, grads_ref,
):
    fill_bias(table_ref, bias_ref)
    score_ref[...] = jnp.zeros_like(score_ref)
    size = n0.shape[0]
    width = q_ref.shape[1]
    for j, u in enumerate((u0, u1, u2, u3)):
        m_ref[j * size : (j + 1) * size, :] = dot_nt(u[...], wo_ref[...]).astype(bf16)

    def step(i, carry):
        rows = pl.ds(pl.multiple_of(i * TGT_LEN, TGT_LEN), TGT_LEN)
        length = len_ref[(rank_ref[0] * (size // TGT_LEN)) ^ i]
        queries = stack_heads(q_ref[rows, :])
        grads = stack_heads(m_ref[rows, :])
        key_block = k_ref[rows, :]
        probs = self_probs(queries, key_block, bias_ref[...], length)
        dv_ref[rows, :] = dot_tn(probs.astype(bf16), grads).astype(bf16)
        prob_grad = dot_nt(grads, v_ref[rows, :])
        score_grad = probs * (prob_grad - jnp.sum(probs * prob_grad, -1, keepdims=True))
        score_ref[...] += score_grad
        low = score_grad.astype(bf16)
        dq_ref[rows, :] = unstack_heads(dot_nn(low, key_block)).astype(bf16)
        dk_ref[rows, :] = dot_tn(low, queries).astype(bf16)
        return carry

    lax.fori_loop(0, 4 * size // TGT_LEN, step, 0, unroll=UNROLL_BACK)
    normed = jnp.concatenate([n[...] for n in (n0, n1, n2, n3)], 0)
    upstream = jnp.concatenate([u[...] for u in (u0, u1, u2, u3)], 0)
    for index, (left, right) in enumerate(
        ((dq_ref[...], normed), (dk_ref[...], normed), (dv_ref[...], normed), (mixed_ref[...], upstream))
    ):
        store_rows(grads_ref, (), index, dot_tn(left, right), turn_ref[0])
    store_halves(low_ref, high_ref, grads_ref)
    heads = width // HEAD_DIM
    sums = [diagonal_sums(score_ref[h * TGT_LEN : (h + 1) * TGT_LEN, :]) for h in range(heads)]
    sums_ref[:heads, :] = jnp.concatenate(sums, 0)
    sums_ref[heads:, :] = jnp.zeros((sums_ref.shape[0] - heads, TGT_LEN), f32)

    def part(j):
        rows = slice(j * size, (j + 1) * size)
        out = dot_nn(dq_ref[rows, :], wq_ref[...])
        return out + dot_nn(dk_ref[rows, :], wk_ref[...]) + dot_nn(dv_ref[rows, :], wv_ref[...])

    store_parts(own_ref, chip_ref, send_ref, (part(j) for j in range(4)))


def last_norm(grad_one_ref, own_ref, near_ref, far_ref, x_ref, gain_ref, late_ref, sums_ref, rank_ref, grad_ref, small_ref):
    upstream = own_ref[...] + near_ref[0].astype(f32) + far_ref[...].astype(f32)
    hidden = x_ref[...].astype(f32)
    scale = row_scale(hidden)
    small_ref[...] = jnp.zeros_like(small_ref)
    small_ref[0:1, :] = jnp.sum(upstream * hidden * scale, 0, keepdims=True)
    small_ref[1:3, :] = late_ref[...]
    for j in range(4):
        here = (rank_ref[0] == j).astype(f32)
        small_ref[8 * (j + 1) : 8 * (j + 2), :TGT_LEN] = sums_ref[...] * here
    grad_ref[...] = grad_one_ref[...] + norm_backward(hidden, scale, gain_ref[...].reshape(1, -1), upstream)


def gather_rows(low_ref, high_ref, index, turn):
    half = low_ref.shape[0]
    pieces = []
    for a in range(2 * half):
        place = a ^ turn
        inside = lax.rem(place, half)
        pieces.append(jnp.where(place < half, low_ref[inside, index].astype(f32), high_ref[inside, index].astype(f32)))
    return jnp.concatenate(pieces, 0)


def finish(low_ref, high_ref, turn_ref, *outs):
    for index, ref in enumerate(outs):
        ref[...] = gather_rows(low_ref, high_ref, index, turn_ref[0])


def memory_backward(dk_ref, dv_ref, w0, w1, w2, w3, grad_ref):
    blocks = (w0, w1, w2, w3)
    width = dk_ref.shape[0] // 4
    grad_ref[...] = dot_tn(dk_ref[...], matrix(blocks, 2, width)) + dot_tn(dv_ref[...], matrix(blocks, 3, width))


def call(kernel, operands, outs, scratch=(), flops=0, smem=()):
    moved = sum(a.size * a.dtype.itemsize for a in operands)
    moved += sum(functools.reduce(lambda x, y: x * y, s) * jnp.dtype(t).itemsize for s, t in outs)
    return pl.pallas_call(
        kernel,
        out_shape=[jax.ShapeDtypeStruct(s, t) for s, t in outs],
        in_specs=[
            pl.BlockSpec(memory_space=pltpu.SMEM if i in smem else pltpu.VMEM) for i in range(len(operands))
        ],
        out_specs=[pl.BlockSpec(memory_space=pltpu.VMEM) for _ in outs],
        scratch_shapes=[pltpu.VMEM(s, t) for s, t in scratch],
        compiler_params=pltpu.CompilerParams(vmem_limit_bytes=VMEM_LIMIT),
        cost_estimate=pl.CostEstimate(flops=flops, bytes_accessed=moved, transcendentals=0),
    )(*operands)


VMEM_LIMIT = 56 * 1024 * 1024


def after(value, *others):
    return lax.optimization_barrier((value, *others))[0]


def swap_core(a):
    return lax.ppermute(a, "mp", [(0, 1), (1, 0), (2, 3), (3, 2)])


def swap_chip(a):
    return lax.ppermute(a, "mp", [(0, 2), (2, 0), (1, 3), (3, 1)])


def gather_blocks(a):
    far = swap_chip(a)
    return (a, swap_core(a), far, swap_core(far))


def core_sum(chip, send):
    got = swap_core(send)
    return got, (chip.astype(f32) + got[1].astype(f32)).astype(bf16)


def dp_chain(keep, send):
    size = lax.axis_size("dp")
    bits = range(size.bit_length() - 1)
    for bit in bits:
        pairs = [(i, i ^ (1 << bit)) for i in range(size)]
        got = lax.ppermute(send, "dp", pairs)
        token = yield send
        got = after(got, token)
        half = keep.shape[0] // 2
        if half:
            send = (keep[half:].astype(f32) + got[half:].astype(f32)).astype(bf16)
            keep = (keep[:half].astype(f32) + got[:half].astype(f32)).astype(bf16)
        else:
            value = (keep.astype(f32) + got.astype(f32)).astype(bf16)
    for bit in reversed(bits):
        pairs = [(i, i ^ (1 << bit)) for i in range(size)]
        other = lax.ppermute(value, "dp", pairs)
        token = yield value
        other = after(other, token)
        if bit:
            value = jnp.concatenate([value, other], 0)
    yield value, other


def sum_all(value):
    steps = [("mp", 1), ("mp", 2)] + [("dp", 1 << bit) for bit in range(lax.axis_size("dp").bit_length() - 1)]
    for axis, flip in steps:
        pairs = [(i, i ^ flip) for i in range(lax.axis_size(axis))]
        got = lax.ppermute(value, axis, pairs)
        token = yield value
        value = value + after(got, token)
    yield value


def next_step(chain, token, first=False):
    try:
        return next(chain) if first else chain.send(token)
    except StopIteration:
        return None


def body(
    inputs,
    memory,
    target_len,
    memory_len,
    bucket_map,
    self_gain,
    self_query,
    self_key,
    self_value,
    self_out,
    bias_table,
    cross_gain,
    cross_query,
    cross_key,
    cross_value,
    cross_out,
    feed_gain,
    feed_input,
    feed_output,
    cotangent,
):
    rank = lax.axis_index("mp")
    rows, d = inputs.shape
    key_rows = memory.shape[0]
    width = self_query.shape[1]
    wide = 4 * width
    heads = bias_table.shape[1]
    units = feed_input.shape[1]
    examples = rows // TGT_LEN
    rank_value = rank.astype(jnp.int32).reshape(1)
    blocks = lax.axis_size("dp")
    place = lax.axis_index("dp").astype(jnp.int32)
    turn = jnp.zeros((1,), jnp.int32)
    for bit in range(blocks.bit_length() - 1):
        turn = 2 * turn + ((place >> bit) & 1)

    distance = (TGT_LEN - jnp.arange(TGT_LEN, dtype=jnp.int32)) % TGT_LEN
    lookup = distance[:, None] == jnp.arange(TGT_LEN, dtype=jnp.int32)[None, :]
    bucket = jnp.sum(jnp.where(lookup, bucket_map[None, :], 0), -1)
    hot = (bucket[:, None] == jnp.arange(BUCKETS, dtype=jnp.int32)[None, :]).astype(f32)
    by_distance = lax.dot_general(bias_table, hot, (((0,), (1,)), ((), ())), precision=highest)
    big = (rows, d)
    head_rows = (rows, wide)
    key_heads = (key_rows, wide)
    heads_key = (wide, key_rows)
    square = ((heads * TGT_LEN, TGT_LEN), f32)
    group_heads = (4 * rows, width)
    pack = ((2, rows, d), bf16)
    product = 2 * rows * d * wide

    def grad_half(count, size):
        return ((blocks // 2, count, size // blocks, d), bf16)

    def grad_rows(count, size, lead=()):
        return ((*lead, blocks, count, size // blocks, d), bf16)

    cross_own = jnp.concatenate([cross_query.T, cross_out, cross_key.T, cross_value.T], 0)
    normed_one = call(first_norm, (inputs, self_gain), [(big, bf16)])[0]
    far = after(swap_chip(normed_one), by_distance)
    ones = (normed_one, swap_core(normed_one), far, swap_core(far))
    cross_far = swap_chip(after(cross_own, far))
    self_q, self_k, self_v, self_mixed, own, chip, send = call(
        self_forward,
        (*ones, self_query.T, self_key.T, self_value.T, self_out, by_distance, rank_value, target_len),
        [(group_heads, bf16)] * 4 + [(big, f32), (big, f32), pack],
        [square],
        flops=4 * product,
        smem=(9, 10),
    )
    near, far_send = core_sum(chip, send)
    far = swap_chip(far_send)
    cross_far = after(cross_far, far_send)
    cross = (cross_own, swap_core(cross_own), cross_far, swap_core(cross_far))
    cross_k, cross_v = call(
        memory_forward, (memory, *cross), [(key_heads, bf16)] * 2, flops=8 * product
    )
    far = after(far, cross_v)
    ups_far = swap_chip(after(cotangent, far))
    after_self, normed_two, cross_q, cross_mixed, after_cross, normed_three = call(
        cross_forward,
        (inputs, own, near, far, cross_k, cross_v, cross_gain, feed_gain, *cross, rank_value, memory_len),
        [(big, f32), (big, bf16), (head_rows, bf16), (head_rows, bf16), (big, f32), (big, bf16)],
        flops=6 * product,
        smem=(12, 13),
    )
    ups_far = after(ups_far, normed_three)
    ups = (cotangent, swap_core(cotangent), ups_far, swap_core(ups_far))
    many = 4 * rows
    far = swap_chip(normed_three)
    hidden = call(feed_hidden, (*ups, feed_output), [((many, units), f32)], flops=4 * product)[0]
    far = after(far, hidden)
    gathered = (normed_three, swap_core(normed_three), far, swap_core(far))
    own, chip, send, activated, pre_grad = call(
        feed_main,
        (*gathered, hidden, feed_input),
        [(big, f32), (big, f32), pack, ((many, units), bf16), ((many, units), bf16)],
        flops=12 * product,
    )
    near, far_send = core_sum(chip, send)
    far = swap_chip(far_send)
    out_own, out_chip, out_send, low, high = call(
        feed_rest,
        (*gathered, *ups, after(activated, far_send), pre_grad, feed_output, turn),
        [(big, f32), (big, f32), pack] + [grad_half(2, d)] * 2,
        [grad_rows(2, d)],
        flops=12 * product,
        smem=(11,),
    )
    zero = dp_chain(low, high)
    token = next(zero)
    far = after(far, token)
    grad_one, up_one, key_grad, value_grad, late_gains, keep, send = call(
        cross_backward,
        (own, near, far, cotangent, after_cross, after_self, cross_gain, feed_gain)
        + (normed_two, cross_q, cross_k, cross_v, cross_mixed, *cross, rank_value, memory_len, turn),
        [(big, f32), (big, bf16), (heads_key, bf16), (heads_key, bf16), ((2, d), f32)] + [grad_rows(2, width, (2,))] * 2,
        [(head_rows, bf16), (head_rows, bf16)],
        flops=16 * product,
        smem=(17, 18, 19),
    )
    up_far = swap_chip(up_one)
    keep, send = call(
        memory_weights,
        (key_grad, value_grad, memory, keep, send, turn),
        [grad_rows(4, width, (2,))] * 2,
        flops=8 * product,
        smem=(5,),
    )
    up_far = after(up_far, keep)
    token = zero.send(up_far)
    one_near, one_send = core_sum(keep[1], after(send, token))
    one_far = swap_chip(one_send)
    self_ups = (up_one, swap_core(up_one), after(up_far, one_send), swap_core(up_far))
    low, high, sums, own, chip, send = call(
        self_backward,
        (*self_ups, *ones, self_q, self_k, self_v, self_mixed)
        + (self_query.T, self_key.T, self_value.T, self_out, by_distance, rank_value, target_len, turn),
        [grad_half(4, width)] * 2 + [((8, TGT_LEN), f32), (big, f32), (big, f32), pack],
        [square, square] + [(group_heads, bf16)] * 4 + [grad_rows(4, width)],
        flops=10 * product,
        smem=(17, 18, 19),
    )
    memory_grad = call(
        memory_backward,
        (after(key_grad, sums), value_grad, *cross),
        [((key_rows, d), f32)],
        flops=8 * product,
    )[0]
    token = zero.send(memory_grad)
    two = dp_chain(low, after(high, token))
    token = next(two)
    near, far_send = core_sum(chip, after(send, token))
    far = swap_chip(far_send)
    one_sum = (keep[0].astype(f32) + one_near[0].astype(f32) + after(one_far, far_send).astype(f32)).astype(bf16)
    one = dp_chain(one_sum[: blocks // 2], one_sum[blocks // 2 :])
    token = next(one)
    token = zero.send(token)
    token = two.send(token)
    inputs_grad, small = call(
        last_norm,
        (grad_one, own, near, after(far, token), inputs, self_gain, late_gains, sums, rank_value),
        [(big, f32), ((40, d), f32)],
        smem=(8,),
    )
    small = sum_all(small)
    token = next_step(small, inputs_grad, True)
    out_near, out_send = core_sum(out_chip, after(out_send, token))
    out_far = swap_chip(out_send)
    total = {}
    waiting = [(zero, "zero"), (two, "two"), (one, "one"), (small, "small")]
    while waiting:
        still = []
        for chain, name in waiting:
            step = next_step(chain, token)
            if step is None:
                continue
            total[name] = step
            token = step[1] if name != "small" and isinstance(step, tuple) else step
            still.append((chain, name))
        waiting = still
    layer_out = (after_cross + out_own + out_near[0].astype(f32) + out_far.astype(f32)).astype(bf16)
    feed_grads = call(finish, (*total["zero"], turn), [((d, units), f32), ((units, d), f32)], smem=(2,))
    cross_grads = call(finish, (*total["one"], turn), [((width, d), f32)] * 4, smem=(2,))
    self_grads = call(finish, (*total["two"], turn), [((width, d), f32)] * 4, smem=(2,))
    gains = total["small"][:3]
    own_sums = lax.dynamic_slice(total["small"], (8 * (rank + 1), 0), (heads, TGT_LEN))
    bias_grad = lax.dot_general(hot, own_sums, (((0,), (1,)), ((), ())), precision=highest)

    return (
        layer_out,
        inputs_grad,
        memory_grad,
        gains[0],
        self_grads[0].T,
        self_grads[1].T,
        self_grads[2].T,
        self_grads[3],
        bias_grad,
        gains[1],
        cross_grads[0].T,
        cross_grads[2].T,
        cross_grads[3].T,
        cross_grads[1],
        gains[2],
        *feed_grads,
    )


def solution(mesh):
    in_specs = (
        P(("dp", "mp"), None),
        P(("dp", "mp"), None),
        P("dp"),
        P("dp"),
        P(),
        P(),
        P(None, "mp"),
        P(None, "mp"),
        P(None, "mp"),
        P("mp", None),
        P(None, "mp"),
        P(),
        P(None, "mp"),
        P(None, "mp"),
        P(None, "mp"),
        P("mp", None),
        P(),
        P(None, "mp"),
        P("mp", None),
        P(("dp", "mp"), None),
    )
    out_specs = (
        P(("dp", "mp"), None),
        P(("dp", "mp"), None),
        P(("dp", "mp"), None),
        P(),
        P(None, "mp"),
        P(None, "mp"),
        P(None, "mp"),
        P("mp", None),
        P(None, "mp"),
        P(),
        P(None, "mp"),
        P(None, "mp"),
        P(None, "mp"),
        P("mp", None),
        P(),
        P(None, "mp"),
        P("mp", None),
    )
    return jax.shard_map(body, mesh=mesh, in_specs=in_specs, out_specs=out_specs, check_vma=False)
```

```python
import functools

import jax
import jax.numpy as jnp
from jax import lax
from jax.experimental import pallas as pl
from jax.experimental.pallas import tpu as pltpu
from jax.sharding import PartitionSpec as P

HEAD_DIM = 64
PAIR = 2 * HEAD_DIM
BUCKETS = 32
TGT_LEN = 128
MEM_LEN = 512

masked_fill = -1000000000.0
epsilon = 1e-06
highest = lax.Precision.HIGHEST
tanh_scale = 0.7978845608
cubic_term = 0.044715
bf16 = jnp.bfloat16
f32 = jnp.float32


def dot_nn(a, b):
    return lax.dot_general(a, b, (((1,), (0,)), ((), ())), preferred_element_type=f32)


def dot_nt(a, b):
    return lax.dot_general(a, b, (((1,), (1,)), ((), ())), preferred_element_type=f32)


def dot_tn(a, b):
    return lax.dot_general(a, b, (((0,), (0,)), ((), ())), preferred_element_type=f32)


def row_scale(hidden):
    return lax.rsqrt(jnp.mean(hidden * hidden, -1, keepdims=True) + epsilon)


def norm_backward(hidden, scale, gain, upstream):
    weighted = gain * upstream
    return scale * weighted - hidden * (scale * scale * scale) * jnp.mean(hidden * weighted, -1, keepdims=True)


def matrix(blocks, index, width):
    return jnp.concatenate([b[index * width : (index + 1) * width, :] for b in blocks], 0)


def store_rows(ref, lead, index, grad, turn):
    blocks = ref.shape[len(lead)]
    size = grad.shape[0] // blocks
    for a in range(blocks):
        ref[(*lead, a ^ turn, index)] = grad[a * size : (a + 1) * size].astype(bf16)


def store_halves(low_ref, high_ref, ref):
    half = ref.shape[0] // 2
    low_ref[...] = ref[:half]
    high_ref[...] = ref[half:]


def store_grad(keep_ref, send_ref, index, grad, turn):
    width = grad.shape[0] // 4
    for j in range(4):
        store_rows((keep_ref, send_ref)[j % 2], (j // 2,), index, grad[j * width : (j + 1) * width], turn)


def pair_masks():
    lane = lax.broadcasted_iota(jnp.int32, (1, PAIR), 1)
    return (lane < HEAD_DIM).astype(bf16), (lane >= HEAD_DIM).astype(bf16)


def stack_pair(rows, masks):
    return jnp.concatenate([rows * masks[0], rows * masks[1]], 0)


def unstack_pair(both):
    lane = lax.broadcasted_iota(jnp.int32, (TGT_LEN, PAIR), 1)
    return jnp.where(lane < HEAD_DIM, both[:TGT_LEN], both[TGT_LEN:])


def softmax_rows(scores):
    weights = jnp.exp(scores - jnp.max(scores, -1, keepdims=True))
    return weights * (1.0 / jnp.sum(weights, -1, keepdims=True))


def locate(step, pairs, keys):
    example = lax.div(step, pairs)
    pair = lax.rem(step, pairs)
    rows = pl.ds(pl.multiple_of(example * TGT_LEN, TGT_LEN), TGT_LEN)
    key_rows = pl.ds(pl.multiple_of(example * keys, keys), keys)
    cols = pl.ds(pl.multiple_of(pair * PAIR, PAIR), PAIR)
    return example, pair, rows, key_rows, cols


def cross_probs(queries, key_rows, length):
    scores = dot_nt(queries, key_rows)
    key = lax.broadcasted_iota(jnp.int32, scores.shape, 1)
    return softmax_rows(jnp.where(key < length, scores, masked_fill))


def attend(q_ref, k_ref, v_ref, mixed_ref, keys, probs_of):
    masks = pair_masks()
    pairs = q_ref.shape[1] // PAIR
    examples = q_ref.shape[0] // TGT_LEN

    def step(i, carry):
        example, pair, rows, key_rows, cols = locate(i, pairs, keys)
        probs = probs_of(stack_pair(q_ref[rows, cols], masks), k_ref[key_rows, cols], example, pair)
        mixed = dot_nn(probs.astype(bf16), v_ref[key_rows, cols])
        mixed_ref[rows, cols] = unstack_pair(mixed).astype(bf16)
        return carry

    lax.fori_loop(0, examples * pairs, step, 0, unroll=UNROLL)


def attend_back(q_ref, k_ref, v_ref, m_ref, dq_ref, dk_ref, dv_ref, keys, probs_of):
    masks = pair_masks()
    pairs = q_ref.shape[1] // PAIR
    examples = q_ref.shape[0] // TGT_LEN

    def step(i, carry):
        example, pair, rows, key_rows, cols = locate(i, pairs, keys)
        queries = stack_pair(q_ref[rows, cols], masks)
        grads = stack_pair(m_ref[rows, cols], masks)
        key_block = k_ref[key_rows, cols]
        probs = probs_of(queries, key_block, example, pair)
        dv_ref[cols, key_rows] = dot_tn(grads, probs.astype(bf16)).astype(bf16)
        prob_grad = dot_nt(grads, v_ref[key_rows, cols])
        score_grad = probs * (prob_grad - jnp.sum(probs * prob_grad, -1, keepdims=True))
        low = score_grad.astype(bf16)
        dq_ref[rows, cols] = unstack_pair(dot_nn(low, key_block)).astype(bf16)
        dk_ref[cols, key_rows] = dot_tn(queries, low).astype(bf16)
        return carry

    lax.fori_loop(0, examples * pairs, step, 0, unroll=UNROLL)


UNROLL = 4


def fill_bias(table_ref, bias_ref):
    for head in range(bias_ref.shape[0] // TGT_LEN):
        row = jnp.broadcast_to(table_ref[head : head + 1, :], (TGT_LEN, TGT_LEN))
        bias_ref[head * TGT_LEN : (head + 1) * TGT_LEN, :] = pltpu.roll(row, 0, axis=1, stride=1, stride_axis=0)


def stack_heads(rows):
    lane = lax.broadcasted_iota(jnp.int32, (1, rows.shape[1]), 1)
    heads = rows.shape[1] // HEAD_DIM
    return jnp.concatenate([rows * (lax.div(lane, HEAD_DIM) == h).astype(bf16) for h in range(heads)], 0)


def unstack_heads(stacked):
    length = TGT_LEN
    lane = lax.broadcasted_iota(jnp.int32, (length, stacked.shape[1]), 1)
    out = stacked[:length]
    for h in range(1, stacked.shape[1] // HEAD_DIM):
        out = jnp.where(lane >= h * HEAD_DIM, stacked[h * length : (h + 1) * length], out)
    return out


def self_probs(queries, key_rows, bias, length):
    scores = dot_nt(queries, key_rows) + bias
    key = lax.broadcasted_iota(jnp.int32, scores.shape, 1)
    query = lax.rem(lax.broadcasted_iota(jnp.int32, scores.shape, 0), TGT_LEN)
    return softmax_rows(jnp.where((key <= query) & (key < length), scores, masked_fill))


def diagonal_sums(grad):
    query = lax.broadcasted_iota(jnp.int32, grad.shape, 0)
    for bit in range(TGT_LEN.bit_length() - 1):
        moved = pltpu.roll(grad, TGT_LEN - (1 << bit), axis=1)
        grad = jnp.where((query >> bit) & 1 == 1, moved, grad)
    return jnp.sum(grad, 0, keepdims=True)


def first_norm(x_ref, gain_ref, n_ref):
    hidden = x_ref[...].astype(f32)
    n_ref[...] = (hidden * row_scale(hidden) * gain_ref[...].reshape(1, -1)).astype(bf16)


def self_forward(
    base, n0, n1, wq_ref, wk_ref, wv_ref, wo_ref, table_ref, rank_ref, len_ref,
    q_ref, k_ref, v_ref, mixed_ref, keep_ref, send_ref, bias_ref,
):
    fill_bias(table_ref, bias_ref)
    size = n0.shape[0]
    for j, n in enumerate((n0, n1)):
        rows = slice(j * size, (j + 1) * size)
        for ref, w in ((q_ref, wq_ref), (k_ref, wk_ref), (v_ref, wv_ref)):
            ref[rows, :] = dot_nt(n[...], w[...]).astype(bf16)

    def step(i, carry):
        rows = pl.ds(pl.multiple_of(i * TGT_LEN, TGT_LEN), TGT_LEN)
        length = len_ref[(rank_ref[0] * (size // TGT_LEN)) ^ (base + i)]
        probs = self_probs(stack_heads(q_ref[rows, :]), k_ref[rows, :], bias_ref[...], length)
        mixed_ref[rows, :] = unstack_heads(dot_nn(probs.astype(bf16), v_ref[rows, :])).astype(bf16)
        return carry

    lax.fori_loop(0, 2 * size // TGT_LEN, step, 0, unroll=UNROLL)
    keep_ref[...] = dot_nn(mixed_ref[:size, :], wo_ref[...])
    send_ref[...] = dot_nn(mixed_ref[size:, :], wo_ref[...]).astype(bf16)


def store_parts(own_ref, chip_ref, send_ref, parts):
    for j, part in enumerate(parts):
        if j == 0:
            own_ref[...] = part
        elif j == 2:
            chip_ref[...] = part
        else:
            send_ref[j // 2] = part.astype(bf16)


def memory_forward(mem_ref, w0, w1, w2, w3, k_ref, v_ref):
    width = k_ref.shape[1] // 4
    blocks = (w0, w1, w2, w3)
    k_ref[...] = dot_nt(mem_ref[...], matrix(blocks, 2, width)).astype(bf16)
    v_ref[...] = dot_nt(mem_ref[...], matrix(blocks, 3, width)).astype(bf16)


def cross_forward(
    x_ref, own_ref, near_ref, far_ref, k_ref, v_ref, gain_two_ref, gain_three_ref, w0, w1, w2, w3, rank_ref, len_ref,
    after_self_ref, n2_ref, q_ref, mixed_ref, after_ref, n3_ref,
):
    blocks = (w0, w1, w2, w3)
    width = q_ref.shape[1] // 4
    after_self = x_ref[...].astype(f32) + own_ref[...] + near_ref[...].astype(f32) + far_ref[...].astype(f32)
    after_self_ref[...] = after_self
    normed = (after_self * row_scale(after_self) * gain_two_ref[...].reshape(1, -1)).astype(bf16)
    n2_ref[...] = normed
    q_ref[...] = dot_nt(normed, matrix(blocks, 0, width)).astype(bf16)

    def probs(queries, key_rows, example, pair):
        return cross_probs(queries, key_rows, len_ref[rank_ref[0] * (q_ref.shape[0] // TGT_LEN) + example])

    attend(q_ref, k_ref, v_ref, mixed_ref, MEM_LEN, probs)
    after = after_self_ref[...] + dot_nn(mixed_ref[...], matrix(blocks, 1, width))
    after_ref[...] = after
    n3_ref[...] = (after * row_scale(after) * gain_three_ref[...].reshape(1, -1)).astype(bf16)


def feed_hidden(c0, c1, c2, c3, out_ref, hidden_ref):
    for j, c in enumerate((c0, c1, c2, c3)):
        hidden_ref[j * c.shape[0] : (j + 1) * c.shape[0], :] = dot_nt(c[...], out_ref[...])


def feed_main(base, g0, g1, hidden_ref, in_ref, keep_ref, send_ref, act_ref, pre_grad_ref):
    size = g0.shape[0]
    for j, g in enumerate((g0, g1)):
        rows = slice(j * size, (j + 1) * size)
        pre = dot_nn(g[...], in_ref[...])
        square = pre * pre
        tanh = jnp.tanh(tanh_scale * (pre + cubic_term * square * pre))
        act_ref[rows, :] = (0.5 * pre * (1.0 + tanh)).astype(bf16)
        slope = 0.5 * (1.0 + tanh) + 0.5 * pre * (1.0 - tanh * tanh) * (
            tanh_scale * (1.0 + 3.0 * cubic_term * square)
        )
        low = (hidden_ref[base + j * size : base + (j + 1) * size, :] * slope).astype(bf16)
        pre_grad_ref[rows, :] = low
        grad = dot_nt(low, in_ref[...])
        if j == 0:
            keep_ref[...] = grad
        else:
            send_ref[...] = grad.astype(bf16)


def feed_rest(
    g0, g1, g2, g3, c0, c1, c2, c3, act_a, act_b, pre_grad_a, pre_grad_b, out_ref, turn_ref, own_ref, chip_ref, send_ref, low_ref, high_ref, grads_ref
):
    activated = jnp.concatenate([act_a[...], act_b[...]], 0)
    pre_grad = jnp.concatenate([pre_grad_a[...], pre_grad_b[...]], 0)
    gathered = jnp.concatenate([g[...] for g in (g0, g1, g2, g3)], 0)
    store_rows(grads_ref, (), 0, dot_tn(gathered, pre_grad), turn_ref[0])
    upstream = jnp.concatenate([c[...] for c in (c0, c1, c2, c3)], 0)
    store_rows(grads_ref, (), 1, dot_tn(activated, upstream), turn_ref[0])
    store_halves(low_ref, high_ref, grads_ref)
    for j in range(4):
        rows = slice(j * g0.shape[0], (j + 1) * g0.shape[0])
        part = dot_nn(activated[rows, :], out_ref[...])
        if j == 0:
            own_ref[...] = part
        elif j == 2:
            chip_ref[...] = part
        else:
            send_ref[j // 2] = part.astype(bf16)


def cross_backward(
    own_ref, near_ref, far_ref, cot_ref, after_ref, after_self_ref, gain_two_ref, gain_three_ref,
    n2_ref, q_ref, k_ref, v_ref, mixed_ref, w0, w1, w2, w3, rank_ref, len_ref, turn_ref,
    grad_one_ref, up_ref, dk_ref, dv_ref, gains_ref, keep_ref, send_ref, m_ref, dq_ref,
):
    blocks = (w0, w1, w2, w3)
    width = q_ref.shape[1] // 4
    after = after_ref[...]
    scale = row_scale(after)
    upstream = own_ref[...] + near_ref[...].astype(f32) + far_ref[...].astype(f32)
    gains_ref[1:2, :] = jnp.sum(upstream * after * scale, 0, keepdims=True)
    grad_two = cot_ref[...].astype(f32) + norm_backward(after, scale, gain_three_ref[...].reshape(1, -1), upstream)
    grad_one_ref[...] = grad_two
    up_two = grad_two.astype(bf16)
    m_ref[...] = dot_nt(up_two, matrix(blocks, 1, width)).astype(bf16)
    store_grad(keep_ref, send_ref, 1, dot_tn(mixed_ref[...], up_two), turn_ref[0])

    def probs(queries, key_rows, example, pair):
        return cross_probs(queries, key_rows, len_ref[rank_ref[0] * (q_ref.shape[0] // TGT_LEN) + example])

    attend_back(q_ref, k_ref, v_ref, m_ref, dq_ref, dk_ref, dv_ref, MEM_LEN, probs)
    store_grad(keep_ref, send_ref, 0, dot_tn(dq_ref[...], n2_ref[...]), turn_ref[0])
    upstream = dot_nn(dq_ref[...], matrix(blocks, 0, width))
    hidden = after_self_ref[...]
    scale = row_scale(hidden)
    gains_ref[0:1, :] = jnp.sum(upstream * hidden * scale, 0, keepdims=True)
    grad_one = grad_one_ref[...] + norm_backward(hidden, scale, gain_two_ref[...].reshape(1, -1), upstream)
    grad_one_ref[...] = grad_one
    up_ref[...] = grad_one.astype(bf16)


def memory_weights(dk_ref, dv_ref, mem_ref, keep_in, send_in, turn_ref, keep_ref, send_ref):
    count = keep_in.shape[2]
    for j in range(2):
        for a in range(keep_in.shape[1]):
            keep_ref[j, a, :count] = keep_in[j, a]
            send_ref[j, a, :count] = send_in[j, a]
    store_grad(keep_ref, send_ref, count, dot_nn(dk_ref[...], mem_ref[...]), turn_ref[0])
    store_grad(keep_ref, send_ref, count + 1, dot_nn(dv_ref[...], mem_ref[...]), turn_ref[0])


def self_backward(
    u0, u1, u2, u3, n0, n1, n2, n3, qa, ka, va, xa, qb, kb, vb, xb, wq_ref, wk_ref, wv_ref, wo_ref,
    table_ref, rank_ref, len_ref, turn_ref,
    low_ref, high_ref, sums_ref, own_ref, chip_ref, send_ref,
    bias_ref, score_ref, m_ref, dq_ref, dk_ref, dv_ref, grads_ref,
):
    fill_bias(table_ref, bias_ref)
    score_ref[...] = jnp.zeros_like(score_ref)
    size = n0.shape[0]
    width = qa.shape[1]
    for j, u in enumerate((u0, u1, u2, u3)):
        m_ref[j * size : (j + 1) * size, :] = dot_nt(u[...], wo_ref[...]).astype(bf16)

    for base, q_ref, k_ref, v_ref in ((0, qa, ka, va), (2 * size, qb, kb, vb)):

        def step(i, carry, base=base, q_ref=q_ref, k_ref=k_ref, v_ref=v_ref):
            rows = pl.ds(pl.multiple_of(i * TGT_LEN, TGT_LEN), TGT_LEN)
            all_rows = pl.ds(pl.multiple_of(base + i * TGT_LEN, TGT_LEN), TGT_LEN)
            length = len_ref[(rank_ref[0] * (size // TGT_LEN)) ^ (base // TGT_LEN + i)]
            queries = stack_heads(q_ref[rows, :])
            grads = stack_heads(m_ref[all_rows, :])
            key_block = k_ref[rows, :]
            probs = self_probs(queries, key_block, bias_ref[...], length)
            dv_ref[all_rows, :] = dot_tn(probs.astype(bf16), grads).astype(bf16)
            prob_grad = dot_nt(grads, v_ref[rows, :])
            score_grad = probs * (prob_grad - jnp.sum(probs * prob_grad, -1, keepdims=True))
            score_ref[...] += score_grad
            low = score_grad.astype(bf16)
            dq_ref[all_rows, :] = unstack_heads(dot_nn(low, key_block)).astype(bf16)
            dk_ref[all_rows, :] = dot_tn(low, queries).astype(bf16)
            return carry

        lax.fori_loop(0, 2 * size // TGT_LEN, step, 0, unroll=UNROLL)
    normed = jnp.concatenate([n[...] for n in (n0, n1, n2, n3)], 0)
    upstream = jnp.concatenate([u[...] for u in (u0, u1, u2, u3)], 0)
    mixed = jnp.concatenate([xa[...], xb[...]], 0)
    for index, (left, right) in enumerate(
        ((dq_ref[...], normed), (dk_ref[...], normed), (dv_ref[...], normed), (mixed, upstream))
    ):
        store_rows(grads_ref, (), index, dot_tn(left, right), turn_ref[0])
    store_halves(low_ref, high_ref, grads_ref)
    heads = width // HEAD_DIM
    sums = [diagonal_sums(score_ref[h * TGT_LEN : (h + 1) * TGT_LEN, :]) for h in range(heads)]
    sums_ref[:heads, :] = jnp.concatenate(sums, 0)
    sums_ref[heads:, :] = jnp.zeros((sums_ref.shape[0] - heads, TGT_LEN), f32)

    def part(j):
        rows = slice(j * size, (j + 1) * size)
        out = dot_nn(dq_ref[rows, :], wq_ref[...])
        return out + dot_nn(dk_ref[rows, :], wk_ref[...]) + dot_nn(dv_ref[rows, :], wv_ref[...])

    store_parts(own_ref, chip_ref, send_ref, (part(j) for j in range(4)))


def last_norm(grad_one_ref, own_ref, near_ref, far_ref, x_ref, gain_ref, late_ref, sums_ref, rank_ref, grad_ref, small_ref):
    upstream = own_ref[...] + near_ref[...].astype(f32) + far_ref[...].astype(f32)
    hidden = x_ref[...].astype(f32)
    scale = row_scale(hidden)
    small_ref[...] = jnp.zeros_like(small_ref)
    small_ref[0:1, :] = jnp.sum(upstream * hidden * scale, 0, keepdims=True)
    small_ref[1:3, :] = late_ref[...]
    for j in range(4):
        here = (rank_ref[0] == j).astype(f32)
        small_ref[8 * (j + 1) : 8 * (j + 2), :TGT_LEN] = sums_ref[...] * here
    grad_ref[...] = grad_one_ref[...] + norm_backward(hidden, scale, gain_ref[...].reshape(1, -1), upstream)


def gather_order(bits, early):
    return [0, bits - 1, *range(1, bits - 1)] if early else list(range(bits))


def gather_rows(low_ref, high_ref, index, turn, early):
    half = low_ref.shape[0]
    order = gather_order((2 * half).bit_length() - 1, early)
    pieces = []
    for a in range(2 * half):
        place = a ^ turn
        inside = sum(((place >> bit) & 1) << i for i, bit in enumerate(order[:-1]))
        low = (place >> order[-1]) & 1 == 0
        pieces.append(jnp.where(low, low_ref[inside, index].astype(f32), high_ref[inside, index].astype(f32)))
    return jnp.concatenate(pieces, 0)


def finish(early, low_ref, high_ref, turn_ref, *outs):
    for index, ref in enumerate(outs):
        ref[...] = gather_rows(low_ref, high_ref, index, turn_ref[0], early)


def memory_backward(dk_ref, dv_ref, w0, w1, w2, w3, grad_ref):
    blocks = (w0, w1, w2, w3)
    width = dk_ref.shape[0] // 4
    grad_ref[...] = dot_tn(dk_ref[...], matrix(blocks, 2, width)) + dot_tn(dv_ref[...], matrix(blocks, 3, width))


def call(kernel, operands, outs, scratch=(), flops=0, smem=()):
    moved = sum(a.size * a.dtype.itemsize for a in operands)
    moved += sum(functools.reduce(lambda x, y: x * y, s) * jnp.dtype(t).itemsize for s, t in outs)
    return pl.pallas_call(
        kernel,
        out_shape=[jax.ShapeDtypeStruct(s, t) for s, t in outs],
        in_specs=[
            pl.BlockSpec(memory_space=pltpu.SMEM if i in smem else pltpu.VMEM) for i in range(len(operands))
        ],
        out_specs=[pl.BlockSpec(memory_space=pltpu.VMEM) for _ in outs],
        scratch_shapes=[pltpu.VMEM(s, t) for s, t in scratch],
        compiler_params=pltpu.CompilerParams(vmem_limit_bytes=VMEM_LIMIT),
        cost_estimate=pl.CostEstimate(flops=flops, bytes_accessed=moved, transcendentals=0),
    )(*operands)


VMEM_LIMIT = 56 * 1024 * 1024


def after(value, *others):
    return lax.optimization_barrier((value, *others))[0]


def swap_core(a):
    return lax.ppermute(a, "mp", [(0, 1), (1, 0), (2, 3), (3, 2)])


def swap_chip(a):
    return lax.ppermute(a, "mp", [(0, 2), (2, 0), (1, 3), (3, 1)])


def gather_blocks(a):
    far = swap_chip(a)
    return (a, swap_core(a), far, swap_core(far))


def core_sum(chip, got):
    return (chip.astype(f32) + got.astype(f32)).astype(bf16)


def plus(a, b):
    return (a.astype(f32) + b.astype(f32)).astype(bf16)


def swap_dp(a, bit):
    return lax.ppermute(a, "dp", [(i, i ^ (1 << bit)) for i in range(lax.axis_size("dp"))])


def dp_chain(keep, send, early=False):
    bits = lax.axis_size("dp").bit_length() - 1
    for bit in range(bits):
        got = swap_dp(send, bit)
        tokens = yield send
        got = after(got, *tokens)
        half = keep.shape[0] // 2
        if half:
            send, keep = plus(keep[half:], got[half:]), plus(keep[:half], got[:half])
        else:
            value = plus(keep, got)
    for step, bit in enumerate(gather_order(bits, early)):
        other = swap_dp(value, bits - 1 - bit)
        tokens = yield value
        other = after(other, *tokens)
        if step < bits - 1:
            value = jnp.concatenate([value, other], 0)
    yield value, other


def sum_all(value):
    steps = [("mp", 1), ("mp", 2)] + [("dp", 1 << bit) for bit in reversed(range(lax.axis_size("dp").bit_length() - 1))]
    for axis, flip in steps:
        pairs = [(i, i ^ flip) for i in range(lax.axis_size(axis))]
        got = lax.ppermute(value, axis, pairs)
        tokens = yield value
        value = value + after(got, *tokens)
    yield value


ROUNDS = (
    ("two",),
    ("zero", "one"),
    ("small",),
    ("two", "one"),
    ("small",),
    ("two", "one"),
    ("small",),
    ("two",),
    ("one",),
    ("small",),
    ("zero",),
    ("one",),
)


class Chains:
    def __init__(self):
        self.under_way, self.last, self.tokens = {}, {}, ()

    def start(self, name, chain):
        self.under_way[name] = chain
        self.last[name] = next(chain)
        return self.last[name]

    def turn(self, *names):
        sent = []
        for name in names:
            try:
                self.last[name] = self.under_way[name].send(self.tokens)
                sent.append(self.last[name])
            except (StopIteration, KeyError):
                self.under_way.pop(name, None)
        if sent:
            self.tokens = tuple(t for t in sent if not isinstance(t, tuple)) or sent[0]
        return self.tokens

    def drain(self):
        while self.under_way:
            for name in list(self.under_way):
                self.turn(name)


def body(
    inputs,
    memory,
    target_len,
    memory_len,
    bucket_map,
    self_gain,
    self_query,
    self_key,
    self_value,
    self_out,
    bias_table,
    cross_gain,
    cross_query,
    cross_key,
    cross_value,
    cross_out,
    feed_gain,
    feed_input,
    feed_output,
    cotangent,
):
    rank = lax.axis_index("mp")
    rows, d = inputs.shape
    key_rows = memory.shape[0]
    width = self_query.shape[1]
    wide = 4 * width
    heads = bias_table.shape[1]
    units = feed_input.shape[1]
    examples = rows // TGT_LEN
    rank_value = rank.astype(jnp.int32).reshape(1)
    blocks = lax.axis_size("dp")
    place = lax.axis_index("dp").astype(jnp.int32)
    turn = jnp.zeros((1,), jnp.int32)
    for bit in range(blocks.bit_length() - 1):
        turn = 2 * turn + ((place >> bit) & 1)

    distance = (TGT_LEN - jnp.arange(TGT_LEN, dtype=jnp.int32)) % TGT_LEN
    lookup = distance[:, None] == jnp.arange(TGT_LEN, dtype=jnp.int32)[None, :]
    bucket = jnp.sum(jnp.where(lookup, bucket_map[None, :], 0), -1)
    hot = (bucket[:, None] == jnp.arange(BUCKETS, dtype=jnp.int32)[None, :]).astype(f32)
    by_distance = lax.dot_general(bias_table, hot, (((0,), (1,)), ((), ())), precision=highest)
    big = (rows, d)
    head_rows = (rows, wide)
    key_heads = (key_rows, wide)
    heads_key = (wide, key_rows)
    square = ((heads * TGT_LEN, TGT_LEN), f32)
    group_heads = (4 * rows, width)
    half_heads = (2 * rows, width)
    pack = ((2, rows, d), bf16)
    product = 2 * rows * d * wide

    def grad_half(count, size):
        return ((blocks // 2, count, size // blocks, d), bf16)

    def grad_rows(count, size, lead=()):
        return ((*lead, blocks, count, size // blocks, d), bf16)

    cross_own = jnp.concatenate([cross_query.T, cross_out, cross_key.T, cross_value.T], 0)
    normed_one = call(first_norm, (inputs, self_gain), [(big, bf16)])[0]
    far = swap_chip(normed_one)
    cross_far = swap_chip(after(cross_own, normed_one))
    self_weights = (self_query.T, self_key.T, self_value.T, self_out)

    def self_half(base, pair):
        return call(
            functools.partial(self_forward, base),
            (*pair, *self_weights, by_distance, rank_value, target_len),
            [(half_heads, bf16)] * 4 + [(big, f32), (big, bf16)],
            [square],
            flops=2 * product,
            smem=(7, 8),
        )

    ones = (normed_one, swap_core(normed_one))
    *self_a, own, send = self_half(0, ones)
    near = swap_core(send)
    far = after(far, near)
    ones = (*ones, far, swap_core(far))
    *self_b, chip, send = self_half(2 * rows // TGT_LEN, ones[2:])
    far_send = core_sum(chip, swap_core(send))
    far = swap_chip(far_send)
    cross_far = after(cross_far, far_send)
    cross = (cross_own, swap_core(cross_own), cross_far, swap_core(cross_far))
    cross_k, cross_v = call(
        memory_forward, (memory, *cross), [(key_heads, bf16)] * 2, flops=8 * product
    )
    far = after(far, cross_v)
    ups_far = swap_chip(after(cotangent, far))
    after_self, normed_two, cross_q, cross_mixed, after_cross, normed_three = call(
        cross_forward,
        (inputs, own, near, far, cross_k, cross_v, cross_gain, feed_gain, *cross, rank_value, memory_len),
        [(big, f32), (big, bf16), (head_rows, bf16), (head_rows, bf16), (big, f32), (big, bf16)],
        flops=6 * product,
        smem=(12, 13),
    )
    ups_far = after(ups_far, normed_three)
    ups = (cotangent, swap_core(cotangent), ups_far, swap_core(ups_far))
    many = 4 * rows
    far = swap_chip(normed_three)
    hidden = call(feed_hidden, (*ups, feed_output), [((many, units), f32)], flops=4 * product)[0]

    def feed_half(base, pair):
        return call(
            functools.partial(feed_main, base),
            (*pair, hidden, feed_input),
            [(big, f32), (big, bf16), ((2 * rows, units), bf16), ((2 * rows, units), bf16)],
            flops=4 * product,
        )

    gathered = (normed_three, swap_core(normed_three))
    own, send, act_a, pre_grad_a = feed_half(0, gathered)
    near = swap_core(send)
    far = after(far, near)
    gathered = (*gathered, far, swap_core(far))
    chip, send, act_b, pre_grad_b = feed_half(2 * rows, gathered[2:])
    far_send = core_sum(chip, swap_core(send))
    far = swap_chip(far_send)
    out_own, out_chip, out_send, low, high = call(
        feed_rest,
        (*gathered, *ups, act_a, after(act_b, far_send), pre_grad_a, pre_grad_b, feed_output, turn),
        [(big, f32), (big, f32), pack] + [grad_half(2, d)] * 2,
        [grad_rows(2, d)],
        flops=12 * product,
        smem=(13,),
    )
    chains = Chains()
    token = chains.start("zero", dp_chain(low, high, early=True))
    far = after(far, token)
    grad_one, up_one, key_grad, value_grad, late_gains, keep, send = call(
        cross_backward,
        (own, near, far, cotangent, after_cross, after_self, cross_gain, feed_gain)
        + (normed_two, cross_q, cross_k, cross_v, cross_mixed, *cross, rank_value, memory_len, turn),
        [(big, f32), (big, bf16), (heads_key, bf16), (heads_key, bf16), ((2, d), f32)] + [grad_rows(2, width, (2,))] * 2,
        [(head_rows, bf16), (head_rows, bf16)],
        flops=16 * product,
        smem=(17, 18, 19),
    )
    up_far = swap_chip(up_one)
    keep, send = call(
        memory_weights,
        (key_grad, value_grad, memory, keep, send, turn),
        [grad_rows(4, width, (2,))] * 2,
        flops=8 * product,
        smem=(5,),
    )
    up_far = after(up_far, keep)
    chains.tokens = (up_far,)
    token = chains.turn("zero")
    got = swap_core(after(send, *token))
    one_send = core_sum(keep[1], got[1])
    one_far = swap_chip(one_send)
    self_ups = (up_one, swap_core(up_one), after(up_far, one_send), swap_core(up_far))
    low, high, sums, own, chip, send = call(
        self_backward,
        (*self_ups, *ones, *self_a, *self_b)
        + (*self_weights, by_distance, rank_value, target_len, turn),
        [grad_half(4, width)] * 2 + [((8, TGT_LEN), f32), (big, f32), (big, f32), pack],
        [square, square] + [(group_heads, bf16)] * 4 + [grad_rows(4, width)],
        flops=10 * product,
        smem=(21, 22, 23),
    )
    chains.tokens = (sums,)
    token = chains.turn("zero")
    token = chains.start("two", dp_chain(low, after(high, *token)))
    got_self = swap_core(after(send, token))
    far_send = core_sum(chip, got_self[1])
    far = swap_chip(far_send)
    one_sum = keep[0].astype(f32) + got[0].astype(f32) + after(one_far, far_send).astype(f32)
    one_sum = one_sum.astype(bf16)
    token = chains.start("one", dp_chain(one_sum[: blocks // 2], one_sum[blocks // 2 :]))
    memory_grad = call(
        memory_backward,
        (after(key_grad, token), value_grad, *cross),
        [((key_rows, d), f32)],
        flops=8 * product,
    )[0]
    chains.tokens = (memory_grad,)
    chains.turn("zero")
    token = chains.turn("two")
    inputs_grad, small = call(
        last_norm,
        (grad_one, own, got_self[0], after(far, *token), inputs, self_gain, late_gains, sums, rank_value),
        [(big, f32), ((40, d), f32)],
        smem=(8,),
    )
    chains.start("small", sum_all(small))
    got_out = swap_core(after(out_send, inputs_grad))
    out_far = swap_chip(core_sum(out_chip, got_out[1]))
    chains.tokens = (inputs_grad,)
    for names in ROUNDS:
        chains.turn(*names)
    grads = {}
    for name in ("small", "two", "one", "zero"):
        while name in chains.under_way:
            chains.turn(name)
        if name == "small":
            continue
        early, size, count = {"two": (False, width, 4), "one": (False, width, 4), "zero": (True, d, 2)}[name]
        grads[name] = call(
            functools.partial(finish, early), (*chains.last[name], turn), [((size, d), f32)] * count, smem=(2,)
        )
        chains.tokens = (grads[name][0],)
    total = chains.last
    layer_out = (after_cross + out_own + got_out[0].astype(f32) + out_far.astype(f32)).astype(bf16)
    feed_grads, cross_grads, self_grads = grads["zero"], grads["one"], grads["two"]
    gains = total["small"][:3]
    own_sums = lax.dynamic_slice(total["small"], (8 * (rank + 1), 0), (heads, TGT_LEN))
    bias_grad = lax.dot_general(hot, own_sums, (((0,), (1,)), ((), ())), precision=highest)

    return (
        layer_out,
        inputs_grad,
        memory_grad,
        gains[0],
        self_grads[0].T,
        self_grads[1].T,
        self_grads[2].T,
        self_grads[3],
        bias_grad,
        gains[1],
        cross_grads[0].T,
        cross_grads[2].T,
        cross_grads[3].T,
        cross_grads[1],
        gains[2],
        *feed_grads,
    )


def solution(mesh):
    in_specs = (
        P(("dp", "mp"), None),
        P(("dp", "mp"), None),
        P("dp"),
        P("dp"),
        P(),
        P(),
        P(None, "mp"),
        P(None, "mp"),
        P(None, "mp"),
        P("mp", None),
        P(None, "mp"),
        P(),
        P(None, "mp"),
        P(None, "mp"),
        P(None, "mp"),
        P("mp", None),
        P(),
        P(None, "mp"),
        P("mp", None),
        P(("dp", "mp"), None),
    )
    out_specs = (
        P(("dp", "mp"), None),
        P(("dp", "mp"), None),
        P(("dp", "mp"), None),
        P(),
        P(None, "mp"),
        P(None, "mp"),
        P(None, "mp"),
        P("mp", None),
        P(None, "mp"),
        P(),
        P(None, "mp"),
        P(None, "mp"),
        P(None, "mp"),
        P("mp", None),
        P(),
        P(None, "mp"),
        P("mp", None),
    )
    return jax.shard_map(body, mesh=mesh, in_specs=in_specs, out_specs=out_specs, check_vma=False)
```

```python
import functools

import jax
import jax.numpy as jnp
from jax import lax
from jax.experimental import pallas as pl
from jax.experimental.pallas import tpu as pltpu
from jax.sharding import PartitionSpec as P

HEAD_DIM = 64
PAIR = 2 * HEAD_DIM
BUCKETS = 32
TGT_LEN = 128
MEM_LEN = 512

masked_fill = -1000000000.0
epsilon = 1e-06
highest = lax.Precision.HIGHEST
tanh_scale = 0.7978845608
cubic_term = 0.044715
bf16 = jnp.bfloat16
f32 = jnp.float32


def dot_nn(a, b):
    return lax.dot_general(a, b, (((1,), (0,)), ((), ())), preferred_element_type=f32)


def dot_nt(a, b):
    return lax.dot_general(a, b, (((1,), (1,)), ((), ())), preferred_element_type=f32)


def dot_tn(a, b):
    return lax.dot_general(a, b, (((0,), (0,)), ((), ())), preferred_element_type=f32)


def row_scale(hidden):
    return lax.rsqrt(jnp.mean(hidden * hidden, -1, keepdims=True) + epsilon)


def norm_backward(hidden, scale, gain, upstream):
    weighted = gain * upstream
    return scale * weighted - hidden * (scale * scale * scale) * jnp.mean(hidden * weighted, -1, keepdims=True)


def matrix(blocks, index, width):
    return jnp.concatenate([b[index * width : (index + 1) * width, :] for b in blocks], 0)


def store_rows(ref, lead, index, grad, turn):
    blocks = ref.shape[len(lead)]
    size = grad.shape[0] // blocks
    for a in range(blocks):
        ref[(*lead, a ^ turn, slice(index * size, (index + 1) * size))] = grad[a * size : (a + 1) * size].astype(bf16)


def store_extra(ref, lead, start, rows, turn):
    for a in range(ref.shape[len(lead)]):
        ref[(*lead, a ^ turn, slice(start, start + EXTRA))] = (rows if a == 0 else jnp.zeros_like(rows)).astype(bf16)


EXTRA = 8


def first_of(turn_ref):
    return turn_ref[1] == 0


def passed_on(blocks, first, index):
    own, core, far, far_y, both, both_y = blocks
    width = far.shape[0]
    rows = slice(index * width, (index + 1) * width)
    straight = first == (index == 0)
    pieces = [own[rows, :], core[rows, :]]
    for here, there in ((far, far_y), (both, both_y)):
        pieces.append(jnp.where(straight, here[...], there[...]))
    return jnp.concatenate(pieces, 0)


def store_halves(low_ref, high_ref, ref):
    half = ref.shape[0] // 2
    low_ref[...] = ref[:half]
    high_ref[...] = ref[half:]


def store_grad(keep_ref, send_ref, index, grad, turn):
    width = grad.shape[0] // 4
    for j in range(4):
        store_rows((keep_ref, send_ref)[j % 2], (j // 2,), index, grad[j * width : (j + 1) * width], turn)


def pair_masks():
    lane = lax.broadcasted_iota(jnp.int32, (1, PAIR), 1)
    return (lane < HEAD_DIM).astype(bf16), (lane >= HEAD_DIM).astype(bf16)


def stack_pair(rows, masks):
    return jnp.concatenate([rows * masks[0], rows * masks[1]], 0)


def unstack_pair(both):
    lane = lax.broadcasted_iota(jnp.int32, (TGT_LEN, PAIR), 1)
    return jnp.where(lane < HEAD_DIM, both[:TGT_LEN], both[TGT_LEN:])


def softmax_rows(scores):
    weights = jnp.exp(scores - jnp.max(scores, -1, keepdims=True))
    return weights * (1.0 / jnp.sum(weights, -1, keepdims=True))


def locate(step, pairs, keys):
    example = lax.div(step, pairs)
    pair = lax.rem(step, pairs)
    rows = pl.ds(pl.multiple_of(example * TGT_LEN, TGT_LEN), TGT_LEN)
    key_rows = pl.ds(pl.multiple_of(example * keys, keys), keys)
    cols = pl.ds(pl.multiple_of(pair * PAIR, PAIR), PAIR)
    return example, pair, rows, key_rows, cols


def cross_probs(queries, key_rows, length):
    scores = dot_nt(queries, key_rows)
    key = lax.broadcasted_iota(jnp.int32, scores.shape, 1)
    return softmax_rows(jnp.where(key < length, scores, masked_fill))


def attend(q_ref, k_ref, v_ref, mixed_ref, keys, probs_of):
    masks = pair_masks()
    pairs = q_ref.shape[1] // PAIR
    examples = q_ref.shape[0] // TGT_LEN

    def step(i, carry):
        example, pair, rows, key_rows, cols = locate(i, pairs, keys)
        probs = probs_of(stack_pair(q_ref[rows, cols], masks), k_ref[key_rows, cols], example, pair)
        mixed = dot_nn(probs.astype(bf16), v_ref[key_rows, cols])
        mixed_ref[rows, cols] = unstack_pair(mixed).astype(bf16)
        return carry

    lax.fori_loop(0, examples * pairs, step, 0, unroll=2)


def attend_back(q_ref, k_ref, v_ref, m_ref, dq_ref, dk_ref, dv_ref, keys, probs_of):
    masks = pair_masks()
    pairs = q_ref.shape[1] // PAIR
    examples = q_ref.shape[0] // TGT_LEN

    def step(i, carry):
        example, pair, rows, key_rows, cols = locate(i, pairs, keys)
        queries = stack_pair(q_ref[rows, cols], masks)
        grads = stack_pair(m_ref[rows, cols], masks)
        key_block = k_ref[key_rows, cols]
        probs = probs_of(queries, key_block, example, pair)
        dv_ref[cols, key_rows] = dot_tn(grads, probs.astype(bf16)).astype(bf16)
        prob_grad = dot_nt(grads, v_ref[key_rows, cols])
        score_grad = probs * (prob_grad - jnp.sum(probs * prob_grad, -1, keepdims=True))
        low = score_grad.astype(bf16)
        dq_ref[rows, cols] = unstack_pair(dot_nn(low, key_block)).astype(bf16)
        dk_ref[cols, key_rows] = dot_tn(queries, low).astype(bf16)
        return carry

    lax.fori_loop(0, examples * pairs, step, 0, unroll=UNROLL)


UNROLL = 4


def fill_bias(table_ref, bias_ref):
    for head in range(bias_ref.shape[0] // TGT_LEN):
        row = jnp.broadcast_to(table_ref[head : head + 1, :], (TGT_LEN, TGT_LEN))
        bias_ref[head * TGT_LEN : (head + 1) * TGT_LEN, :] = pltpu.roll(row, 0, axis=1, stride=1, stride_axis=0)


def stack_heads(rows):
    lane = lax.broadcasted_iota(jnp.int32, (1, rows.shape[1]), 1)
    heads = rows.shape[1] // HEAD_DIM
    return jnp.concatenate([rows * (lax.div(lane, HEAD_DIM) == h).astype(bf16) for h in range(heads)], 0)


def unstack_heads(stacked):
    length = TGT_LEN
    lane = lax.broadcasted_iota(jnp.int32, (length, stacked.shape[1]), 1)
    out = stacked[:length]
    for h in range(1, stacked.shape[1] // HEAD_DIM):
        out = jnp.where(lane >= h * HEAD_DIM, stacked[h * length : (h + 1) * length], out)
    return out


def self_probs(queries, key_rows, bias, length):
    scores = dot_nt(queries, key_rows) + bias
    key = lax.broadcasted_iota(jnp.int32, scores.shape, 1)
    query = lax.rem(lax.broadcasted_iota(jnp.int32, scores.shape, 0), TGT_LEN)
    return softmax_rows(jnp.where((key <= query) & (key < length), scores, masked_fill))


def diagonal_sums(grad):
    query = lax.broadcasted_iota(jnp.int32, grad.shape, 0)
    for bit in range(TGT_LEN.bit_length() - 1):
        moved = pltpu.roll(grad, TGT_LEN - (1 << bit), axis=1)
        grad = jnp.where((query >> bit) & 1 == 1, moved, grad)
    return jnp.sum(grad, 0, keepdims=True)


def first_norm(x_ref, gain_ref, n_ref):
    hidden = x_ref[...].astype(f32)
    n_ref[...] = (hidden * row_scale(hidden) * gain_ref[...].reshape(1, -1)).astype(bf16)


def self_forward(
    base, n0, n1, wq_ref, wk_ref, wv_ref, wo_ref, table_ref, rank_ref, len_ref,
    q_ref, k_ref, v_ref, mixed_ref, keep_ref, send_ref, bias_ref,
):
    fill_bias(table_ref, bias_ref)
    size = n0.shape[0]
    for j, n in enumerate((n0, n1)):
        rows = slice(j * size, (j + 1) * size)
        for ref, w in ((q_ref, wq_ref), (k_ref, wk_ref), (v_ref, wv_ref)):
            ref[rows, :] = dot_nt(n[...], w[...]).astype(bf16)

    def step(i, carry):
        rows = pl.ds(pl.multiple_of(i * TGT_LEN, TGT_LEN), TGT_LEN)
        length = len_ref[(rank_ref[0] * (size // TGT_LEN)) ^ (base + i)]
        probs = self_probs(stack_heads(q_ref[rows, :]), k_ref[rows, :], bias_ref[...], length)
        mixed_ref[rows, :] = unstack_heads(dot_nn(probs.astype(bf16), v_ref[rows, :])).astype(bf16)
        return carry

    lax.fori_loop(0, 2 * size // TGT_LEN, step, 0, unroll=2)
    keep_ref[...] = dot_nn(mixed_ref[:size, :], wo_ref[...])
    send_ref[...] = dot_nn(mixed_ref[size:, :], wo_ref[...]).astype(bf16)


def store_parts(own_ref, chip_ref, send_ref, parts):
    for j, part in enumerate(parts):
        if j == 0:
            own_ref[...] = part
        elif j == 2:
            chip_ref[...] = part
        else:
            send_ref[j // 2] = part.astype(bf16)


def memory_forward(mem_ref, w0, w1, w2, w3, k_ref, v_ref):
    width = k_ref.shape[1] // 4
    half = mem_ref.shape[0] // 2
    blocks = (w0, w1, w2, w3)

    def step(i, carry):
        rows = pl.ds(pl.multiple_of(i * half, half), half)
        k_ref[rows, :] = dot_nt(mem_ref[rows, :], matrix(blocks, KEY, width)).astype(bf16)
        v_ref[rows, :] = dot_nt(mem_ref[rows, :], matrix(blocks, KEY + 1, width)).astype(bf16)
        return carry

    lax.fori_loop(0, 2, step, 0)


def cross_forward(
    x_ref, own_ref, near_ref, far_ref, k_ref, v_ref, gain_two_ref, gain_three_ref, w0, w1, w2, w3, w4, w5, rank_ref, len_ref, turn_ref,
    after_self_ref, n2_ref, q_ref, mixed_ref, after_ref, n3_ref,
):
    blocks = (w0, w1, w2, w3, w4, w5)
    first = first_of(turn_ref)
    after_self = x_ref[...].astype(f32) + own_ref[...] + near_ref[...].astype(f32) + far_ref[...].astype(f32)
    after_self_ref[...] = after_self
    normed = (after_self * row_scale(after_self) * gain_two_ref[...].reshape(1, -1)).astype(bf16)
    n2_ref[...] = normed
    q_ref[...] = dot_nt(normed, passed_on(blocks, first, 0)).astype(bf16)

    def probs(queries, key_rows, example, pair):
        return cross_probs(queries, key_rows, len_ref[rank_ref[0] * (q_ref.shape[0] // TGT_LEN) + example])

    attend(q_ref, k_ref, v_ref, mixed_ref, MEM_LEN, probs)
    after = after_self_ref[...] + dot_nn(mixed_ref[...], passed_on(blocks, first, 1))
    after_ref[...] = after
    n3_ref[...] = (after * row_scale(after) * gain_three_ref[...].reshape(1, -1)).astype(bf16)


def feed_hidden(c0, c1, c2, c3, out_ref, hidden_ref):
    size = c0.shape[0]
    for base, first, second in ((0, c0, c1), (2 * size, c2, c3)):

        def step(i, carry, base=base, first=first, second=second):
            rows = pl.ds(pl.multiple_of(base + i * size, size), size)
            hidden_ref[rows, :] = dot_nt(jnp.where(i == 0, first[...], second[...]), out_ref[...])
            return carry

        lax.fori_loop(0, 2, step, 0)


def feed_main(base, g0, g1, hidden_ref, in_ref, keep_ref, send_ref, act_ref, pre_grad_ref):
    size = g0.shape[0]
    for j, g in enumerate((g0, g1)):
        rows = slice(j * size, (j + 1) * size)
        pre = dot_nn(g[...], in_ref[...])
        square = pre * pre
        tanh = jnp.tanh(tanh_scale * (pre + cubic_term * square * pre))
        act_ref[rows, :] = (0.5 * pre * (1.0 + tanh)).astype(bf16)
        slope = 0.5 * (1.0 + tanh) + 0.5 * pre * (1.0 - tanh * tanh) * (
            tanh_scale * (1.0 + 3.0 * cubic_term * square)
        )
        low = (hidden_ref[base + j * size : base + (j + 1) * size, :] * slope).astype(bf16)
        pre_grad_ref[rows, :] = low
        grad = dot_nt(low, in_ref[...])
        if j == 0:
            keep_ref[...] = grad
        else:
            send_ref[...] = grad.astype(bf16)


def feed_rest(
    g0, g1, g2, g3, c0, c1, c2, c3, act_a, act_b, pre_grad_a, pre_grad_b, out_ref, turn_ref, own_ref, chip_ref, send_ref, low_ref, high_ref, grads_ref
):
    activated = jnp.concatenate([act_a[...], act_b[...]], 0)
    pre_grad = jnp.concatenate([pre_grad_a[...], pre_grad_b[...]], 0)
    gathered = jnp.concatenate([g[...] for g in (g0, g1, g2, g3)], 0)
    store_rows(grads_ref, (), 0, dot_tn(gathered, pre_grad), turn_ref[0])
    upstream = jnp.concatenate([c[...] for c in (c0, c1, c2, c3)], 0)
    store_rows(grads_ref, (), 1, dot_tn(activated, upstream), turn_ref[0])
    store_halves(low_ref, high_ref, grads_ref)
    size = g0.shape[0]
    for slot, act, keep_ref in ((0, act_a, own_ref), (1, act_b, chip_ref)):

        def step(i, carry, slot=slot, act=act, keep_ref=keep_ref):
            part = dot_nn(act[pl.ds(pl.multiple_of(i * size, size), size), :], out_ref[...])

            @pl.when(i == 0)
            def _():
                keep_ref[...] = part

            @pl.when(i == 1)
            def _():
                send_ref[slot] = part.astype(bf16)

            return carry

        lax.fori_loop(0, 2, step, 0)


def cross_backward(
    own_ref, near_ref, far_ref, cot_ref, after_ref, after_self_ref, gain_two_ref, gain_three_ref,
    n2_ref, q_ref, k_ref, v_ref, mixed_ref, w0, w1, w2, w3, w4, w5, rank_ref, len_ref, turn_ref,
    grad_one_ref, up_ref, dk_ref, dv_ref, gains_ref, keep_ref, send_ref, m_ref, dq_ref,
):
    blocks = (w0, w1, w2, w3, w4, w5)
    first = first_of(turn_ref)
    after = after_ref[...]
    scale = row_scale(after)
    upstream = own_ref[...] + near_ref[...].astype(f32) + far_ref[...].astype(f32)
    gains_ref[1:2, :] = jnp.sum(upstream * after * scale, 0, keepdims=True)
    grad_two = cot_ref[...].astype(f32) + norm_backward(after, scale, gain_three_ref[...].reshape(1, -1), upstream)
    grad_one_ref[...] = grad_two
    up_two = grad_two.astype(bf16)
    m_ref[...] = dot_nt(up_two, passed_on(blocks, first, 1)).astype(bf16)
    store_grad(keep_ref, send_ref, 1, dot_tn(mixed_ref[...], up_two), turn_ref[0])

    def probs(queries, key_rows, example, pair):
        return cross_probs(queries, key_rows, len_ref[rank_ref[0] * (q_ref.shape[0] // TGT_LEN) + example])

    attend_back(q_ref, k_ref, v_ref, m_ref, dq_ref, dk_ref, dv_ref, MEM_LEN, probs)
    store_grad(keep_ref, send_ref, 0, dot_tn(dq_ref[...], n2_ref[...]), turn_ref[0])
    upstream = dot_nn(dq_ref[...], passed_on(blocks, first, 0))
    hidden = after_self_ref[...]
    scale = row_scale(hidden)
    gains_ref[0:1, :] = jnp.sum(upstream * hidden * scale, 0, keepdims=True)
    grad_one = grad_one_ref[...] + norm_backward(hidden, scale, gain_two_ref[...].reshape(1, -1), upstream)
    grad_one_ref[...] = grad_one
    up_ref[...] = grad_one.astype(bf16)


def memory_weights(dk_ref, dv_ref, mem_ref, keep_in, send_in, late_ref, turn_ref, keep_ref, send_ref):
    count = keep_in.shape[2]
    late = jnp.concatenate([late_ref[...], jnp.zeros((EXTRA - 2, late_ref.shape[1]), f32)], 0)
    for j in range(2):
        for ref, given in ((keep_ref, keep_in), (send_ref, send_in)):
            for a in range(keep_in.shape[1]):
                ref[j, a, :count] = given[j, a]
            store_extra(ref, (j,), 2 * count, late, turn_ref[0])
    store_grad(keep_ref, send_ref, 2, dot_nn(dk_ref[...], mem_ref[...]), turn_ref[0])
    store_grad(keep_ref, send_ref, 3, dot_nn(dv_ref[...], mem_ref[...]), turn_ref[0])


def self_backward(
    u0, u1, u2, u3, n0, n1, n2, n3, qa, ka, va, xa, qb, kb, vb, xb, wq_ref, wk_ref, wv_ref, wo_ref, gain_ref,
    table_ref, rank_ref, len_ref, turn_ref,
    low_ref, high_ref, own_ref, chip_ref, send_ref,
    bias_ref, score_ref, m_ref, dq_ref, dk_ref, dv_ref, grads_ref,
):
    fill_bias(table_ref, bias_ref)
    score_ref[...] = jnp.zeros_like(score_ref)
    size = n0.shape[0]
    width = qa.shape[1]
    for j, u in enumerate((u0, u1, u2, u3)):
        m_ref[j * size : (j + 1) * size, :] = dot_nt(u[...], wo_ref[...]).astype(bf16)

    for base, q_ref, k_ref, v_ref in ((0, qa, ka, va), (2 * size, qb, kb, vb)):

        def step(i, carry, base=base, q_ref=q_ref, k_ref=k_ref, v_ref=v_ref):
            rows = pl.ds(pl.multiple_of(i * TGT_LEN, TGT_LEN), TGT_LEN)
            all_rows = pl.ds(pl.multiple_of(base + i * TGT_LEN, TGT_LEN), TGT_LEN)
            length = len_ref[(rank_ref[0] * (size // TGT_LEN)) ^ (base // TGT_LEN + i)]
            queries = stack_heads(q_ref[rows, :])
            grads = stack_heads(m_ref[all_rows, :])
            key_block = k_ref[rows, :]
            probs = self_probs(queries, key_block, bias_ref[...], length)
            dv_ref[all_rows, :] = dot_tn(probs.astype(bf16), grads).astype(bf16)
            prob_grad = dot_nt(grads, v_ref[rows, :])
            score_grad = probs * (prob_grad - jnp.sum(probs * prob_grad, -1, keepdims=True))
            score_ref[...] += score_grad
            low = score_grad.astype(bf16)
            dq_ref[all_rows, :] = unstack_heads(dot_nn(low, key_block)).astype(bf16)
            dk_ref[all_rows, :] = dot_tn(low, queries).astype(bf16)
            return carry

        lax.fori_loop(0, 2 * size // TGT_LEN, step, 0, unroll=2)
    normed = jnp.concatenate([n[...] for n in (n0, n1, n2, n3)], 0)
    upstream = jnp.concatenate([u[...] for u in (u0, u1, u2, u3)], 0)
    mixed = jnp.concatenate([xa[...], xb[...]], 0)
    for index, (left, right) in enumerate(
        ((dq_ref[...], normed), (dk_ref[...], normed), (dv_ref[...], normed), (mixed, upstream))
    ):
        store_rows(grads_ref, (), index, dot_tn(left, right), turn_ref[0])
    gain = jnp.zeros((1, n0.shape[1]), f32)
    parts = []
    for j, n in enumerate((n0, n1, n2, n3)):
        rows = slice(j * size, (j + 1) * size)
        part = dot_nn(dq_ref[rows, :], wq_ref[...])
        part = part + dot_nn(dk_ref[rows, :], wk_ref[...]) + dot_nn(dv_ref[rows, :], wv_ref[...])
        gain += jnp.sum(part * n[...].astype(f32), 0, keepdims=True)
        if j == 0:
            own_ref[...] = part
        elif j == 2:
            chip_ref[...] = part
        else:
            send_ref[j // 2] = part.astype(bf16)
    gain = gain * (1.0 / gain_ref[...].reshape(1, -1))
    heads = width // HEAD_DIM
    sums = [diagonal_sums(score_ref[h * TGT_LEN : (h + 1) * TGT_LEN, :]) for h in range(heads)]
    sums = jnp.concatenate(sums + [jnp.zeros((EXTRA - 1 - heads, TGT_LEN), f32)], 0)
    sums = jnp.concatenate([sums, jnp.zeros((EXTRA - 1, gain.shape[1] - TGT_LEN), f32)], 1)
    store_extra(grads_ref, (), 4 * (width // grads_ref.shape[0]), jnp.concatenate([gain, sums], 0), turn_ref[0])
    store_halves(low_ref, high_ref, grads_ref)


def last_norm(grad_one_ref, own_ref, near_ref, far_ref, x_ref, gain_ref, grad_ref):
    upstream = own_ref[...] + near_ref[...].astype(f32) + far_ref[...].astype(f32)
    hidden = x_ref[...].astype(f32)
    grad_ref[...] = grad_one_ref[...] + norm_backward(hidden, row_scale(hidden), gain_ref[...].reshape(1, -1), upstream)


def gather_order(bits, early):
    return [0, bits - 1, *range(1, bits - 1)] if early else list(range(bits))


def gather_rows(low_ref, high_ref, rows, places, turn, early):
    half = low_ref.shape[0]
    order = gather_order((2 * half).bit_length() - 1, early)
    pieces = []
    for a in places:
        place = a ^ turn
        inside = sum(((place >> bit) & 1) << i for i, bit in enumerate(order[:-1]))
        low = (place >> order[-1]) & 1 == 0
        pieces.append(jnp.where(low, low_ref[inside, rows].astype(f32), high_ref[inside, rows].astype(f32)))
    return jnp.concatenate(pieces, 0)


def finish(early, low_ref, high_ref, turn_ref, *outs):
    blocks = 2 * low_ref.shape[0]
    start = 0
    for ref in outs:
        extra = ref.shape[0] == EXTRA
        places = range(1) if extra else range(blocks)
        size = EXTRA if extra else ref.shape[0] // blocks
        ref[...] = gather_rows(low_ref, high_ref, slice(start, start + size), places, turn_ref[0], early)
        start += size


def memory_backward(dk_ref, dv_ref, w0, w1, w2, w3, grad_ref):
    blocks = (w0, w1, w2, w3)
    width = dk_ref.shape[0] // 4
    half = grad_ref.shape[0] // 2

    def step(i, carry):
        rows = pl.ds(pl.multiple_of(i * half, half), half)
        keys = dot_tn(dk_ref[:, rows], matrix(blocks, KEY, width))
        grad_ref[rows, :] = keys + dot_tn(dv_ref[:, rows], matrix(blocks, KEY + 1, width))
        return carry

    lax.fori_loop(0, 2, step, 0)


KEY = 0


def call(kernel, operands, outs, scratch=(), flops=0, smem=()):
    moved = sum(a.size * a.dtype.itemsize for a in operands)
    moved += sum(functools.reduce(lambda x, y: x * y, s) * jnp.dtype(t).itemsize for s, t in outs)
    return pl.pallas_call(
        kernel,
        out_shape=[jax.ShapeDtypeStruct(s, t) for s, t in outs],
        in_specs=[
            pl.BlockSpec(memory_space=pltpu.SMEM if i in smem else pltpu.VMEM) for i in range(len(operands))
        ],
        out_specs=[pl.BlockSpec(memory_space=pltpu.VMEM) for _ in outs],
        scratch_shapes=[pltpu.VMEM(s, t) for s, t in scratch],
        compiler_params=pltpu.CompilerParams(vmem_limit_bytes=VMEM_LIMIT),
        cost_estimate=pl.CostEstimate(flops=flops, bytes_accessed=moved, transcendentals=0),
    )(*operands)


VMEM_LIMIT = 56 * 1024 * 1024


def after(value, *others):
    return lax.optimization_barrier((value, *others))[0]


def swap_core(a):
    return lax.ppermute(a, "mp", [(0, 1), (1, 0), (2, 3), (3, 2)])


def swap_chip(a):
    return lax.ppermute(a, "mp", [(0, 2), (2, 0), (1, 3), (3, 1)])


def gather_blocks(a):
    far = swap_chip(a)
    return (a, swap_core(a), far, swap_core(far))


def core_sum(chip, got):
    return (chip.astype(f32) + got.astype(f32)).astype(bf16)


def plus(a, b):
    return (a.astype(f32) + b.astype(f32)).astype(bf16)


def swap_dp(a, bit):
    return lax.ppermute(a, "dp", [(i, i ^ (1 << bit)) for i in range(lax.axis_size("dp"))])


def dp_chain(keep, send, steps=None):
    bits = lax.axis_size("dp").bit_length() - 1
    for bit in range(bits):
        got = swap_dp(send, bit)
        tokens = yield send
        got = after(got, *tokens)
        half = keep.shape[0] // 2
        if half:
            send, keep = plus(keep[half:], got[half:]), plus(keep[:half], got[:half])
        else:
            value = plus(keep, got)
    yield from gather_chain(value, range(bits)[:steps])


def gather_chain(value, order):
    bits = lax.axis_size("dp").bit_length() - 1
    order = list(order)
    for bit in order:
        other = swap_dp(value, bits - 1 - bit)
        tokens = yield value
        other = after(other, *tokens)
        if bit != order[-1]:
            value = jnp.concatenate([value, other], 0)
    yield value, other


ROUNDS = (
    ("zero",),
    ("two",),
    ("two",),
    ("zero", "one"),
    ("two", "one"),
)
LATE_ROUNDS = (
    ("two", "one"),
    ("in", "out"),
    ("two",),
    ("one",),
)
FINISH = ("in", "out", "one", "two", "one+")


class Chains:
    def __init__(self):
        self.under_way, self.last, self.tokens = {}, {}, ()

    def start(self, name, chain):
        self.under_way[name] = chain
        self.last[name] = next(chain)
        return self.last[name]

    def turn(self, *names):
        sent = []
        for name in names:
            try:
                self.last[name] = self.under_way[name].send(self.tokens)
                sent.append(self.last[name])
            except (StopIteration, KeyError):
                self.under_way.pop(name, None)
        if sent:
            self.tokens = tuple(t for t in sent if not isinstance(t, tuple)) or sent[0]
        return self.tokens

    def drain(self):
        while self.under_way:
            for name in list(self.under_way):
                self.turn(name)


def body(
    inputs,
    memory,
    target_len,
    memory_len,
    bucket_map,
    self_gain,
    self_query,
    self_key,
    self_value,
    self_out,
    bias_table,
    cross_gain,
    cross_query,
    cross_key,
    cross_value,
    cross_out,
    feed_gain,
    feed_input,
    feed_output,
    cotangent,
):
    rank = lax.axis_index("mp")
    rows, d = inputs.shape
    key_rows = memory.shape[0]
    width = self_query.shape[1]
    wide = 4 * width
    heads = bias_table.shape[1]
    units = feed_input.shape[1]
    examples = rows // TGT_LEN
    rank_value = rank.astype(jnp.int32).reshape(1)
    blocks = lax.axis_size("dp")
    place = lax.axis_index("dp").astype(jnp.int32)
    turn = jnp.zeros((1,), jnp.int32)
    for bit in range(blocks.bit_length() - 1):
        turn = 2 * turn + ((place >> bit) & 1)
    turn = jnp.concatenate([turn, (place & 1).reshape(1)])

    distance = (TGT_LEN - jnp.arange(TGT_LEN, dtype=jnp.int32)) % TGT_LEN
    lookup = distance[:, None] == jnp.arange(TGT_LEN, dtype=jnp.int32)[None, :]
    bucket = jnp.sum(jnp.where(lookup, bucket_map[None, :], 0), -1)
    hot = (bucket[:, None] == jnp.arange(BUCKETS, dtype=jnp.int32)[None, :]).astype(f32)
    by_distance = lax.dot_general(bias_table, hot, (((0,), (1,)), ((), ())), precision=highest)
    big = (rows, d)
    head_rows = (rows, wide)
    key_heads = (key_rows, wide)
    heads_key = (wide, key_rows)
    square = ((heads * TGT_LEN, TGT_LEN), f32)
    group_heads = (4 * rows, width)
    half_heads = (2 * rows, width)
    pack = ((2, rows, d), bf16)
    product = 2 * rows * d * wide

    def grad_half(count, size, more=0):
        return ((blocks // 2, count * (size // blocks) + more, d), bf16)

    def grad_rows(count, size, lead=(), more=0):
        return ((*lead, blocks, count * (size // blocks) + more, d), bf16)

    pair_own = jnp.concatenate([cross_key.T, cross_value.T], 0)
    query_own = jnp.concatenate([cross_query.T, cross_out], 0)
    half_own = lax.dynamic_slice_in_dim(query_own, (place & 1) * width, width, 0)
    normed_one = call(first_norm, (inputs, self_gain), [(big, bf16)])[0]
    far = swap_chip(normed_one)
    pair_far = swap_chip(after(pair_own, normed_one))
    self_weights = (self_query.T, self_key.T, self_value.T, self_out)

    def self_half(base, pair):
        return call(
            functools.partial(self_forward, base),
            (*pair, *self_weights, by_distance, rank_value, target_len),
            [(half_heads, bf16)] * 4 + [(big, f32), (big, bf16)],
            [square],
            flops=2 * product,
            smem=(7, 8),
        )

    ones = (normed_one, swap_core(normed_one))
    *self_a, own, send = self_half(0, ones)
    near = swap_core(send)
    far = after(far, near)
    ones = (*ones, far, swap_core(far))
    *self_b, chip, send = self_half(2 * rows // TGT_LEN, ones[2:])
    pair_far = after(pair_far, chip)
    half_far = swap_chip(after(half_own, normed_one))
    far_send = core_sum(chip, swap_core(after(send, pair_far)))
    far = swap_chip(far_send)
    pair = (pair_own, swap_core(pair_own), pair_far, swap_core(pair_far))
    cross_k, cross_v = call(
        memory_forward, (after(memory, far_send), *pair), [(key_heads, bf16)] * 2, flops=8 * product
    )
    half_far = after(half_far, cross_v)
    half_passed = swap_dp(half_far, 0)
    far = after(far, half_far)
    half_passed = after(half_passed, far)
    query = (query_own, swap_core(query_own), half_far, half_passed, swap_core(half_far), swap_core(half_passed))
    ups_far = swap_chip(after(cotangent, far))
    after_self, normed_two, cross_q, cross_mixed, after_cross, normed_three = call(
        cross_forward,
        (inputs, own, near, far, cross_k, cross_v, cross_gain, feed_gain, *query, rank_value, memory_len, turn),
        [(big, f32), (big, bf16), (head_rows, bf16), (head_rows, bf16), (big, f32), (big, bf16)],
        flops=6 * product,
        smem=(14, 15, 16),
    )
    ups_far = after(ups_far, normed_three)
    ups = (cotangent, swap_core(cotangent), ups_far, swap_core(ups_far))
    many = 4 * rows
    far = swap_chip(normed_three)
    hidden = call(feed_hidden, (*ups, feed_output), [((many, units), f32)], flops=4 * product)[0]

    def feed_half(base, pair):
        return call(
            functools.partial(feed_main, base),
            (*pair, hidden, feed_input),
            [(big, f32), (big, bf16), ((2 * rows, units), bf16), ((2 * rows, units), bf16)],
            flops=4 * product,
        )

    gathered = (normed_three, swap_core(normed_three))
    own, send, act_a, pre_grad_a = feed_half(0, gathered)
    near = swap_core(send)
    far = after(far, near)
    gathered = (*gathered, far, swap_core(far))
    chip, send, act_b, pre_grad_b = feed_half(2 * rows, gathered[2:])
    far_send = core_sum(chip, swap_core(send))
    far = swap_chip(far_send)
    out_own, out_chip, out_send, low, high = call(
        feed_rest,
        (*gathered, *ups, act_a, after(act_b, far_send), pre_grad_a, pre_grad_b, feed_output, turn),
        [(big, f32), (big, f32), pack] + [grad_half(2, d)] * 2,
        [grad_rows(2, d)],
        flops=12 * product,
        smem=(13,),
    )
    chains = Chains()
    token = chains.start("zero", dp_chain(low, high, steps=1))
    far = after(far, token)
    grad_one, up_one, key_grad, value_grad, late_gains, keep, send = call(
        cross_backward,
        (own, near, far, cotangent, after_cross, after_self, cross_gain, feed_gain)
        + (normed_two, cross_q, cross_k, cross_v, cross_mixed, *query, rank_value, memory_len, turn),
        [(big, f32), (big, bf16), (heads_key, bf16), (heads_key, bf16), ((2, d), f32)] + [grad_rows(2, width, (2,))] * 2,
        [(head_rows, bf16), (head_rows, bf16)],
        flops=16 * product,
        smem=(19, 20, 21),
    )
    up_far = swap_chip(up_one)
    keep, send = call(
        memory_weights,
        (key_grad, value_grad, memory, keep, send, late_gains, turn),
        [grad_rows(4, width, (2,), EXTRA)] * 2,
        flops=8 * product,
        smem=(6,),
    )
    up_far = after(up_far, keep)
    chains.tokens = (up_far,)
    token = chains.turn("zero")
    got = swap_core(after(send, *token))
    one_send = core_sum(keep[1], got[1])
    one_far = swap_chip(one_send)
    self_ups = (up_one, swap_core(up_one), after(up_far, one_send), swap_core(up_far))
    low, high, own, chip, send = call(
        self_backward,
        (*self_ups, *ones, *self_a, *self_b)
        + (*self_weights, self_gain, by_distance, rank_value, target_len, turn),
        [grad_half(4, width, EXTRA)] * 2 + [(big, f32), (big, f32), pack],
        [square, square] + [(group_heads, bf16)] * 4 + [grad_rows(4, width, (), EXTRA)],
        flops=10 * product,
        smem=(22, 23, 24),
    )
    chains.tokens = (own,)
    token = chains.turn("zero")
    token = chains.start("two", dp_chain(low, after(high, *token)))
    got_self = swap_core(after(send, token))
    far_send = core_sum(chip, got_self[1])
    far = swap_chip(far_send)
    one_sum = keep[0].astype(f32) + got[0].astype(f32) + after(one_far, far_send).astype(f32)
    one_sum = one_sum.astype(bf16)
    token = chains.start("one", dp_chain(one_sum[: blocks // 2], one_sum[blocks // 2 :]))
    memory_grad = call(
        memory_backward,
        (after(key_grad, token), value_grad, *pair),
        [((key_rows, d), f32)],
        flops=8 * product,
    )[0]
    chains.tokens = (memory_grad,)
    more = blocks.bit_length() - 1 - 3
    for _ in range(more):
        chains.turn("zero")
    for names in ROUNDS:
        chains.turn(*names)
        if "feed" not in chains.last and isinstance(chains.last["zero"], tuple):
            bits = blocks.bit_length() - 1
            both = jnp.concatenate(chains.last["zero"], 0)
            half = both.shape[1] // 2
            chains.last["feed"] = None
            chains.start("in", gather_chain(both[:, :half], gather_order(bits, True)[1:]))
            chains.start("out", gather_chain(both[:, half:], gather_order(bits, False)[1:]))
    inputs_grad = call(
        last_norm,
        (grad_one, own, got_self[0], after(far, *chains.tokens), inputs, self_gain),
        [(big, f32)],
    )[0]
    chains.tokens = (inputs_grad,)
    got_out = swap_core(after(out_send, *chains.tokens))
    out_far = swap_chip(core_sum(out_chip, got_out[1]))
    for _ in range(2 * more):
        chains.turn("two", "one")
    for names in LATE_ROUNDS:
        chains.turn(*names)
    grads = {}
    for name in FINISH:
        if name == "in":
            for _ in range(more):
                chains.turn("in", "out")
            chains.turn("in", "out")
        elif name == "one":
            chains.turn("one")
            continue
        elif name == "two":
            chains.turn("two", "one")
        name = name.strip("+")
        feed = name in ("in", "out")
        outs = [((d, d), f32)] if feed else [((width, d), f32)] * 4 + [((EXTRA, d), f32)]
        grads[name] = call(
            functools.partial(finish, name == "in"), (*chains.last[name], turn), outs, smem=(2,)
        )
        if feed or name == "one":
            chains.tokens = (grads[name][-1],)
    extra = grads["two"][-1]
    gain_one = after(extra[:1], *chains.tokens)
    gain_one = gain_one + swap_core(gain_one)
    gain_one = gain_one + swap_chip(gain_one)
    layer_out = (after_cross + out_own + got_out[0].astype(f32) + out_far.astype(f32)).astype(bf16)
    feed_grads, cross_grads, self_grads = (grads["in"][0], grads["out"][0]), grads["one"], grads["two"]
    own_sums = extra[1 : 1 + heads, :TGT_LEN]
    bias_grad = lax.dot_general(hot, own_sums, (((0,), (1,)), ((), ())), precision=highest)

    return (
        layer_out,
        inputs_grad,
        memory_grad,
        gain_one[0],
        self_grads[0].T,
        self_grads[1].T,
        self_grads[2].T,
        self_grads[3],
        bias_grad,
        cross_grads[4][0],
        cross_grads[0].T,
        cross_grads[2].T,
        cross_grads[3].T,
        cross_grads[1],
        cross_grads[4][1],
        *feed_grads,
    )


def solution(mesh):
    in_specs = (
        P(("dp", "mp"), None),
        P(("dp", "mp"), None),
        P("dp"),
        P("dp"),
        P(),
        P(),
        P(None, "mp"),
        P(None, "mp"),
        P(None, "mp"),
        P("mp", None),
        P(None, "mp"),
        P(),
        P(None, "mp"),
        P(None, "mp"),
        P(None, "mp"),
        P("mp", None),
        P(),
        P(None, "mp"),
        P("mp", None),
        P(("dp", "mp"), None),
    )
    out_specs = (
        P(("dp", "mp"), None),
        P(("dp", "mp"), None),
        P(("dp", "mp"), None),
        P(),
        P(None, "mp"),
        P(None, "mp"),
        P(None, "mp"),
        P("mp", None),
        P(None, "mp"),
        P(),
        P(None, "mp"),
        P(None, "mp"),
        P(None, "mp"),
        P("mp", None),
        P(),
        P(None, "mp"),
        P("mp", None),
    )
    return jax.shard_map(body, mesh=mesh, in_specs=in_specs, out_specs=out_specs, check_vma=False)
```

```python
import functools

import jax
import jax.numpy as jnp
from jax import lax
from jax.experimental import pallas as pl
from jax.experimental.pallas import tpu as pltpu
from jax.sharding import PartitionSpec as P

HEAD_DIM = 64
PAIR = 2 * HEAD_DIM
BUCKETS = 32
TGT_LEN = 128
MEM_LEN = 512

masked_fill = -1000000000.0
epsilon = 1e-06
highest = lax.Precision.HIGHEST
tanh_scale = 0.7978845608
cubic_term = 0.044715
bf16 = jnp.bfloat16
f32 = jnp.float32


def dot_nn(a, b):
    return lax.dot_general(a, b, (((1,), (0,)), ((), ())), preferred_element_type=f32)


def dot_nt(a, b):
    return lax.dot_general(a, b, (((1,), (1,)), ((), ())), preferred_element_type=f32)


def dot_tn(a, b):
    return lax.dot_general(a, b, (((0,), (0,)), ((), ())), preferred_element_type=f32)


def row_scale(hidden):
    return lax.rsqrt(jnp.mean(hidden * hidden, -1, keepdims=True) + epsilon)


def norm_backward(hidden, scale, gain, upstream):
    weighted = gain * upstream
    return scale * weighted - hidden * (scale * scale * scale) * jnp.mean(hidden * weighted, -1, keepdims=True)


def matrix(blocks, index, width):
    return jnp.concatenate([b[index * width : (index + 1) * width, :] for b in blocks], 0)


def store_rows(ref, lead, index, grad, turn):
    blocks = ref.shape[len(lead)]
    size = grad.shape[0] // blocks
    for a in range(blocks):
        ref[(*lead, a ^ turn, slice(index * size, (index + 1) * size))] = grad[a * size : (a + 1) * size].astype(bf16)


def store_extra(ref, lead, start, rows, turn):
    for a in range(ref.shape[len(lead)]):
        ref[(*lead, a ^ turn, slice(start, start + EXTRA))] = (rows if a == 0 else jnp.zeros_like(rows)).astype(bf16)


EXTRA = 8


def first_of(turn_ref):
    return turn_ref[1] == 0


def passed_on(blocks, first, index):
    own, core, far, far_y, both, both_y = blocks
    width = far.shape[0]
    rows = slice(index * width, (index + 1) * width)
    straight = first == (index == 0)
    pieces = [own[rows, :], core[rows, :]]
    for here, there in ((far, far_y), (both, both_y)):
        pieces.append(jnp.where(straight, here[...], there[...]))
    return jnp.concatenate(pieces, 0)


def store_halves(low_ref, high_ref, ref):
    half = ref.shape[0] // 2
    low_ref[...] = ref[:half]
    high_ref[...] = ref[half:]


def store_grad(keep_ref, send_ref, index, grad, turn):
    width = grad.shape[0] // 4
    for j in range(4):
        store_rows((keep_ref, send_ref)[j % 2], (j // 2,), index, grad[j * width : (j + 1) * width], turn)


def pair_masks():
    lane = lax.broadcasted_iota(jnp.int32, (1, PAIR), 1)
    return (lane < HEAD_DIM).astype(bf16), (lane >= HEAD_DIM).astype(bf16)


def stack_pair(rows, masks):
    return jnp.concatenate([rows * masks[0], rows * masks[1]], 0)


def unstack_pair(both):
    lane = lax.broadcasted_iota(jnp.int32, (TGT_LEN, PAIR), 1)
    return jnp.where(lane < HEAD_DIM, both[:TGT_LEN], both[TGT_LEN:])


def softmax_rows(scores):
    weights = jnp.exp(scores - jnp.max(scores, -1, keepdims=True))
    return weights * (1.0 / jnp.sum(weights, -1, keepdims=True))


def locate(step, pairs, keys):
    example = lax.div(step, pairs)
    pair = lax.rem(step, pairs)
    rows = pl.ds(pl.multiple_of(example * TGT_LEN, TGT_LEN), TGT_LEN)
    key_rows = pl.ds(pl.multiple_of(example * keys, keys), keys)
    cols = pl.ds(pl.multiple_of(pair * PAIR, PAIR), PAIR)
    return example, pair, rows, key_rows, cols


def cross_probs(queries, key_rows, length):
    scores = dot_nt(queries, key_rows)
    key = lax.broadcasted_iota(jnp.int32, scores.shape, 1)
    return softmax_rows(jnp.where(key < length, scores, masked_fill))


def attend(q_ref, k_ref, v_ref, mixed_ref, keys, probs_of):
    masks = pair_masks()
    pairs = q_ref.shape[1] // PAIR
    examples = q_ref.shape[0] // TGT_LEN

    def step(i, carry):
        example, pair, rows, key_rows, cols = locate(i, pairs, keys)
        probs = probs_of(stack_pair(q_ref[rows, cols], masks), k_ref[key_rows, cols], example, pair)
        mixed = dot_nn(probs.astype(bf16), v_ref[key_rows, cols])
        mixed_ref[rows, cols] = unstack_pair(mixed).astype(bf16)
        return carry

    lax.fori_loop(0, examples * pairs, step, 0, unroll=2)


def attend_back(q_ref, k_ref, v_ref, m_ref, dq_ref, dk_ref, dv_ref, keys, probs_of):
    masks = pair_masks()
    pairs = q_ref.shape[1] // PAIR
    examples = q_ref.shape[0] // TGT_LEN

    def step(i, carry):
        example, pair, rows, key_rows, cols = locate(i, pairs, keys)
        queries = stack_pair(q_ref[rows, cols], masks)
        grads = stack_pair(m_ref[rows, cols], masks)
        key_block = k_ref[key_rows, cols]
        probs = probs_of(queries, key_block, example, pair)
        dv_ref[cols, key_rows] = dot_tn(grads, probs.astype(bf16)).astype(bf16)
        prob_grad = dot_nt(grads, v_ref[key_rows, cols])
        score_grad = probs * (prob_grad - jnp.sum(probs * prob_grad, -1, keepdims=True))
        low = score_grad.astype(bf16)
        dq_ref[rows, cols] = unstack_pair(dot_nn(low, key_block)).astype(bf16)
        dk_ref[cols, key_rows] = dot_tn(queries, low).astype(bf16)
        return carry

    lax.fori_loop(0, examples * pairs, step, 0, unroll=UNROLL)


UNROLL = 4


def fill_bias(table_ref, bias_ref):
    for head in range(bias_ref.shape[0] // TGT_LEN):
        row = jnp.broadcast_to(table_ref[head : head + 1, :], (TGT_LEN, TGT_LEN))
        bias_ref[head * TGT_LEN : (head + 1) * TGT_LEN, :] = pltpu.roll(row, 0, axis=1, stride=1, stride_axis=0)


def stack_heads(rows):
    lane = lax.broadcasted_iota(jnp.int32, (1, rows.shape[1]), 1)
    heads = rows.shape[1] // HEAD_DIM
    return jnp.concatenate([rows * (lax.div(lane, HEAD_DIM) == h).astype(bf16) for h in range(heads)], 0)


def unstack_heads(stacked):
    length = TGT_LEN
    lane = lax.broadcasted_iota(jnp.int32, (length, stacked.shape[1]), 1)
    out = stacked[:length]
    for h in range(1, stacked.shape[1] // HEAD_DIM):
        out = jnp.where(lane >= h * HEAD_DIM, stacked[h * length : (h + 1) * length], out)
    return out


def self_probs(queries, key_rows, bias, length):
    scores = dot_nt(queries, key_rows) + bias
    key = lax.broadcasted_iota(jnp.int32, scores.shape, 1)
    query = lax.rem(lax.broadcasted_iota(jnp.int32, scores.shape, 0), TGT_LEN)
    return softmax_rows(jnp.where((key <= query) & (key < length), scores, masked_fill))


def diagonal_sums(grad):
    query = lax.broadcasted_iota(jnp.int32, grad.shape, 0)
    for bit in range(TGT_LEN.bit_length() - 1):
        moved = pltpu.roll(grad, TGT_LEN - (1 << bit), axis=1)
        grad = jnp.where((query >> bit) & 1 == 1, moved, grad)
    return jnp.sum(grad, 0, keepdims=True)


def first_norm(x_ref, gain_ref, n_ref):
    hidden = x_ref[...].astype(f32)
    n_ref[...] = (hidden * row_scale(hidden) * gain_ref[...].reshape(1, -1)).astype(bf16)


def self_forward(
    base, n0, n1, wq_ref, wk_ref, wv_ref, wo_ref, table_ref, rank_ref, len_ref,
    q_ref, k_ref, v_ref, mixed_ref, keep_ref, send_ref, bias_ref,
):
    fill_bias(table_ref, bias_ref)
    size = n0.shape[0]
    for j, n in enumerate((n0, n1)):
        rows = slice(j * size, (j + 1) * size)
        for ref, w in ((q_ref, wq_ref), (k_ref, wk_ref), (v_ref, wv_ref)):
            ref[rows, :] = dot_nt(n[...], w[...]).astype(bf16)

    def step(i, carry):
        rows = pl.ds(pl.multiple_of(i * TGT_LEN, TGT_LEN), TGT_LEN)
        length = len_ref[(rank_ref[0] * (size // TGT_LEN)) ^ (base + i)]
        probs = self_probs(stack_heads(q_ref[rows, :]), k_ref[rows, :], bias_ref[...], length)
        mixed_ref[rows, :] = unstack_heads(dot_nn(probs.astype(bf16), v_ref[rows, :])).astype(bf16)
        return carry

    lax.fori_loop(0, 2 * size // TGT_LEN, step, 0, unroll=2)
    keep_ref[...] = dot_nn(mixed_ref[:size, :], wo_ref[...])
    send_ref[...] = dot_nn(mixed_ref[size:, :], wo_ref[...]).astype(bf16)


def store_parts(own_ref, chip_ref, send_ref, parts):
    for j, part in enumerate(parts):
        if j == 0:
            own_ref[...] = part
        elif j == 2:
            chip_ref[...] = part
        else:
            send_ref[j // 2] = part.astype(bf16)


def memory_forward(mem_ref, w0, w1, w2, w3, k_ref, v_ref):
    width = k_ref.shape[1] // 4
    half = mem_ref.shape[0] // 2
    blocks = (w0, w1, w2, w3)

    def step(i, carry):
        rows = pl.ds(pl.multiple_of(i * half, half), half)
        k_ref[rows, :] = dot_nt(mem_ref[rows, :], matrix(blocks, KEY, width)).astype(bf16)
        v_ref[rows, :] = dot_nt(mem_ref[rows, :], matrix(blocks, KEY + 1, width)).astype(bf16)
        return carry

    lax.fori_loop(0, 2, step, 0)


def cross_forward(
    x_ref, own_ref, near_ref, far_ref, k_ref, v_ref, gain_two_ref, gain_three_ref, w0, w1, w2, w3, w4, w5, rank_ref, len_ref, turn_ref,
    after_self_ref, n2_ref, q_ref, mixed_ref, after_ref, n3_ref,
):
    blocks = (w0, w1, w2, w3, w4, w5)
    first = first_of(turn_ref)
    after_self = x_ref[...].astype(f32) + own_ref[...] + near_ref[...].astype(f32) + far_ref[...].astype(f32)
    after_self_ref[...] = after_self
    normed = (after_self * row_scale(after_self) * gain_two_ref[...].reshape(1, -1)).astype(bf16)
    n2_ref[...] = normed
    q_ref[...] = dot_nt(normed, passed_on(blocks, first, 0)).astype(bf16)

    def probs(queries, key_rows, example, pair):
        return cross_probs(queries, key_rows, len_ref[rank_ref[0] * (q_ref.shape[0] // TGT_LEN) + example])

    attend(q_ref, k_ref, v_ref, mixed_ref, MEM_LEN, probs)
    after = after_self_ref[...] + dot_nn(mixed_ref[...], passed_on(blocks, first, 1))
    after_ref[...] = after
    n3_ref[...] = (after * row_scale(after) * gain_three_ref[...].reshape(1, -1)).astype(bf16)


def feed_hidden(c0, c1, c2, c3, out_ref, hidden_ref):
    size = c0.shape[0]
    for base, first, second in ((0, c0, c1), (2 * size, c2, c3)):

        def step(i, carry, base=base, first=first, second=second):
            rows = pl.ds(pl.multiple_of(base + i * size, size), size)
            hidden_ref[rows, :] = dot_nt(jnp.where(i == 0, first[...], second[...]), out_ref[...])
            return carry

        lax.fori_loop(0, 2, step, 0)


def feed_main(base, g0, g1, hidden_ref, in_ref, keep_ref, send_ref, act_ref, pre_grad_ref):
    size = g0.shape[0]
    for j, g in enumerate((g0, g1)):
        rows = slice(j * size, (j + 1) * size)
        pre = dot_nn(g[...], in_ref[...])
        square = pre * pre
        tanh = jnp.tanh(tanh_scale * (pre + cubic_term * square * pre))
        act_ref[rows, :] = (0.5 * pre * (1.0 + tanh)).astype(bf16)
        slope = 0.5 * (1.0 + tanh) + 0.5 * pre * (1.0 - tanh * tanh) * (
            tanh_scale * (1.0 + 3.0 * cubic_term * square)
        )
        low = (hidden_ref[base + j * size : base + (j + 1) * size, :] * slope).astype(bf16)
        pre_grad_ref[rows, :] = low
        grad = dot_nt(low, in_ref[...])
        if j == 0:
            keep_ref[...] = grad
        else:
            send_ref[...] = grad.astype(bf16)


def feed_rest(
    g0, g1, g2, g3, c0, c1, c2, c3, act_a, act_b, pre_grad_a, pre_grad_b, out_ref, turn_ref, own_ref, chip_ref, send_ref, low_ref, high_ref, grads_ref
):
    activated = jnp.concatenate([act_a[...], act_b[...]], 0)
    pre_grad = jnp.concatenate([pre_grad_a[...], pre_grad_b[...]], 0)
    gathered = jnp.concatenate([g[...] for g in (g0, g1, g2, g3)], 0)
    store_rows(grads_ref, (), 0, dot_tn(gathered, pre_grad), turn_ref[0])
    upstream = jnp.concatenate([c[...] for c in (c0, c1, c2, c3)], 0)
    store_rows(grads_ref, (), 1, dot_tn(activated, upstream), turn_ref[0])
    store_halves(low_ref, high_ref, grads_ref)
    size = g0.shape[0]
    for slot, act, keep_ref in ((0, act_a, own_ref), (1, act_b, chip_ref)):

        def step(i, carry, slot=slot, act=act, keep_ref=keep_ref):
            part = dot_nn(act[pl.ds(pl.multiple_of(i * size, size), size), :], out_ref[...])

            @pl.when(i == 0)
            def _():
                keep_ref[...] = part

            @pl.when(i == 1)
            def _():
                send_ref[slot] = part.astype(bf16)

            return carry

        lax.fori_loop(0, 2, step, 0)


def cross_backward(
    own_ref, near_ref, far_ref, cot_ref, after_ref, after_self_ref, gain_two_ref, gain_three_ref,
    n2_ref, q_ref, k_ref, v_ref, mixed_ref, w0, w1, w2, w3, w4, w5, rank_ref, len_ref, turn_ref,
    grad_one_ref, up_ref, dk_ref, dv_ref, gains_ref, keep_ref, send_ref, m_ref, dq_ref,
):
    blocks = (w0, w1, w2, w3, w4, w5)
    first = first_of(turn_ref)
    after = after_ref[...]
    scale = row_scale(after)
    upstream = own_ref[...] + near_ref[...].astype(f32) + far_ref[...].astype(f32)
    gains_ref[1:2, :] = jnp.sum(upstream * after * scale, 0, keepdims=True)
    grad_two = cot_ref[...].astype(f32) + norm_backward(after, scale, gain_three_ref[...].reshape(1, -1), upstream)
    grad_one_ref[...] = grad_two
    up_two = grad_two.astype(bf16)
    m_ref[...] = dot_nt(up_two, passed_on(blocks, first, 1)).astype(bf16)
    store_grad(keep_ref, send_ref, 1, dot_tn(mixed_ref[...], up_two), turn_ref[0])

    def probs(queries, key_rows, example, pair):
        return cross_probs(queries, key_rows, len_ref[rank_ref[0] * (q_ref.shape[0] // TGT_LEN) + example])

    attend_back(q_ref, k_ref, v_ref, m_ref, dq_ref, dk_ref, dv_ref, MEM_LEN, probs)
    store_grad(keep_ref, send_ref, 0, dot_tn(dq_ref[...], n2_ref[...]), turn_ref[0])
    upstream = dot_nn(dq_ref[...], passed_on(blocks, first, 0))
    hidden = after_self_ref[...]
    scale = row_scale(hidden)
    gains_ref[0:1, :] = jnp.sum(upstream * hidden * scale, 0, keepdims=True)
    grad_one = grad_one_ref[...] + norm_backward(hidden, scale, gain_two_ref[...].reshape(1, -1), upstream)
    grad_one_ref[...] = grad_one
    up_ref[...] = grad_one.astype(bf16)


def memory_weights(dk_ref, dv_ref, mem_ref, keep_in, send_in, late_ref, turn_ref, keep_ref, send_ref):
    count = keep_in.shape[2]
    late = jnp.concatenate([late_ref[...], jnp.zeros((EXTRA - 2, late_ref.shape[1]), f32)], 0)
    for j in range(2):
        for ref, given in ((keep_ref, keep_in), (send_ref, send_in)):
            for a in range(keep_in.shape[1]):
                ref[j, a, :count] = given[j, a]
            store_extra(ref, (j,), 2 * count, late, turn_ref[0])
    store_grad(keep_ref, send_ref, 2, dot_nn(dk_ref[...], mem_ref[...]), turn_ref[0])
    store_grad(keep_ref, send_ref, 3, dot_nn(dv_ref[...], mem_ref[...]), turn_ref[0])


def self_backward(
    u0, u1, u2, u3, n0, n1, n2, n3, qa, ka, va, xa, qb, kb, vb, xb, wq_ref, wk_ref, wv_ref, wo_ref, gain_ref,
    table_ref, rank_ref, len_ref, turn_ref,
    low_ref, high_ref, own_ref, chip_ref, send_ref,
    bias_ref, score_ref, m_ref, dq_ref, dk_ref, dv_ref, grads_ref,
):
    fill_bias(table_ref, bias_ref)
    score_ref[...] = jnp.zeros_like(score_ref)
    size = n0.shape[0]
    width = qa.shape[1]
    for j, u in enumerate((u0, u1, u2, u3)):
        m_ref[j * size : (j + 1) * size, :] = dot_nt(u[...], wo_ref[...]).astype(bf16)

    for base, q_ref, k_ref, v_ref in ((0, qa, ka, va), (2 * size, qb, kb, vb)):

        def step(i, carry, base=base, q_ref=q_ref, k_ref=k_ref, v_ref=v_ref):
            rows = pl.ds(pl.multiple_of(i * TGT_LEN, TGT_LEN), TGT_LEN)
            all_rows = pl.ds(pl.multiple_of(base + i * TGT_LEN, TGT_LEN), TGT_LEN)
            length = len_ref[(rank_ref[0] * (size // TGT_LEN)) ^ (base // TGT_LEN + i)]
            queries = stack_heads(q_ref[rows, :])
            grads = stack_heads(m_ref[all_rows, :])
            key_block = k_ref[rows, :]
            probs = self_probs(queries, key_block, bias_ref[...], length)
            dv_ref[all_rows, :] = dot_tn(probs.astype(bf16), grads).astype(bf16)
            prob_grad = dot_nt(grads, v_ref[rows, :])
            score_grad = probs * (prob_grad - jnp.sum(probs * prob_grad, -1, keepdims=True))
            score_ref[...] += score_grad
            low = score_grad.astype(bf16)
            dq_ref[all_rows, :] = unstack_heads(dot_nn(low, key_block)).astype(bf16)
            dk_ref[all_rows, :] = dot_tn(low, queries).astype(bf16)
            return carry

        lax.fori_loop(0, 2 * size // TGT_LEN, step, 0, unroll=2)
    normed = jnp.concatenate([n[...] for n in (n0, n1, n2, n3)], 0)
    upstream = jnp.concatenate([u[...] for u in (u0, u1, u2, u3)], 0)
    mixed = jnp.concatenate([xa[...], xb[...]], 0)
    for index, (left, right) in enumerate(
        ((dq_ref[...], normed), (dk_ref[...], normed), (dv_ref[...], normed), (mixed, upstream))
    ):
        store_rows(grads_ref, (), index, dot_tn(left, right), turn_ref[0])
    gain = jnp.zeros((1, n0.shape[1]), f32)
    parts = []
    for j, n in enumerate((n0, n1, n2, n3)):
        rows = slice(j * size, (j + 1) * size)
        part = dot_nn(dq_ref[rows, :], wq_ref[...])
        part = part + dot_nn(dk_ref[rows, :], wk_ref[...]) + dot_nn(dv_ref[rows, :], wv_ref[...])
        gain += jnp.sum(part * n[...].astype(f32), 0, keepdims=True)
        if j == 0:
            own_ref[...] = part
        elif j == 2:
            chip_ref[...] = part
        else:
            send_ref[j // 2] = part.astype(bf16)
    gain = gain * (1.0 / gain_ref[...].reshape(1, -1))
    heads = width // HEAD_DIM
    sums = [diagonal_sums(score_ref[h * TGT_LEN : (h + 1) * TGT_LEN, :]) for h in range(heads)]
    sums = jnp.concatenate(sums + [jnp.zeros((EXTRA - 1 - heads, TGT_LEN), f32)], 0)
    sums = jnp.concatenate([sums, jnp.zeros((EXTRA - 1, gain.shape[1] - TGT_LEN), f32)], 1)
    store_extra(grads_ref, (), 4 * (width // grads_ref.shape[0]), jnp.concatenate([gain, sums], 0), turn_ref[0])
    store_halves(low_ref, high_ref, grads_ref)


def last_norm(grad_one_ref, own_ref, near_ref, far_ref, x_ref, gain_ref, grad_ref):
    upstream = own_ref[...] + near_ref[...].astype(f32) + far_ref[...].astype(f32)
    hidden = x_ref[...].astype(f32)
    grad_ref[...] = grad_one_ref[...] + norm_backward(hidden, row_scale(hidden), gain_ref[...].reshape(1, -1), upstream)


def gather_order(bits, early):
    return [0, bits - 1, *range(1, bits - 1)] if early else list(range(bits))


def gather_rows(low_ref, high_ref, rows, places, turn, early):
    half = low_ref.shape[0]
    order = gather_order((2 * half).bit_length() - 1, early)
    pieces = []
    for a in places:
        place = a ^ turn
        inside = sum(((place >> bit) & 1) << i for i, bit in enumerate(order[:-1]))
        low = (place >> order[-1]) & 1 == 0
        pieces.append(jnp.where(low, low_ref[inside, rows].astype(f32), high_ref[inside, rows].astype(f32)))
    return jnp.concatenate(pieces, 0)


def finish(early, low_ref, high_ref, turn_ref, *outs):
    blocks = 2 * low_ref.shape[0]
    start = 0
    for ref in outs:
        extra = ref.shape[0] == EXTRA
        places = range(1) if extra else range(blocks)
        size = EXTRA if extra else ref.shape[0] // blocks
        ref[...] = gather_rows(low_ref, high_ref, slice(start, start + size), places, turn_ref[0], early)
        start += size


def memory_backward(dk_ref, dv_ref, w0, w1, w2, w3, grad_ref):
    blocks = (w0, w1, w2, w3)
    width = dk_ref.shape[0] // 4
    half = grad_ref.shape[0] // 2

    def step(i, carry):
        rows = pl.ds(pl.multiple_of(i * half, half), half)
        keys = dot_tn(dk_ref[:, rows], matrix(blocks, KEY, width))
        grad_ref[rows, :] = keys + dot_tn(dv_ref[:, rows], matrix(blocks, KEY + 1, width))
        return carry

    lax.fori_loop(0, 2, step, 0)


KEY = 0


def call(kernel, operands, outs, scratch=(), flops=0, smem=()):
    moved = sum(a.size * a.dtype.itemsize for a in operands)
    moved += sum(functools.reduce(lambda x, y: x * y, s) * jnp.dtype(t).itemsize for s, t in outs)
    return pl.pallas_call(
        kernel,
        out_shape=[jax.ShapeDtypeStruct(s, t) for s, t in outs],
        in_specs=[
            pl.BlockSpec(memory_space=pltpu.SMEM if i in smem else pltpu.VMEM) for i in range(len(operands))
        ],
        out_specs=[pl.BlockSpec(memory_space=pltpu.VMEM) for _ in outs],
        scratch_shapes=[pltpu.VMEM(s, t) for s, t in scratch],
        compiler_params=pltpu.CompilerParams(vmem_limit_bytes=VMEM_LIMIT),
        cost_estimate=pl.CostEstimate(flops=flops, bytes_accessed=moved, transcendentals=0),
    )(*operands)


VMEM_LIMIT = 56 * 1024 * 1024


def after(value, *others):
    return lax.optimization_barrier((value, *others))[0]


def swap_core(a):
    return lax.ppermute(a, "mp", [(0, 1), (1, 0), (2, 3), (3, 2)])


def swap_chip(a):
    return lax.ppermute(a, "mp", [(0, 2), (2, 0), (1, 3), (3, 1)])


def gather_blocks(a):
    far = swap_chip(a)
    return (a, swap_core(a), far, swap_core(far))


def core_sum(chip, got):
    return (chip.astype(f32) + got.astype(f32)).astype(bf16)


def plus(a, b):
    return (a.astype(f32) + b.astype(f32)).astype(bf16)


def swap_dp(a, bit):
    return lax.ppermute(a, "dp", [(i, i ^ (1 << bit)) for i in range(lax.axis_size("dp"))])


def dp_chain(keep, send, steps=None):
    bits = lax.axis_size("dp").bit_length() - 1
    for bit in range(bits):
        got = swap_dp(send, bit)
        tokens = yield send
        got = after(got, *tokens)
        half = keep.shape[0] // 2
        if half:
            send, keep = plus(keep[half:], got[half:]), plus(keep[:half], got[:half])
        else:
            value = plus(keep, got)
    yield from gather_chain(value, range(bits)[:steps])


def gather_chain(value, order):
    bits = lax.axis_size("dp").bit_length() - 1
    order = list(order)
    for bit in order:
        other = swap_dp(value, bits - 1 - bit)
        tokens = yield value
        other = after(other, *tokens)
        if bit != order[-1]:
            value = jnp.concatenate([value, other], 0)
    yield value, other


ROUNDS = (
    ("zero",),
    ("two",),
    ("two",),
    ("zero", "one"),
    ("two", "one"),
)
LATE_ROUNDS = (
    ("two", "one"),
    ("in", "out"),
    ("two",),
    ("one",),
)
FINISH = ("in", "out", "one", "two", "one+")


class Chains:
    def __init__(self):
        self.under_way, self.last, self.tokens = {}, {}, ()

    def start(self, name, chain):
        self.under_way[name] = chain
        self.last[name] = next(chain)
        return self.last[name]

    def turn(self, *names):
        sent = []
        for name in names:
            try:
                self.last[name] = self.under_way[name].send(self.tokens)
                sent.append(self.last[name])
            except (StopIteration, KeyError):
                self.under_way.pop(name, None)
        if sent:
            self.tokens = tuple(t for t in sent if not isinstance(t, tuple)) or sent[0]
        return self.tokens

    def drain(self):
        while self.under_way:
            for name in list(self.under_way):
                self.turn(name)


def body(
    inputs,
    memory,
    target_len,
    memory_len,
    bucket_map,
    self_gain,
    self_query,
    self_key,
    self_value,
    self_out,
    bias_table,
    cross_gain,
    cross_query,
    cross_key,
    cross_value,
    cross_out,
    feed_gain,
    feed_input,
    feed_output,
    cotangent,
):
    rank = lax.axis_index("mp")
    rows, d = inputs.shape
    key_rows = memory.shape[0]
    width = self_query.shape[1]
    wide = 4 * width
    heads = bias_table.shape[1]
    units = feed_input.shape[1]
    examples = rows // TGT_LEN
    rank_value = rank.astype(jnp.int32).reshape(1)
    blocks = lax.axis_size("dp")
    place = lax.axis_index("dp").astype(jnp.int32)
    turn = jnp.zeros((1,), jnp.int32)
    for bit in range(blocks.bit_length() - 1):
        turn = 2 * turn + ((place >> bit) & 1)
    turn = jnp.concatenate([turn, (place & 1).reshape(1)])

    distance = (TGT_LEN - jnp.arange(TGT_LEN, dtype=jnp.int32)) % TGT_LEN
    lookup = distance[:, None] == jnp.arange(TGT_LEN, dtype=jnp.int32)[None, :]
    bucket = jnp.sum(jnp.where(lookup, bucket_map[None, :], 0), -1)
    hot = (bucket[:, None] == jnp.arange(BUCKETS, dtype=jnp.int32)[None, :]).astype(f32)
    by_distance = lax.dot_general(bias_table, hot, (((0,), (1,)), ((), ())), precision=highest)
    big = (rows, d)
    head_rows = (rows, wide)
    key_heads = (key_rows, wide)
    heads_key = (wide, key_rows)
    square = ((heads * TGT_LEN, TGT_LEN), f32)
    group_heads = (4 * rows, width)
    half_heads = (2 * rows, width)
    pack = ((2, rows, d), bf16)
    product = 2 * rows * d * wide

    def grad_half(count, size, more=0):
        return ((blocks // 2, count * (size // blocks) + more, d), bf16)

    def grad_rows(count, size, lead=(), more=0):
        return ((*lead, blocks, count * (size // blocks) + more, d), bf16)

    pair_own = jnp.concatenate([cross_key.T, cross_value.T], 0)
    query_own = jnp.concatenate([cross_query.T, cross_out], 0)
    half_own = lax.dynamic_slice_in_dim(query_own, (place & 1) * width, width, 0)
    normed_one = call(first_norm, (inputs, self_gain), [(big, bf16)])[0]
    far = swap_chip(normed_one)
    pair_far = swap_chip(after(pair_own, normed_one))
    self_weights = (self_query.T, self_key.T, self_value.T, self_out)

    def self_half(base, pair):
        return call(
            functools.partial(self_forward, base),
            (*pair, *self_weights, by_distance, rank_value, target_len),
            [(half_heads, bf16)] * 4 + [(big, f32), (big, bf16)],
            [square],
            flops=2 * product,
            smem=(7, 8),
        )

    ones = (normed_one, swap_core(normed_one))
    *self_a, own, send = self_half(0, ones)
    near = swap_core(send)
    far = after(far, near)
    ones = (*ones, far, swap_core(far))
    *self_b, chip, send = self_half(2 * rows // TGT_LEN, ones[2:])
    pair_far = after(pair_far, chip)
    half_far = swap_chip(after(half_own, normed_one))
    far_send = core_sum(chip, swap_core(after(send, pair_far)))
    far = swap_chip(far_send)
    pair = (pair_own, swap_core(pair_own), pair_far, swap_core(pair_far))
    cross_k, cross_v = call(
        memory_forward, (after(memory, far_send), *pair), [(key_heads, bf16)] * 2, flops=8 * product
    )
    half_far = after(half_far, cross_v)
    half_passed = swap_dp(half_far, 0)
    far = after(far, half_far)
    half_passed = after(half_passed, far)
    query = (query_own, swap_core(query_own), half_far, half_passed, swap_core(half_far), swap_core(half_passed))
    ups_far = swap_chip(after(cotangent, far))
    after_self, normed_two, cross_q, cross_mixed, after_cross, normed_three = call(
        cross_forward,
        (inputs, own, near, far, cross_k, cross_v, cross_gain, feed_gain, *query, rank_value, memory_len, turn),
        [(big, f32), (big, bf16), (head_rows, bf16), (head_rows, bf16), (big, f32), (big, bf16)],
        flops=6 * product,
        smem=(14, 15, 16),
    )
    ups_far = after(ups_far, normed_three)
    ups = (cotangent, swap_core(cotangent), ups_far, swap_core(ups_far))
    many = 4 * rows
    far = swap_chip(normed_three)
    hidden = call(feed_hidden, (*ups, feed_output), [((many, units), f32)], flops=4 * product)[0]

    def feed_half(base, pair):
        return call(
            functools.partial(feed_main, base),
            (*pair, hidden, feed_input),
            [(big, f32), (big, bf16), ((2 * rows, units), bf16), ((2 * rows, units), bf16)],
            flops=4 * product,
        )

    gathered = (normed_three, swap_core(normed_three))
    own, send, act_a, pre_grad_a = feed_half(0, gathered)
    near = swap_core(send)
    far = after(far, near)
    gathered = (*gathered, far, swap_core(far))
    chip, send, act_b, pre_grad_b = feed_half(2 * rows, gathered[2:])
    far_send = core_sum(chip, swap_core(send))
    far = swap_chip(far_send)
    out_own, out_chip, out_send, low, high = call(
        feed_rest,
        (*gathered, *ups, act_a, after(act_b, far_send), pre_grad_a, pre_grad_b, feed_output, turn),
        [(big, f32), (big, f32), pack] + [grad_half(2, d)] * 2,
        [grad_rows(2, d)],
        flops=12 * product,
        smem=(13,),
    )
    chains = Chains()
    token = chains.start("zero", dp_chain(low, high, steps=1))
    far = after(far, token)
    grad_one, up_one, key_grad, value_grad, late_gains, keep, send = call(
        cross_backward,
        (own, near, far, cotangent, after_cross, after_self, cross_gain, feed_gain)
        + (normed_two, cross_q, cross_k, cross_v, cross_mixed, *query, rank_value, memory_len, turn),
        [(big, f32), (big, bf16), (heads_key, bf16), (heads_key, bf16), ((2, d), f32)] + [grad_rows(2, width, (2,))] * 2,
        [(head_rows, bf16), (head_rows, bf16)],
        flops=16 * product,
        smem=(19, 20, 21),
    )
    up_far = swap_chip(up_one)
    keep, send = call(
        memory_weights,
        (key_grad, value_grad, memory, keep, send, late_gains, turn),
        [grad_rows(4, width, (2,), EXTRA)] * 2,
        flops=8 * product,
        smem=(6,),
    )
    up_far = after(up_far, keep)
    chains.tokens = (up_far,)
    token = chains.turn("zero")
    got = swap_core(after(send, *token))
    one_send = core_sum(keep[1], got[1])
    one_far = swap_chip(one_send)
    self_ups = (up_one, swap_core(up_one), after(up_far, one_send), swap_core(up_far))
    low, high, own, chip, send = call(
        self_backward,
        (*self_ups, *ones, *self_a, *self_b)
        + (*self_weights, self_gain, by_distance, rank_value, target_len, turn),
        [grad_half(4, width, EXTRA)] * 2 + [(big, f32), (big, f32), pack],
        [square, square] + [(group_heads, bf16)] * 4 + [grad_rows(4, width, (), EXTRA)],
        flops=10 * product,
        smem=(22, 23, 24),
    )
    chains.tokens = (own,)
    token = chains.turn("zero")
    token = chains.start("two", dp_chain(low, after(high, *token)))
    got_self = swap_core(after(send, token))
    far_send = core_sum(chip, got_self[1])
    far = swap_chip(far_send)
    one_sum = keep[0].astype(f32) + got[0].astype(f32) + after(one_far, far_send).astype(f32)
    one_sum = one_sum.astype(bf16)
    token = chains.start("one", dp_chain(one_sum[: blocks // 2], one_sum[blocks // 2 :]))
    memory_grad = call(
        memory_backward,
        (after(key_grad, token), value_grad, *pair),
        [((key_rows, d), f32)],
        flops=8 * product,
    )[0]
    chains.tokens = (memory_grad,)
    more = blocks.bit_length() - 1 - 3
    for _ in range(more):
        chains.turn("zero")
    for names in ROUNDS:
        chains.turn(*names)
        if "feed" not in chains.last and isinstance(chains.last["zero"], tuple):
            bits = blocks.bit_length() - 1
            both = jnp.concatenate(chains.last["zero"], 0)
            half = both.shape[1] // 2
            chains.last["feed"] = None
            chains.start("in", gather_chain(both[:, :half], gather_order(bits, True)[1:]))
            chains.start("out", gather_chain(both[:, half:], gather_order(bits, False)[1:]))
    inputs_grad = call(
        last_norm,
        (grad_one, own, got_self[0], after(far, *chains.tokens), inputs, self_gain),
        [(big, f32)],
    )[0]
    chains.tokens = (inputs_grad,)
    got_out = swap_core(after(out_send, *chains.tokens))
    out_far = swap_chip(core_sum(out_chip, got_out[1]))
    for _ in range(2 * more):
        chains.turn("two", "one")
    for names in LATE_ROUNDS:
        chains.turn(*names)
    grads = {}
    for name in FINISH:
        if name == "in":
            for _ in range(more):
                chains.turn("in", "out")
            chains.turn("in", "out")
        elif name == "one":
            chains.turn("one")
            continue
        elif name == "two":
            chains.turn("two", "one")
        name = name.strip("+")
        feed = name in ("in", "out")
        outs = [((d, d), f32)] if feed else [((width, d), f32)] * 4 + [((EXTRA, d), f32)]
        grads[name] = call(
            functools.partial(finish, name == "in"), (*chains.last[name], turn), outs, smem=(2,)
        )
        if feed or name == "one":
            chains.tokens = (grads[name][-1],)
    extra = grads["two"][-1]
    gain_one = after(extra[:1], chains.last["one"][1])
    gain_one = gain_one + swap_core(gain_one)
    gain_one = gain_one + swap_chip(gain_one)
    layer_out = (after_cross + out_own + got_out[0].astype(f32) + out_far.astype(f32)).astype(bf16)
    feed_grads, cross_grads, self_grads = (grads["in"][0], grads["out"][0]), grads["one"], grads["two"]
    own_sums = extra[1 : 1 + heads, :TGT_LEN]
    bias_grad = lax.dot_general(hot, own_sums, (((0,), (1,)), ((), ())), precision=highest)

    return (
        layer_out,
        inputs_grad,
        memory_grad,
        gain_one[0],
        self_grads[0].T,
        self_grads[1].T,
        self_grads[2].T,
        self_grads[3],
        bias_grad,
        cross_grads[4][0],
        cross_grads[0].T,
        cross_grads[2].T,
        cross_grads[3].T,
        cross_grads[1],
        cross_grads[4][1],
        *feed_grads,
    )


def solution(mesh):
    in_specs = (
        P(("dp", "mp"), None),
        P(("dp", "mp"), None),
        P("dp"),
        P("dp"),
        P(),
        P(),
        P(None, "mp"),
        P(None, "mp"),
        P(None, "mp"),
        P("mp", None),
        P(None, "mp"),
        P(),
        P(None, "mp"),
        P(None, "mp"),
        P(None, "mp"),
        P("mp", None),
        P(),
        P(None, "mp"),
        P("mp", None),
        P(("dp", "mp"), None),
    )
    out_specs = (
        P(("dp", "mp"), None),
        P(("dp", "mp"), None),
        P(("dp", "mp"), None),
        P(),
        P(None, "mp"),
        P(None, "mp"),
        P(None, "mp"),
        P("mp", None),
        P(None, "mp"),
        P(),
        P(None, "mp"),
        P(None, "mp"),
        P(None, "mp"),
        P("mp", None),
        P(),
        P(None, "mp"),
        P("mp", None),
    )
    return jax.shard_map(body, mesh=mesh, in_specs=in_specs, out_specs=out_specs, check_vma=False)
```
